32 devices in a mesh: gx: 8 (over z, y), gy: 4 (over x, core).
Axes of the slice: x: 2, y: 2, z: 4, core: 2. Of those that a mesh axis runs over, the one named last changes fastest.
Arguments:
- block_input: bfloat16 [960, 8192], P('gx', 'gy'), may hold values from -6 to 6
- attn_gain: float32 [960], P('gx'), may hold values from 0.5 to 1.5
- query_weight: bfloat16 [960, 960], P('gx', 'gy'), may hold values from -2 to 2
- key_weight: bfloat16 [960, 320], P('gx', 'gy'), may hold values from -2 to 2
- value_weight: bfloat16 [960, 320], P('gx', 'gy'), may hold values from -0.1875 to 0.1875
- output_weight: bfloat16 [960, 960], P('gy', 'gx'), may hold values from -0.5 to 0.5
- ffn_gain: float32 [960], P('gx'), may hold values from 0.5 to 1.5
- gate_weight: bfloat16 [960, 2560], P('gx', 'gy'), may hold values from -0.1875 to 0.1875
- up_weight: bfloat16 [960, 2560], P('gx', 'gy'), may hold values from -0.1875 to 0.1875
- down_weight: bfloat16 [2560, 960], P('gy', 'gx'), may hold values from -0.125 to 0.125
- segment_ids: int32 [8, 1024], P('gx'), may hold values from 0 to 7, never falling along the last dimension, each value on 1 to 512 neighbouring positions
- out_cotangent: bfloat16 [960, 8192], P('gx', 'gy'), may hold values from -6 to 6
Outputs:
- block_output: bfloat16 [960, 8192], P('gx', 'gy')
- input_grad: float32 [960, 8192], P('gx', 'gy')
- grad_attngain: float32 [960], P('gx')
- grad_query: float32 [960, 960], P('gx', 'gy')
- grad_key: float32 [960, 320], P('gx', 'gy')
- grad_value: float32 [960, 320], P('gx', 'gy')
- grad_outproj: float32 [960, 960], P('gy', 'gx')
- grad_ffngain: float32 [960], P('gx')
- grad_gate: float32 [960, 2560], P('gx', 'gy')
- grad_up: float32 [960, 2560], P('gx', 'gy')
- grad_down: float32 [2560, 960], P('gy', 'gx')
The draws below stay inside these ranges and needn't reach their ends.
Inputs may be any that keep to these rules, and one draw needn't show every extreme that they name: `segment_ids`: along each packed sequence the numbers never fall.
All inputs are finite; a program needn't handle non-finite values.
Results may differ from the reference program's by a relative error of at most 0.023.
The reference program's roundings to bfloat16 on the way count: a program that leaves them out, or rounds other values in their place, can miss the bound.
Values may be sent and summed in bfloat16 or wider, within the bound.
A program may use at most 256 MiB of HBM per device.

```python
import math
import jax
import jax.numpy as jnp
import numpy as np
from jax import lax

D = 960
QUERY_HEADS = 15
KEY_VALUE_HEADS = 5
HEAD_SIZE = 64
FF = 2560
PACKED_LENGTH = 1024
Q = 960
KV = 320
NSEQ = 8
TOKENS = 8192


def draw_query_weight(key, part):
    unrotated = jax.random.normal(jax.random.fold_in(key, 11), (D, Q), jnp.float32) / D ** 0.5
    return jnp.clip(unrotated, -2.0, 2.0).astype(jnp.bfloat16)


def draw_key_weight(key, part):
    unrotated = jax.random.normal(jax.random.fold_in(key, 13), (D, KV), jnp.float32) / D ** 0.5
    return jnp.clip(unrotated, -2.0, 2.0).astype(jnp.bfloat16)


def levels(rng, extent, pieces, least, high):
    def one(position, blocks):
        heights = jax.random.uniform(jax.random.fold_in(jax.random.fold_in(rng, 6), position), (blocks,), jnp.float32, least / len(pieces), high / len(pieces))
        return jnp.repeat(jnp.exp(heights), extent[position] // blocks).reshape((-1,) + (1,) * (len(extent) - position - 1))

    loudness = one(*pieces[0])
    for cut in pieces[1:]:
        loudness = loudness * one(*cut)
    return loudness


def split_up(number_of, total, bound, lean):
    portions = [(1 << 20) // math.isqrt(standing ** lean) + 1 for standing in range(2, number_of + 1)]
    rest, counts = total - bound - (number_of - 1), [1] * (number_of - 1)
    while rest > 0:
        movable = [i for i in range(number_of - 1) if counts[i] < bound]
        whole, budget = sum([portions[i] for i in movable]), rest
        for i in movable:
            addition = min(bound - counts[i], max(1, budget * portions[i] // whole), rest)
            counts[i] = counts[i] + addition
            rest = rest - addition
    return np.array([bound] + counts)


def uneven(key, number_of, total, bound, slope):
    if number_of == 2:
        one = jax.random.randint(key, (), max(1, total - bound), min(bound, total - 1) + 1)
        return jnp.stack([one, total - one])
    tallies = jnp.asarray(split_up(number_of, total, bound, slope), jnp.int32)
    couples = (number_of - 1) // 2
    source_of, taker = tallies[1:1 + 2 * couples:2], tallies[2:2 + 2 * couples:2]
    slack = jnp.minimum(source_of - 1, bound - taker)
    shifted = jax.random.randint(jax.random.fold_in(key, 1), (couples,), 0, 1 << 20) % (slack + 1)
    tallies = tallies.at[1:1 + 2 * couples:2].set(source_of - shifted).at[2:2 + 2 * couples:2].set(taker + shifted)
    return tallies[jax.random.permutation(jax.random.fold_in(key, 2), number_of)]


def centred(stream_key, dims, deviation, bound, pieces=(), kind=jnp.bfloat16):
    factor_of = levels(stream_key, dims, pieces, -0.22, 0.18) if pieces else 1.0
    result = jax.random.normal(stream_key, dims, jnp.float32) * deviation * factor_of
    return jnp.minimum(jnp.maximum(result, -bound), bound).astype(kind)


def setup_inputs(seed: int = 0) -> dict:
    seeds = jax.random.split(jax.random.key(seed), 13)
    block_input = centred(seeds[0], (D, TOKENS), 1.0, 6.0, ((0, 8), (1, 4)))
    attn_gain = jnp.clip(1.0 + 0.1 * jax.random.normal(seeds[1], (D,), jnp.float32), 0.5, 1.5)
    query_weight = draw_query_weight(jax.random.fold_in(seeds[12], 71), 0)
    key_weight = draw_key_weight(jax.random.fold_in(seeds[12], 71), 0)
    value_weight = centred(seeds[4], (D, KV), D ** -0.5, 0.1875, ((0, 8), (1, 4)))
    output_weight = centred(seeds[5], (Q, D), (Q // 8) ** -0.5, 0.5, ((0, 4), (1, 8)))
    ffn_gain = jnp.clip(1.0 + 0.1 * jax.random.normal(seeds[6], (D,), jnp.float32), 0.5, 1.5)
    gate_weight = centred(seeds[7], (D, FF), D ** -0.5, 0.1875, ((0, 8), (1, 4)))
    up_weight = centred(seeds[8], (D, FF), D ** -0.5, 0.1875, ((0, 8), (1, 4)))
    down_weight = centred(seeds[9], (FF, D), FF ** -0.5, 0.125, ((0, 4), (1, 8)))
    segment_ids = jax.vmap(lambda own: jnp.searchsorted(jnp.cumsum(uneven(own, 8, PACKED_LENGTH, PACKED_LENGTH // 2, 2)), jnp.arange(PACKED_LENGTH), side="right"))(jax.random.split(seeds[10], NSEQ)).reshape((NSEQ, PACKED_LENGTH)).astype(jnp.int32)
    out_cotangent = centred(seeds[11], (D, TOKENS), 1.0, 6.0, ((0, 8), (1, 4)))
    return dict(block_input=block_input, attn_gain=attn_gain, query_weight=query_weight, key_weight=key_weight, value_weight=value_weight, output_weight=output_weight, ffn_gain=ffn_gain, gate_weight=gate_weight, up_weight=up_weight, down_weight=down_weight, segment_ids=segment_ids, out_cotangent=out_cotangent)


EPS = 1e-05
THETA = 10000.0

def product(left, right):
    return jnp.dot(left.astype(jnp.float32), right.astype(jnp.float32), preferred_element_type=jnp.float32, precision=lax.Precision.HIGHEST)

def segment_positions(segments):
    row_index = jnp.broadcast_to(jnp.arange(segments.shape[1], dtype=jnp.int32)[None, :], segments.shape)
    starts = jnp.concatenate([jnp.ones((segments.shape[0], 1), dtype=jnp.bool_), segments[:, 1:] != segments[:, :-1]], axis=1)
    seg_first = lax.cummax(jnp.where(starts, row_index, jnp.zeros_like(row_index)), axis=1)
    return row_index - seg_first

def rope_tables(positions, half_dim):
    frequency = jnp.exp(-math.log(THETA) * jnp.arange(half_dim, dtype=jnp.float32) / half_dim)
    angles = positions.astype(jnp.float32)[:, None] * frequency[None, :]
    return (jnp.cos(angles)[:, None, :], jnp.sin(angles)[:, None, :])

def rotate(values, cos_table, sine_table, rotate_direction):
    n_rows = values.shape[0]
    half_dim = cos_table.shape[-1]
    split_heads = values.reshape(n_rows, -1, 2 * half_dim)
    lower_half = split_heads[..., :half_dim]
    upper_half = split_heads[..., half_dim:]
    new_lower = lower_half * cos_table - rotate_direction * upper_half * sine_table
    new_upper = upper_half * cos_table + rotate_direction * lower_half * sine_table
    return jnp.concatenate([new_lower, new_upper], axis=-1).reshape(n_rows, -1)

def seq_mask(segments):
    key_index = jnp.arange(segments.shape[0], dtype=jnp.int32)
    causal = key_index[None, :] <= key_index[:, None]
    return causal & (segments[:, None] == segments[None, :])

def seq_scores(query_per_head, key_per_head, allowed):
    scores = jnp.einsum('qkgd,ckd->kgqc', query_per_head.astype(jnp.float32), key_per_head.astype(jnp.float32), precision=lax.Precision.HIGHEST) * HEAD_SIZE ** (-0.5)
    return jnp.where(allowed[None, None], scores, -jnp.inf)

def seq_forward(inputs):
    query_sequence, key_sequence, value_sequence, segments = inputs
    allowed = seq_mask(segments)
    query_per_head = query_sequence.reshape(PACKED_LENGTH, KEY_VALUE_HEADS, QUERY_HEADS // KEY_VALUE_HEADS, HEAD_SIZE)
    key_per_head = key_sequence.reshape(PACKED_LENGTH, KEY_VALUE_HEADS, HEAD_SIZE)
    value_per_head = value_sequence.reshape(PACKED_LENGTH, KEY_VALUE_HEADS, HEAD_SIZE)
    scores = seq_scores(query_per_head, key_per_head, allowed)
    row_top = lax.optimization_barrier(jnp.max(scores, axis=-1, keepdims=True))
    log_total = row_top + jnp.log(lax.optimization_barrier(jnp.sum(jnp.exp(scores - row_top), axis=-1, keepdims=True)))
    prob_half = lax.optimization_barrier(jnp.exp(scores - log_total).astype(jnp.bfloat16)).astype(jnp.float32)
    mixed = jnp.einsum('kgqc,ckd->qkgd', prob_half, value_per_head.astype(jnp.float32), precision=lax.Precision.HIGHEST)
    return (mixed.reshape(PACKED_LENGTH, -1).astype(jnp.bfloat16), log_total)

def seq_backward(inputs):
    query_sequence, key_sequence, value_sequence, segments, sequence_gradient, log_total = inputs
    allowed = seq_mask(segments)
    query_per_head = query_sequence.reshape(PACKED_LENGTH, KEY_VALUE_HEADS, QUERY_HEADS // KEY_VALUE_HEADS, HEAD_SIZE)
    key_per_head = key_sequence.reshape(PACKED_LENGTH, KEY_VALUE_HEADS, HEAD_SIZE)
    value_per_head = value_sequence.reshape(PACKED_LENGTH, KEY_VALUE_HEADS, HEAD_SIZE).astype(jnp.float32)
    head_gradient = sequence_gradient.reshape(PACKED_LENGTH, KEY_VALUE_HEADS, QUERY_HEADS // KEY_VALUE_HEADS, HEAD_SIZE).astype(jnp.float32)
    scores = seq_scores(query_per_head, key_per_head, allowed)
    prob_full = jnp.exp(scores - log_total)
    prob_half = lax.optimization_barrier(prob_full.astype(jnp.bfloat16)).astype(jnp.float32)
    prob_grad = jnp.einsum('qkgd,ckd->kgqc', head_gradient, value_per_head, precision=lax.Precision.HIGHEST)
    row_dot = lax.optimization_barrier(jnp.sum(prob_full * prob_grad, axis=-1, keepdims=True))
    score_grad = lax.optimization_barrier((prob_full * (prob_grad - row_dot) * HEAD_SIZE ** (-0.5)).astype(jnp.bfloat16)).astype(jnp.float32)
    query_grad = jnp.einsum('kgqc,ckd->qkgd', score_grad, key_per_head.astype(jnp.float32), precision=lax.Precision.HIGHEST).reshape(PACKED_LENGTH, -1)
    key_grad = jnp.einsum('kgqc,qkgd->ckd', score_grad, query_per_head.astype(jnp.float32), precision=lax.Precision.HIGHEST).reshape(PACKED_LENGTH, -1)
    value_grad = jnp.einsum('kgqc,qkgd->ckd', prob_half, head_gradient, precision=lax.Precision.HIGHEST).reshape(PACKED_LENGTH, -1)
    return (query_grad, key_grad, value_grad)

def reference(block_input, attn_gain, query_weight, key_weight, value_weight, output_weight, ffn_gain, gate_weight, up_weight, down_weight, segment_ids, out_cotangent):
    resid_in = block_input.T.astype(jnp.float32)
    cot_rows = out_cotangent.T
    scale_one = lax.rsqrt(lax.optimization_barrier(jnp.mean(resid_in * resid_in, axis=1)) + EPS)
    normed_one = (resid_in * scale_one[:, None] * attn_gain[None, :]).astype(jnp.bfloat16)
    query_raw = product(normed_one, query_weight).astype(jnp.bfloat16)
    key_raw = product(normed_one, key_weight).astype(jnp.bfloat16)
    value_rows = product(normed_one, value_weight).astype(jnp.bfloat16)
    positions = segment_positions(segment_ids).reshape(-1)
    cos_table, sine_table = rope_tables(positions, HEAD_SIZE // 2)
    query_rotated = rotate(query_raw.astype(jnp.float32), cos_table, sine_table, 1.0).astype(jnp.bfloat16)
    key_rotated = rotate(key_raw.astype(jnp.float32), cos_table, sine_table, 1.0).astype(jnp.bfloat16)
    query_seqs = query_rotated.reshape(NSEQ, PACKED_LENGTH, -1)
    key_seqs = key_rotated.reshape(NSEQ, PACKED_LENGTH, -1)
    value_seqs = value_rows.reshape(NSEQ, PACKED_LENGTH, -1)
    attn_seqs, log_totals = lax.map(seq_forward, (query_seqs, key_seqs, value_seqs, segment_ids))
    attn_rows = attn_seqs.reshape(TOKENS, -1)
    hidden_in = resid_in + product(attn_rows, output_weight)
    scale_two = lax.rsqrt(lax.optimization_barrier(jnp.mean(hidden_in * hidden_in, axis=1)) + EPS)
    normed_two = (hidden_in * scale_two[:, None] * ffn_gain[None, :]).astype(jnp.bfloat16)
    gate_pre = product(normed_two, gate_weight)
    up_pre = product(normed_two, up_weight)
    hidden = (jax.nn.silu(gate_pre) * up_pre).astype(jnp.bfloat16)
    block_output = (hidden_in + product(hidden, down_weight)).astype(jnp.bfloat16)
    grad_down = product(hidden.T, cot_rows)
    hidden_grad = product(cot_rows, down_weight.T)
    gate_sigmoid = jax.nn.sigmoid(gate_pre)
    gate_back = (hidden_grad * up_pre * gate_sigmoid * (1.0 + gate_pre * (1.0 - gate_sigmoid))).astype(jnp.bfloat16)
    up_back = (hidden_grad * gate_pre * gate_sigmoid).astype(jnp.bfloat16)
    grad_gate = product(normed_two.T, gate_back)
    grad_up = product(normed_two.T, up_back)
    normed_two_grad = product(gate_back, gate_weight.T) + product(up_back, up_weight.T)
    weighted_two = normed_two_grad * ffn_gain[None, :]
    grad_ffngain = lax.optimization_barrier(jnp.sum(normed_two_grad * hidden_in * scale_two[:, None], axis=0))
    inner_two = lax.optimization_barrier(jnp.mean(weighted_two * hidden_in, axis=1))
    hidden_in_grad = cot_rows.astype(jnp.float32) + scale_two[:, None] * weighted_two - hidden_in * (scale_two * scale_two * scale_two * inner_two)[:, None]
    hidden_in_half = hidden_in_grad.astype(jnp.bfloat16)
    grad_outproj = product(attn_rows.T, hidden_in_half)
    attn_grad = product(hidden_in_half, output_weight.T).astype(jnp.bfloat16)
    query_grad, key_grad, value_grad = lax.map(seq_backward, (query_seqs, key_seqs, value_seqs, segment_ids, attn_grad.reshape(NSEQ, PACKED_LENGTH, -1), log_totals))
    query_back = rotate(query_grad.reshape(TOKENS, -1), cos_table, sine_table, -1.0).astype(jnp.bfloat16)
    key_back = rotate(key_grad.reshape(TOKENS, -1), cos_table, sine_table, -1.0).astype(jnp.bfloat16)
    value_back = value_grad.reshape(TOKENS, -1).astype(jnp.bfloat16)
    grad_query = product(normed_one.T, query_back)
    grad_key = product(normed_one.T, key_back)
    grad_value = product(normed_one.T, value_back)
    normed_one_grad = product(query_back, query_weight.T) + product(key_back, key_weight.T) + product(value_back, value_weight.T)
    weighted_one = normed_one_grad * attn_gain[None, :]
    grad_attngain = lax.optimization_barrier(jnp.sum(normed_one_grad * resid_in * scale_one[:, None], axis=0))
    inner_one = lax.optimization_barrier(jnp.mean(weighted_one * resid_in, axis=1))
    input_grad = hidden_in_grad + scale_one[:, None] * weighted_one - resid_in * (scale_one * scale_one * scale_one * inner_one)[:, None]
    return (block_output.T, input_grad.T, grad_attngain, grad_query, grad_key, grad_value, grad_outproj, grad_ffngain, grad_gate, grad_up, grad_down)
```

```python
import functools
import math

import jax
import jax.numpy as jnp
from jax import lax
from jax.experimental import pallas as pl
from jax.experimental.pallas import tpu as pltpu
from jax.sharding import PartitionSpec as P

QUERY_HEADS = 15
KEY_VALUE_HEADS = 5
HEAD_SIZE = 64
PACKED_LENGTH = 1024
LONGEST_SEGMENT = 512

EPS = 1e-05
THETA = 10000.0
MESH = pl.DeviceIdType.MESH
F32 = jnp.float32
BF16 = jnp.bfloat16


class Grid:
    def __init__(self, gx, gy):
        self.gx, self.gy = gx, gy
        self.C = 2 if gy % 2 == 0 else 1
        self.X = gy // self.C
        self.Y = self.X if gx % self.X == 0 else 1
        self.Z = gx // self.Y
        self.size = {"z": self.Z, "y": self.Y, "x": self.X}

    def here(self):
        i, j = lax.axis_index("gx"), lax.axis_index("gy")
        return {"z": i // self.Y, "y": i % self.Y, "x": j // self.C, "c": j % self.C}

    def device(self, at):
        return (at["z"] * self.Y + at["y"], at["x"] * self.C + at["c"])


def when(condition, body):
    if condition is None:
        body()
    else:
        pl.when(condition)(body)


def remote(src, dst, send, recv, device):
    return pltpu.make_async_remote_copy(
        src_ref=src, dst_ref=dst, send_sem=send, recv_sem=recv, device_id=device, device_id_type=MESH
    )


def greet(devices):
    barrier = pltpu.get_barrier_semaphore()
    for condition, device in devices:

        def signal(device=device):
            pl.semaphore_signal(barrier, inc=1, device_id=device, device_id_type=MESH)

        when(condition, signal)
    count = sum(1 for condition, _ in devices if condition is None)
    for condition, _ in devices:
        if condition is not None:
            count = count + condition.astype(jnp.int32)
    pl.semaphore_wait(barrier, count)


def row_peers(n, me):
    return [(d, lax.rem(me + d, n)) for d in range(1, n)]


def gather_kernel(grid, tok, cw, pairs, x_ref, dy_ref, small_ref, w_ref, xo, dyo, smallo, wo, x_s, x_r, x_l, w_s, w_r, w_l):
    me = grid.here()
    i, j = lax.axis_index("gx"), lax.axis_index("gy")
    peers = row_peers(grid.gx, i)
    greet([(None, (p, j)) for _, p in peers] + [
        (c, d) for (c, d) in along(grid, me, "x")
    ] + ([(None, grid.device({**me, "c": 1 - me["c"]}))] if grid.C == 2 else []))

    locals_ = []

    def local(src, dst, n):
        copy = pltpu.make_async_copy(src, dst, n)
        copy.start()
        locals_.append(copy)

    def tokens(ref, p):
        return ref.at[:, pl.ds(pl.multiple_of(p * tok, tok), tok)]

    exchanged = []
    for d, p in peers:
        back = lax.rem(i + grid.gx - d, grid.gx)
        for n, (src, dst) in enumerate(
            ((tokens(x_ref, p), xo.at[i]), (tokens(dy_ref, p), dyo.at[i]), (small_ref, smallo.at[i]))
        ):
            copy = remote(src, dst, x_s.at[n, d - 1], x_r.at[n, d - 1], (p, j))
            copy.start()
            land = (xo, dyo, smallo)[n].at[back]
            exchanged.append((copy, remote(land, land, x_s.at[n, d - 1], x_r.at[n, d - 1], (p, j))))
    local(tokens(x_ref, i), xo.at[i], x_l.at[0])
    local(tokens(dy_ref, i), dyo.at[i], x_l.at[1])
    local(small_ref, smallo.at[i], x_l.at[2])
    local(w_ref, wo.at[j, i], w_l.at[0])

    spread(grid, me, cw, pairs, w_ref, wo, w_s, w_r)

    for copy, arrival in exchanged:
        arrival.wait_recv()
        copy.wait_send()
    for copy in locals_:
        copy.wait()


def along(grid, me, axis):
    n = grid.size[axis]
    if n == 1:
        return []
    if n == 2:
        return [(None, grid.device({**me, axis: 1 - me[axis]}))]
    return [
        (me[axis] > 0, grid.device({**me, axis: me[axis] - 1})),
        (me[axis] < n - 1, grid.device({**me, axis: me[axis] + 1})),
    ]


def order_of(here, n):
    if n & (n - 1):
        return [lax.rem(here + k, n) for k in range(n)]
    places = []
    for k in range(n):
        place, bit = 0, 1
        while bit < n:
            digit = (here // bit) % 2
            place = place + bit * ((1 - digit) if k & bit else digit)
            bit *= 2
        places.append(place)
    return places


def gather_sites(grid, me, order):
    other = [(None, grid.device({**me, "c": 1 - me["c"]}))] if grid.C == 2 else []
    onward = [along(grid, me, axis) for axis in order]
    yield 0, None, dict(me), sum(onward, []) + other
    for stage, axis in enumerate(order, 1):
        n = grid.size[axis]
        earlier = [dict(me)]
        for done in order[: stage - 1]:
            earlier = [{**e, done: place} for place in order_of(me[done], grid.size[done]) for e in earlier]
        later = sum(onward[stage:], []) + other
        for distance in range(1, n):
            if n == 2:
                for e in earlier:
                    yield stage, None, {**e, axis: 1 - me[axis]}, later
                continue
            for sign in (-1, 1):
                origin = me[axis] + sign * distance
                exists = origin >= 0 if sign < 0 else origin <= n - 1
                further = me[axis] - sign
                room = further <= n - 1 if sign < 0 else further >= 0
                ahead = [(room, grid.device({**me, axis: further}))]
                if distance == n - 1:
                    ahead = []
                for e in earlier:
                    yield stage, exists, {**e, axis: origin}, ahead + later


def core_sites(grid, me):
    found = [{"c": 1 - me["c"]}]
    for axis in "xyz":
        found = [{**f, axis: place} for place in order_of(me[axis], grid.size[axis]) for f in found]
    return found


ORDERS = ("zyx", "zxy")


def count_sends(grid):
    me = {"z": 0, "y": 0, "x": 0, "c": 0}
    return sum(len(sends) for order in ORDERS for _, _, _, sends in gather_sites(grid, me, order))


def spread(grid, me, cw, pairs, w_ref, wo, w_s, w_r):
    def columns(pair, lane):
        return pl.ds(pl.multiple_of((2 * pair + lane) * cw, cw), cw)

    streams = [list(gather_sites(grid, me, order)) for order in ORDERS]

    def step(stage, pair, finish):
        number = 0
        for lane, sites in enumerate(streams):
            for at, exists, piece, sends in sites:
                first = number
                number += len(sends)
                if at != stage:
                    continue
                pj, pi = piece["x"] * grid.C + piece["c"], piece["z"] * grid.Y + piece["y"]
                land = wo.at[pj, pi, :, columns(pair, lane)]
                src = w_ref.at[:, columns(pair, lane)] if at == 0 else land

                def body(at=at, lane=lane, pi=pi, pj=pj, land=land, src=src, sends=sends, first=first):
                    if at and not finish:
                        remote(land, land, w_s.at[first, pair], w_r.at[pj, pi, 2 * pair + lane], (0, 0)).wait_recv()
                    for n, (condition, device) in enumerate(sends):
                        copy = remote(src, land, w_s.at[first + n, pair], w_r.at[pj, pi, 2 * pair + lane], device)
                        when(condition, copy.wait_send if finish else copy.start)

                when(exists, body)

    for pair in range(pairs):
        step(0, pair, False)

    def slot(t, carry):
        for stage in (1, 2, 3):
            pair = t - (stage - 1)
            pl.when((pair >= 0) & (pair < pairs))(functools.partial(step, stage, pair, False))
        return carry

    lax.fori_loop(0, pairs + 2, slot, 0)

    def end(pair, carry):
        if grid.C == 2:
            for piece in core_sites(grid, me):
                pj, pi = piece["x"] * grid.C + piece["c"], piece["z"] * grid.Y + piece["y"]
                for lane in range(2):
                    land = wo.at[pj, pi, :, columns(pair, lane)]
                    remote(land, land, w_s.at[0, pair], w_r.at[pj, pi, 2 * pair + lane], (0, 0)).wait_recv()
        for stage in range(4):
            step(stage, pair, True)
        return carry

    lax.fori_loop(0, pairs, end, 0)


def gather(grid, tok, x, dy, small, w):
    rows, cols = w.shape
    cw, pairs = column_pairs(grid, cols)
    hbm = pl.BlockSpec(memory_space=pl.ANY)
    vmem = pl.BlockSpec(memory_space=pltpu.VMEM)
    return pl.pallas_call(
        functools.partial(gather_kernel, grid, tok, cw, pairs),
        out_shape=[
            jax.ShapeDtypeStruct((grid.gx, x.shape[0], tok), BF16),
            jax.ShapeDtypeStruct((grid.gx, x.shape[0], tok), BF16),
            jax.ShapeDtypeStruct((grid.gx,) + small.shape, F32),
            jax.ShapeDtypeStruct((grid.gy, grid.gx, rows, cols), BF16),
        ],
        in_specs=[vmem] * 4,
        out_specs=[hbm] * 4,
        scratch_shapes=[
            pltpu.SemaphoreType.DMA((3, grid.gx - 1)),
            pltpu.SemaphoreType.DMA((3, grid.gx - 1)),
            pltpu.SemaphoreType.DMA((3,)),
            pltpu.SemaphoreType.DMA((count_sends(grid), pairs)),
            pltpu.SemaphoreType.DMA((grid.gy, grid.gx, 2 * pairs)),
            pltpu.SemaphoreType.DMA((1,)),
        ],
        compiler_params=pltpu.CompilerParams(collective_id=0, has_side_effects=True),
        name="gather",
    )(x, dy, small, w)


def column_pairs(grid, cols):
    most = max(1, 160 // (grid.gx * grid.gy))
    pairs = max(p for p in range(1, most + 1) if (cols // 128) % (2 * p) == 0)
    return cols // (2 * pairs), pairs


def shift_kernel(grid, span, sign, a_ref, o_ref, send, recv):
    i, j = lax.axis_index("gx"), lax.axis_index("gy")
    base, q = i // span * span, i % span
    n = o_ref.shape[0]
    barrier = pltpu.get_barrier_semaphore()
    for d in range(1, span):
        pl.semaphore_signal(barrier, inc=1, device_id=(base + lax.rem(q + d, span), j), device_id_type=MESH)
    pl.semaphore_wait(barrier, span - 1)
    copies = []
    for d in range(1, n + 1):
        to = base + lax.rem(q + (sign * d) % span, span)
        src = a_ref if a_ref.ndim == 2 else a_ref.at[d - 1]
        copy = remote(src, o_ref.at[d - 1], send.at[d - 1], recv.at[d - 1], (to, j))
        copy.start()
        copies.append(copy)
    for copy in copies:
        copy.wait()


def shift(grid, span, sign, n, a, collective_id):
    vmem = pl.BlockSpec(memory_space=pltpu.VMEM)
    return pl.pallas_call(
        functools.partial(shift_kernel, grid, span, sign),
        out_shape=jax.ShapeDtypeStruct((n,) + a.shape[-2:], a.dtype),
        in_specs=[vmem],
        out_specs=vmem,
        scratch_shapes=[pltpu.SemaphoreType.DMA((n,)), pltpu.SemaphoreType.DMA((n,))],
        compiler_params=pltpu.CompilerParams(collective_id=collective_id, has_side_effects=True),
        name="shift",
    )(a)


def slots_of(n):
    return 1 if n == 2 else max(1, 2 * (n - 1))


def over(ref, body):
    lead = ref.shape[:-2]
    total = math.prod(lead)

    def one(k, carry):
        place = []
        for n in reversed(lead):
            place.append(k % n)
            k = k // n
        body(tuple(reversed(place)))
        return carry

    if total == 1:
        body((0,) * len(lead))
    else:
        lax.fori_loop(0, total, one, 0)


def add_into(target, source):
    def one(place):
        where = place + (slice(None), slice(None))
        target[where] = (target[where].astype(F32) + source[where].astype(F32)).astype(BF16)

    over(target, one)


def reduce_line(n, p, device, pick, land, send, recv, s, waits):
    if n == 1:
        return []

    def arrive(slot):
        where = land(slot)
        remote(where, where, send.at[slot, s], recv.at[slot, s], device(p)).wait_recv()

    if n == 2:
        copy = remote(pick(1 - p), land(0), send.at[0, s], recv.at[0, s], device(1 - p))
        copy.start()
        waits.append((None, copy.wait_send))
        return [(None, 0, arrive)]
    for t in range(n - 1, 0, -1):
        copy = remote(pick(t), land(t - 1), send.at[t - 1, s], recv.at[t - 1, s], device(p + 1))

        def up(t=t, copy=copy):
            def pass_on():
                arrive(t - 1)
                add_into(pick(t), land(t - 1))

            pl.when(p > 0)(pass_on)
            copy.start()

        pl.when(p < t)(up)
        waits.append((p < t, copy.wait_send))
    for t in range(n - 1):
        slot = n - 1 + t
        copy = remote(pick(t), land(slot), send.at[slot, s], recv.at[slot, s], device(p - 1))

        def down(t=t, copy=copy, slot=slot):
            def pass_on():
                arrive(slot)
                add_into(pick(t), land(slot))

            pl.when(p < n - 1)(pass_on)
            copy.start()

        pl.when(p > t)(down)
        waits.append((p > t, copy.wait_send))
    return [(p == t, t - 1, arrive) for t in range(1, n)] + [(p == t, n - 1 + t, arrive) for t in range(n - 1)]


def reduce_kernel(
    grid, tok, cw, pairs, g_ref, bo_ref, ig_ref, gain_ref,
    bo, ig, go, gaino,
    acc, from_core, first_a, first_b, second_a, second_b, from_z, gain_in, gain_row, gain_across,
    o_s, o_r, o_l, c_s, c_r, c_l, f_s, f_r, n_s, n_r, z_s, z_r, g_s, g_r, h_s, h_r,
):
    me = grid.here()
    i, j = lax.axis_index("gx"), lax.axis_index("gy")
    X, Y, Z, C = grid.X, grid.Y, grid.Z, grid.C
    peers = row_peers(grid.gx, i)
    across = row_peers(grid.gy, j)
    greet([(None, (p, j)) for _, p in peers] + [(None, (i, p)) for _, p in across])

    def columns(s):
        return pl.ds(s * cw, cw)

    def half(s):
        return pl.ds(s // 2 * cw, cw)

    streams = 2 * pairs
    waits = []
    other = grid.device({**me, "c": 1 - me["c"]})
    core = {}
    for s in range(streams):
        for x in range(X):
            if C == 2:
                src = g_ref.at[x * C + 1 - me["c"], :, :, :, columns(s)]
                copy = remote(src, from_core.at[x, :, :, :, columns(s)], c_s.at[x, s], c_r.at[x, s], other)
                copy.start()
                waits.append((None, copy.wait_send))
                core[x, s] = copy
            own = pltpu.make_async_copy(
                g_ref.at[x * C + me["c"], :, :, :, columns(s)], acc.at[x, :, :, :, columns(s)], c_l.at[x, s]
            )
            own.start()
            core[x, s, "own"] = own

    def tokens(ref, p):
        return ref.at[:, pl.ds(pl.multiple_of(p * tok, tok), tok)]

    arrivals = []
    for d, p in peers:
        back = lax.rem(i + grid.gx - d, grid.gx)
        for n, (src, dst) in enumerate(((bo_ref, bo), (ig_ref, ig))):
            copy = remote(src.at[p], tokens(dst, i), o_s.at[n, d - 1], o_r.at[n, d - 1], (p, j))
            copy.start()
            waits.append((None, copy.wait_send))
            land = tokens(dst, back)
            arrivals.append(remote(land, land, o_s.at[n, d - 1], o_r.at[n, d - 1], (p, j)))
        copy = remote(gain_ref.at[p], gain_in.at[d - 1], g_s.at[d - 1], g_r.at[d - 1], (p, j))
        copy.start()
        waits.append((None, copy.wait))
    for n, (src, dst) in enumerate(((bo_ref, bo), (ig_ref, ig))):
        copy = pltpu.make_async_copy(src.at[i], tokens(dst, i), o_l.at[n])
        copy.start()
        waits.append((None, copy.wait))

    def stage_core(s):
        for x in range(X):
            core[x, s, "own"].wait()
            if C == 2:
                core[x, s].wait_recv()
                add_into(acc.at[x, :, :, :, columns(s)], from_core.at[x, :, :, :, columns(s)])

    def picks(s):
        if s % 2 == 0:
            return (
                ("x", lambda t: acc.at[t, :, :, :, columns(s)], lambda k: first_a.at[k, :, :, :, half(s)], f_s, f_r),
                ("y", lambda t: acc.at[me["x"], :, t, :, columns(s)], lambda k: second_a.at[k, :, :, half(s)], n_s, n_r),
            )
        return (
            ("y", lambda t: acc.at[:, :, t, :, columns(s)], lambda k: first_b.at[k, :, :, :, half(s)], f_s, f_r),
            ("x", lambda t: acc.at[t, :, me["y"], :, columns(s)], lambda k: second_b.at[k, :, :, half(s)], n_s, n_r),
        )

    due = {}

    def begin(level, s):
        axis, pick, land, send, recv = picks(s)[level]
        due[level, s] = reduce_line(
            grid.size[axis], me[axis], lambda place: grid.device({**me, axis: place}), pick, land, send, recv, s, waits
        )

    def finish(level, s):
        axis, pick, land, _, _ = picks(s)[level]
        for condition, slot, arrive in due[level, s]:

            def take(slot=slot, arrive=arrive):
                arrive(slot)
                add_into(pick(me[axis]), land(slot))

            when(condition, take)

    def z_line(s):
        def pick(t):
            return acc.at[me["x"], t, me["y"], :, columns(s)]

        def land(slot):
            return from_z.at[slot, :, columns(s)]

        rest = reduce_line(Z, me["z"], lambda place: grid.device({**me, "z": place}), pick, land, z_s, z_r, s, waits)
        go[:, columns(s)] = acc[me["x"], me["z"], me["y"], :, columns(s)].astype(F32)
        for condition, slot, arrive in rest:

            def take(slot=slot, arrive=arrive):
                arrive(slot)
                go[:, columns(s)] += from_z[slot, :, columns(s)].astype(F32)

            when(condition, take)

    for t in range(streams + 6):
        if t < streams:
            stage_core(t)
            begin(0, t)
        if 0 <= t - 2 < streams:
            finish(0, t - 2)
            begin(1, t - 2)
        if 0 <= t - 4 < streams:
            finish(1, t - 4)
            z_line(t - 4)

    for condition, wait in waits:
        when(condition, wait)
    gain_row[...] = gain_ref[i]
    for d, _ in peers:
        gain_row[...] += gain_in[d - 1]
    last = []
    for d, p in across:
        copy = remote(gain_row, gain_across.at[d - 1], h_s.at[d - 1], h_r.at[d - 1], (i, p))
        copy.start()
        last.append(copy)
    for arrival in arrivals:
        arrival.wait_recv()
    gaino[...] = gain_row[...]
    for (d, _), copy in zip(across, last):
        copy.wait()
        gaino[...] += gain_across[d - 1]


def reduce(grid, tok, g, bo, ig, gain, collective_id):
    rows, cols = g.shape[-2:]
    width = bo.shape[1]
    cw, pairs = column_pairs(grid, cols)
    X, Y, Z, S = grid.X, grid.Y, grid.Z, 2 * pairs
    hbm = pl.BlockSpec(memory_space=pl.ANY)
    vmem = pl.BlockSpec(memory_space=pltpu.VMEM)
    sem = pltpu.SemaphoreType.DMA
    slots = max(slots_of(X), slots_of(Y))
    return pl.pallas_call(
        functools.partial(reduce_kernel, grid, tok, cw, pairs),
        out_shape=[
            jax.ShapeDtypeStruct((width, grid.gx * tok), BF16),
            jax.ShapeDtypeStruct((width, grid.gx * tok), BF16),
            jax.ShapeDtypeStruct((rows, cols), F32),
            jax.ShapeDtypeStruct((8, 128), F32),
        ],
        in_specs=[hbm] + [vmem] * 3,
        out_specs=[vmem] * 4,
        scratch_shapes=[
            pltpu.VMEM((X, Z, Y, rows, cols), BF16),
            pltpu.VMEM((X, Z, Y, rows, cols), BF16),
            pltpu.VMEM((slots_of(X), Z, Y, rows, cols // 2), BF16),
            pltpu.VMEM((slots_of(Y), X, Z, rows, cols // 2), BF16),
            pltpu.VMEM((slots_of(Y), Z, rows, cols // 2), BF16),
            pltpu.VMEM((slots_of(X), Z, rows, cols // 2), BF16),
            pltpu.VMEM((slots_of(Z), rows, cols), BF16),
            pltpu.VMEM((grid.gx - 1, 8, 128), F32),
            pltpu.VMEM((8, 128), F32),
            pltpu.VMEM((grid.gy - 1, 8, 128), F32),
            sem((2, grid.gx - 1)),
            sem((2, grid.gx - 1)),
            sem((2,)),
            sem((X, S)),
            sem((X, S)),
            sem((X, S)),
            sem((slots, S)),
            sem((slots, S)),
            sem((slots, S)),
            sem((slots, S)),
            sem((slots_of(Z), S)),
            sem((slots_of(Z), S)),
            sem((grid.gx - 1,)),
            sem((grid.gx - 1,)),
            sem((grid.gy - 1,)),
            sem((grid.gy - 1,)),
        ],
        compiler_params=pltpu.CompilerParams(
            collective_id=collective_id, has_side_effects=True, vmem_limit_bytes=60 * 1024 * 1024
        ),
        name="reduce",
    )(g.reshape(grid.gy, Z, Y, rows, cols), bo, ig, gain)


def rotate(values, cos_table, sine_table, direction):
    half = HEAD_SIZE // 2
    lower, upper = values[..., :half], values[..., half:]
    return jnp.concatenate(
        [lower * cos_table - direction * upper * sine_table, upper * cos_table + direction * lower * sine_table], axis=-1
    )


def einsum(form, a, b):
    return jnp.einsum(form, a, b, preferred_element_type=F32)


def padded(a, axis, size):
    pads = [(0, 0)] * a.ndim
    pads[axis] = (0, size - a.shape[axis])
    return jnp.pad(a, pads) if size != a.shape[axis] else a


def norm_backward(values, scale, gain, grad):
    weighted = grad * gain[:, None]
    inner = jnp.sum(weighted * values, axis=0) / values.shape[0]
    back = scale * weighted - values * (scale * scale * scale * inner)
    return back, jnp.sum(grad * values * scale, axis=1)


def shards(
    grid,
    block_input,
    attn_gain,
    query_weight,
    key_weight,
    value_weight,
    output_weight,
    ffn_gain,
    gate_weight,
    up_weight,
    down_weight,
    segment_ids,
    out_cotangent,
):
    GX, GY = grid.gx, grid.gy
    rows, row_tokens = block_input.shape
    tok = row_tokens // GX
    features = rows * GX
    span = PACKED_LENGTH // tok
    before = -(-(LONGEST_SEGMENT - 1) // tok)
    qc, kc, fc = query_weight.shape[1], key_weight.shape[1], gate_weight.shape[1]
    heads, kv_heads = qc * GY // HEAD_SIZE, kc * GY // HEAD_SIZE
    groups = heads // kv_heads
    i, j = lax.axis_index("gx"), lax.axis_index("gy")
    q = i % span

    block = jnp.concatenate(
        [query_weight, key_weight, value_weight, output_weight.T, gate_weight, up_weight, down_weight.T], axis=1
    )
    used = block.shape[1]
    block = padded(block, 1, -(-used // 256) * 256)
    segments_here = segment_ids.reshape(-1, 256).astype(F32)
    small = padded(
        jnp.concatenate([segments_here, padded(jnp.stack([attn_gain, ffn_gain]), 1, 256)], axis=0),
        0,
        -(-(segments_here.shape[0] + 2) // 8) * 8,
    )
    x_parts, dy_parts, small_all, weights = gather(grid, tok, block_input, out_cotangent, small, block)

    x = x_parts.reshape(features, tok).astype(F32)
    dy_half = dy_parts.reshape(features, tok)
    dy = dy_half.astype(F32)
    weights = weights.reshape(GY, features, -1)
    w_qkv = weights[:, :, : qc + 2 * kc]
    w_out = weights[:, :, qc + 2 * kc : 2 * (qc + kc)]
    at = 2 * (qc + kc)
    w_gate, w_up, w_down = (weights[:, :, at + k * fc : at + (k + 1) * fc] for k in range(3))
    n_seg = segments_here.shape[0]
    gain_one, gain_two = (small_all[:, n_seg + k, :rows].reshape(features) for k in range(2))

    sequence = j * (row_tokens // PACKED_LENGTH) + i // span
    segments = lax.dynamic_index_in_dim(small_all[:, :n_seg].reshape(GX, PACKED_LENGTH), sequence, 0, keepdims=False)
    window = (before + 1) * tok
    seg_window = lax.dynamic_slice_in_dim(
        jnp.concatenate([jnp.full((before * tok,), -1.0, F32), segments]), q * tok, window, 0
    )
    seg_query = seg_window[before * tok :]
    first = jnp.sum((segments[None, :] < seg_query[:, None]).astype(F32), axis=1)
    positions = (q * tok).astype(F32) + jnp.arange(tok, dtype=F32) - first
    half = HEAD_SIZE // 2
    frequency = jnp.exp(-math.log(THETA) * jnp.arange(half, dtype=F32) / half)
    angles = positions[:, None] * frequency[None, :]
    cos_table, sine_table = jnp.cos(angles)[:, None, :], jnp.sin(angles)[:, None, :]
    local = jnp.arange(window, dtype=jnp.int32)
    allowed = (seg_query[:, None] == seg_window[None, :]) & (local[None, :] <= local[before * tok :, None])

    scale_one = lax.rsqrt(jnp.mean(x * x, axis=0) + EPS)
    normed_one = (x * scale_one * gain_one[:, None]).astype(BF16)
    qkv = einsum("dt,jdc->jtc", normed_one, w_qkv).astype(BF16)

    def columns(part):
        return part.transpose(1, 0, 2).reshape(tok, -1, HEAD_SIZE)

    query = rotate(columns(qkv[:, :, :qc]).astype(F32), cos_table, sine_table, 1.0).astype(BF16)
    key = rotate(columns(qkv[:, :, qc : qc + kc]).astype(F32), cos_table, sine_table, 1.0).astype(BF16)
    value = columns(qkv[:, :, qc + kc :])
    key_value = jnp.concatenate([key.reshape(tok, -1), value.reshape(tok, -1)], axis=1)
    earlier = shift(grid, span, 1, before, key_value, 1)
    in_window = jnp.concatenate([earlier[::-1].reshape(before * tok, -1), key_value], axis=0)
    key_window = in_window[:, : key_value.shape[1] // 2].reshape(window, kv_heads, HEAD_SIZE)
    value_window = in_window[:, key_value.shape[1] // 2 :].reshape(window, kv_heads, HEAD_SIZE)
    query = query.reshape(tok, kv_heads, groups, HEAD_SIZE)
    scores = einsum("qkgd,ckd->kgqc", query, key_window) * HEAD_SIZE ** (-0.5)
    scores = jnp.where(allowed[None, None], scores, -jnp.inf)
    row_top = jnp.max(scores, axis=-1, keepdims=True)
    log_total = row_top + jnp.log(jnp.sum(jnp.exp(scores - row_top), axis=-1, keepdims=True))
    prob_full = jnp.exp(scores - log_total)
    prob_half = prob_full.astype(BF16)
    mixed = einsum("kgqc,ckd->qkgd", prob_half, value_window).astype(BF16).reshape(tok, GY, qc)
    hidden_in = x + einsum("jdc,tjc->dt", w_out, mixed)
    scale_two = lax.rsqrt(jnp.mean(hidden_in * hidden_in, axis=0) + EPS)
    normed_two = (hidden_in * scale_two * gain_two[:, None]).astype(BF16)
    gate = einsum("dt,jdf->jtf", normed_two, w_gate)
    up = einsum("dt,jdf->jtf", normed_two, w_up)
    sigmoid = jax.nn.sigmoid(gate)
    hidden = (jax.nn.silu(gate) * up).astype(BF16)
    block_output = (hidden_in + einsum("jdf,jtf->dt", w_down, hidden)).astype(BF16)

    hidden_grad = einsum("dt,jdf->jtf", dy_half, w_down)
    gate_back = (hidden_grad * up * sigmoid * (1.0 + gate * (1.0 - sigmoid))).astype(BF16)
    up_back = (hidden_grad * gate * sigmoid).astype(BF16)
    grad_down = einsum("dt,jtf->jdf", dy_half, hidden)
    grad_gate = einsum("dt,jtf->jdf", normed_two, gate_back)
    grad_up = einsum("dt,jtf->jdf", normed_two, up_back)
    normed_two_grad = einsum("jdf,jtf->dt", w_gate, gate_back) + einsum("jdf,jtf->dt", w_up, up_back)
    hidden_in_grad, gain_two_part = norm_backward(hidden_in, scale_two, gain_two, normed_two_grad)
    hidden_in_grad = hidden_in_grad + dy
    hidden_in_half = hidden_in_grad.astype(BF16)
    grad_out = einsum("dt,tjc->jdc", hidden_in_half, mixed)
    head_grad = einsum("dt,jdc->tjc", hidden_in_half, w_out).astype(BF16).reshape(tok, kv_heads, groups, HEAD_SIZE)
    prob_grad = einsum("qkgd,ckd->kgqc", head_grad, value_window)
    row_dot = jnp.sum(prob_full * prob_grad, axis=-1, keepdims=True)
    score_grad = (prob_full * (prob_grad - row_dot) * HEAD_SIZE ** (-0.5)).astype(BF16)
    query_grad = einsum("kgqc,ckd->qkgd", score_grad, key_window).reshape(tok, heads, HEAD_SIZE)
    key_grad = einsum("kgqc,qkgd->ckd", score_grad, query).reshape(window, -1)
    value_grad = einsum("kgqc,qkgd->ckd", prob_half, head_grad).reshape(window, -1)
    key_value_grad = jnp.concatenate([key_grad, value_grad], axis=1).reshape(before + 1, tok, -1)
    later = shift(grid, span, -1, before, key_value_grad[:before][::-1].astype(BF16), 2)
    key_value_grad = key_value_grad[before] + jnp.sum(later.astype(F32), axis=0)
    key_grad, value_grad = jnp.split(key_value_grad, 2, axis=1)
    query_back = rotate(query_grad, cos_table, sine_table, -1.0).astype(BF16).reshape(tok, GY, qc)
    key_back = rotate(key_grad.reshape(tok, -1, HEAD_SIZE), cos_table, sine_table, -1.0).astype(BF16).reshape(tok, GY, kc)
    qkv_back = jnp.concatenate([query_back, key_back, value_grad.astype(BF16).reshape(tok, GY, kc)], axis=2)
    grad_qkv = einsum("dt,tjc->jdc", normed_one, qkv_back)
    normed_one_grad = einsum("jdc,tjc->dt", w_qkv, qkv_back)
    input_grad, gain_one_part = norm_backward(x, scale_one, gain_one, normed_one_grad)
    input_grad = (input_grad + hidden_in_grad).astype(BF16)

    grads = jnp.concatenate([g.astype(BF16) for g in (grad_qkv, grad_out, grad_gate, grad_up, grad_down)], axis=2)
    grads = padded(grads, 2, block.shape[1]).reshape(GY, GX, rows, -1)
    gains = padded(padded(jnp.stack([gain_one_part, gain_two_part]).reshape(2, GX, rows).transpose(1, 0, 2), 1, 8), 2, 128)
    block_output, input_grad, grads, gains = reduce(
        grid, tok, grads, block_output.reshape(GX, rows, tok), input_grad.reshape(GX, rows, tok), gains, 3
    )
    grad_query, grad_key, grad_value, grad_out, grad_gate, grad_up, grad_down = jnp.split(
        grads[:, :used], [qc, qc + kc, qc + 2 * kc, at, at + fc, at + 2 * fc], axis=1
    )
    return (
        block_output,
        input_grad.astype(F32),
        gains[0, :rows],
        grad_query,
        grad_key,
        grad_value,
        grad_out.T,
        gains[1, :rows],
        grad_gate,
        grad_up,
        grad_down.T,
    )


def solution(mesh):
    grid = Grid(mesh.shape["gx"], mesh.shape["gy"])
    return jax.shard_map(
        functools.partial(shards, grid),
        mesh=mesh,
        in_specs=(
            P("gx", "gy"),
            P("gx"),
            P("gx", "gy"),
            P("gx", "gy"),
            P("gx", "gy"),
            P("gy", "gx"),
            P("gx"),
            P("gx", "gy"),
            P("gx", "gy"),
            P("gy", "gx"),
            P("gx", None),
            P("gx", "gy"),
        ),
        out_specs=(
            P("gx", "gy"),
            P("gx", "gy"),
            P("gx"),
            P("gx", "gy"),
            P("gx", "gy"),
            P("gx", "gy"),
            P("gy", "gx"),
            P("gx"),
            P("gx", "gy"),
            P("gx", "gy"),
            P("gy", "gx"),
        ),
        check_vma=False,
    )
```

```python
import functools
import math

import jax
import jax.numpy as jnp
from jax import lax
from jax.experimental import pallas as pl
from jax.experimental.pallas import tpu as pltpu
from jax.sharding import PartitionSpec as P

QUERY_HEADS = 15
KEY_VALUE_HEADS = 5
HEAD_SIZE = 64
PACKED_LENGTH = 1024
LONGEST_SEGMENT = 512

EPS = 1e-05
THETA = 10000.0
MESH = pl.DeviceIdType.MESH
F32 = jnp.float32
BF16 = jnp.bfloat16


class Grid:
    def __init__(self, gx, gy):
        self.gx, self.gy = gx, gy
        self.C = 2 if gy % 2 == 0 else 1
        self.X = gy // self.C
        self.Y = self.X if gx % self.X == 0 else 1
        self.Z = gx // self.Y
        self.size = {"z": self.Z, "y": self.Y, "x": self.X}

    def here(self):
        i, j = lax.axis_index("gx"), lax.axis_index("gy")
        return {"z": i // self.Y, "y": i % self.Y, "x": j // self.C, "c": j % self.C}

    def device(self, at):
        return (at["z"] * self.Y + at["y"], at["x"] * self.C + at["c"])


def when(condition, body):
    if condition is None:
        body()
    else:
        pl.when(condition)(body)


def remote(src, dst, send, recv, device):
    return pltpu.make_async_remote_copy(
        src_ref=src, dst_ref=dst, send_sem=send, recv_sem=recv, device_id=device, device_id_type=MESH
    )


def greet(devices):
    barrier = pltpu.get_barrier_semaphore()
    for condition, device in devices:

        def signal(device=device):
            pl.semaphore_signal(barrier, inc=1, device_id=device, device_id_type=MESH)

        when(condition, signal)
    count = sum(1 for condition, _ in devices if condition is None)
    for condition, _ in devices:
        if condition is not None:
            count = count + condition.astype(jnp.int32)
    pl.semaphore_wait(barrier, count)


def row_peers(n, me):
    return [(d, lax.rem(me + d, n)) for d in range(1, n)]


def along(grid, me, axis):
    n = grid.size[axis]
    if n == 1:
        return []
    if n == 2:
        return [(None, grid.device({**me, axis: 1 - me[axis]}))]
    return [
        (me[axis] > 0, grid.device({**me, axis: me[axis] - 1})),
        (me[axis] < n - 1, grid.device({**me, axis: me[axis] + 1})),
    ]


def order_of(here, n):
    if n & (n - 1):
        return [lax.rem(here + k, n) for k in range(n)]
    places = []
    for k in range(n):
        place, bit = 0, 1
        while bit < n:
            digit = (here // bit) % 2
            place = place + bit * ((1 - digit) if k & bit else digit)
            bit *= 2
        places.append(place)
    return places


def gather_sites(grid, me, order):
    other = [(None, grid.device({**me, "c": 1 - me["c"]}))] if grid.C == 2 else []
    onward = [along(grid, me, axis) for axis in order]
    yield 0, None, dict(me), sum(onward, []) + other
    for stage, axis in enumerate(order, 1):
        n = grid.size[axis]
        earlier = [dict(me)]
        for done in order[: stage - 1]:
            earlier = [{**e, done: place} for place in order_of(me[done], grid.size[done]) for e in earlier]
        later = sum(onward[stage:], []) + other
        for distance in range(1, n):
            if n == 2:
                for e in earlier:
                    yield stage, None, {**e, axis: 1 - me[axis]}, later
                continue
            for sign in (-1, 1):
                origin = me[axis] + sign * distance
                exists = origin >= 0 if sign < 0 else origin <= n - 1
                further = me[axis] - sign
                room = further <= n - 1 if sign < 0 else further >= 0
                ahead = [(room, grid.device({**me, axis: further}))]
                if distance == n - 1:
                    ahead = []
                for e in earlier:
                    yield stage, exists, {**e, axis: origin}, ahead + later


def core_sites(grid, me):
    found = [{"c": 1 - me["c"]}]
    for axis in "xyz":
        found = [{**f, axis: place} for place in order_of(me[axis], grid.size[axis]) for f in found]
    return found


class Lane:
    def __init__(self, order, first, count, width, base, step, every):
        self.order, self.first, self.count, self.width = order, first, count, width
        self.base, self.step, self.every = base, step, every

    def columns(self, m):
        return pl.ds(pl.multiple_of(self.base + m * self.step, 128), self.width)

    def own_columns(self, m):
        return pl.ds(pl.multiple_of(m * self.width, 128), self.width)

    def at(self, slot, body):
        if isinstance(slot, int):
            if slot >= 0 and slot % self.every == 0 and slot // self.every < self.count:
                body(slot // self.every)
            return
        active = (slot >= 0) & (slot < self.count * self.every)
        if self.every > 1:
            active = active & (slot % self.every == 0)
        pl.when(active)(lambda: body(slot // self.every))


class Plan:
    def __init__(self, grid, cols, orders):
        tiles = cols // 128
        third = max(1, round(tiles / 5))
        third += (tiles - third) % 2
        each = (tiles - third) // 2
        self.slots = each if grid.gx * grid.gy <= 64 and each > 2 and 2 * third <= each else 1
        width = each // self.slots * 128
        chunks = third if self.slots > 1 else 1
        every = 2 if self.slots > 1 else 1
        self.lanes = [
            Lane(orders[0], 0, self.slots, width, 0, 2 * width, 1),
            Lane(orders[1], self.slots, self.slots, width, width, 2 * width, 1),
            Lane(orders[2], 2 * self.slots, chunks, third // chunks * 128, 2 * width * self.slots, third // chunks * 128, every),
        ]
        self.chunks = 2 * self.slots + chunks


GATHER_ORDERS = ("zyx", "zxy", "yxz")
REDUCE_ORDERS = ("xyz", "yxz", "zxy")


def place_of(grid, piece):
    return piece["x"] * grid.C + piece["c"], piece["z"] * grid.Y + piece["y"]


def other_core(grid, me):
    return grid.device({**me, "c": 1 - me["c"]})


class Spread:
    def __init__(self, grid, me, plan, w_ref, out, send, recv):
        self.grid, self.me, self.plan = grid, me, plan
        self.w_ref, self.out, self.send, self.recv = w_ref, out, send, recv
        self.sites = [list(gather_sites(grid, me, lane.order)) for lane in plan.lanes]

    @staticmethod
    def count(grid):
        me = {"z": 0, "y": 0, "x": 0, "c": 0}
        return max(sum(len(sends) for _, _, _, sends in gather_sites(grid, me, order)) for order in GATHER_ORDERS)

    @staticmethod
    def semaphores(grid, plan):
        return [
            pltpu.SemaphoreType.DMA((Spread.count(grid), plan.chunks)),
            pltpu.SemaphoreType.DMA((grid.gy, grid.gx, plan.chunks)),
        ]

    def stage(self, stage, slot, finish=False):
        for lane, sites in zip(self.plan.lanes, self.sites):
            lane.at(slot, lambda m, lane=lane, sites=sites: self.chunk(lane, sites, stage, m, finish))

    def chunk(self, lane, sites, stage, m, finish):
        number, chunk = 0, lane.first + m
        for at, exists, piece, sends in sites:
            first = number
            number += len(sends)
            if at != stage:
                continue
            j, i = place_of(self.grid, piece)
            land = self.out.at[j, i, :, lane.columns(m)]
            src = self.w_ref.at[:, lane.columns(m)] if at == 0 else land
            arrived = self.recv.at[j, i, chunk]

            def body(at=at, land=land, src=src, arrived=arrived, sends=sends, first=first):
                if at and not finish:
                    remote(land, land, self.send.at[first, chunk], arrived, (0, 0)).wait_recv()
                for n, (condition, device) in enumerate(sends):
                    copy = remote(src, land, self.send.at[first + n, chunk], arrived, device)
                    when(condition, copy.wait_send if finish else copy.start)

            when(exists, body)

    def start(self):
        for slot in range(self.plan.slots):
            self.stage(0, slot)

    def slot(self, t):
        for stage in (1, 2, 3):
            self.stage(stage, t - (stage - 1))

    def finish(self):
        grid = self.grid

        def end(t, carry):
            for lane in self.plan.lanes:

                def core(m, lane=lane):
                    if grid.C == 2:
                        for piece in core_sites(grid, self.me):
                            j, i = place_of(grid, piece)
                            land = self.out.at[j, i, :, lane.columns(m)]
                            chunk = lane.first + m
                            remote(land, land, self.send.at[0, chunk], self.recv.at[j, i, chunk], (0, 0)).wait_recv()

                lane.at(t, core)
            for stage in range(4):
                self.stage(stage, t, True)
            return carry

        lax.fori_loop(0, self.plan.slots, end, 0)


def gather_peers(grid, me, i, j):
    peers = [(None, (p, j)) for _, p in row_peers(grid.gx, i)] + along(grid, me, "x")
    return peers + ([(None, other_core(grid, me))] if grid.C == 2 else [])


class Tokens:
    def __init__(self, grid, i, j, tok, send, recv, local):
        self.grid, self.i, self.j, self.tok = grid, i, j, tok
        self.send, self.recv, self.local, self.waits = send, recv, local, []

    @staticmethod
    def semaphores(grid, n):
        return [
            pltpu.SemaphoreType.DMA((n, grid.gx - 1)),
            pltpu.SemaphoreType.DMA((n, grid.gx - 1)),
            pltpu.SemaphoreType.DMA((n,)),
        ]

    def of(self, ref, p):
        return ref.at[:, pl.ds(pl.multiple_of(p * self.tok, self.tok), self.tok)]

    def start(self, n, pick, land):
        for d, p in row_peers(self.grid.gx, self.i):
            back = lax.rem(self.i + self.grid.gx - d, self.grid.gx)
            sems = self.send.at[n, d - 1], self.recv.at[n, d - 1]
            copy = remote(pick(p), land(self.i), *sems, (p, self.j))
            copy.start()
            self.waits.append(copy.wait_send)
            self.waits.append(remote(land(back), land(back), *sems, (p, self.j)).wait_recv)
        own = pltpu.make_async_copy(pick(self.i), land(self.i), self.local.at[n])
        own.start()
        self.waits.append(own.wait)

    def finish(self):
        for wait in self.waits:
            wait()


HBM_SPEC = pl.BlockSpec(memory_space=pl.ANY)
VMEM_SPEC = pl.BlockSpec(memory_space=pltpu.VMEM)


def params(collective_id):
    return pltpu.CompilerParams(
        collective_id=collective_id, has_side_effects=True, vmem_limit_bytes=60 * 1024 * 1024
    )


def gather_kernel(grid, tok, plan, x_ref, small_ref, w_ref, xo, smallo, wo, t_s, t_r, t_l, w_l, w_s, w_r):
    me = grid.here()
    i, j = lax.axis_index("gx"), lax.axis_index("gy")
    greet(gather_peers(grid, me, i, j))
    tokens = Tokens(grid, i, j, tok, t_s, t_r, t_l)
    spread = Spread(grid, me, plan, w_ref, wo, w_s, w_r)
    tokens.start(0, lambda p: tokens.of(x_ref, p), lambda p: xo.at[p])
    tokens.start(1, lambda p: small_ref, lambda p: smallo.at[p])
    own = pltpu.make_async_copy(w_ref, wo.at[j, i], w_l.at[0])
    own.start()
    spread.start()

    def slot(t, carry):
        spread.slot(t)
        return carry

    lax.fori_loop(0, plan.slots + 2, slot, 0)
    spread.finish()
    tokens.finish()
    own.wait()


def gather(grid, tok, x, small, w):
    rows, cols = w.shape
    plan = Plan(grid, cols, GATHER_ORDERS)
    return pl.pallas_call(
        functools.partial(gather_kernel, grid, tok, plan),
        out_shape=[
            jax.ShapeDtypeStruct((grid.gx, x.shape[0], tok), BF16),
            jax.ShapeDtypeStruct((grid.gx,) + small.shape, F32),
            jax.ShapeDtypeStruct((grid.gy, grid.gx, rows, cols), BF16),
        ],
        in_specs=[VMEM_SPEC] * 3,
        out_specs=[HBM_SPEC] * 3,
        scratch_shapes=Tokens.semaphores(grid, 2) + [pltpu.SemaphoreType.DMA((1,))] + Spread.semaphores(grid, plan),
        compiler_params=params(0),
        name="gather",
    )(x, small, w)


def dot(a, b, contract):
    return lax.dot_general(a, b, ((contract[:1], contract[1:]), ((), ())), preferred_element_type=F32)


def attention_bias(seg_query, seg_window):
    tok, window = seg_query.shape[0], seg_window.shape[1]
    row = lax.broadcasted_iota(jnp.int32, (tok, window), 0) + (window - tok)
    column = lax.broadcasted_iota(jnp.int32, (tok, window), 1)
    return jnp.where((seg_query == seg_window) & (column <= row), 0.0, -jnp.inf).astype(F32)


def head_rows(head):
    return pl.ds(pl.multiple_of(head * HEAD_SIZE, HEAD_SIZE), HEAD_SIZE)


def in_window(win_ref, own_ref, head):
    parts = [win_ref[n, head_rows(head), :] for n in reversed(range(win_ref.shape[0]))]
    return jnp.concatenate(parts + [own_ref[head_rows(head), :]], axis=1)


def probabilities(query, key, bias):
    scores = dot(query, key, (0, 0)) * HEAD_SIZE ** (-0.5) + bias
    raised = jnp.exp(scores - jnp.max(scores, axis=1, keepdims=True))
    return raised * (1.0 / jnp.sum(raised, axis=1, keepdims=True))


def attend(k, kv_heads, groups, q_ref, win_ref, own_ref, bias_ref, o_ref):
    key, value = in_window(win_ref, own_ref, k), in_window(win_ref, own_ref, kv_heads + k)
    for g in range(groups):
        rows = head_rows(k * groups + g)
        prob = probabilities(q_ref[rows, :], key, bias_ref[...]).astype(BF16)
        o_ref[rows, :] = dot(value, prob, (1, 1)).astype(BF16)


def attend_back(k, kv_heads, groups, q_ref, do_ref, win_ref, own_ref, bias_ref, dq_ref, dkv_out, dkv_own):
    key, value = in_window(win_ref, own_ref, k), in_window(win_ref, own_ref, kv_heads + k)
    key_grad = value_grad = None
    for g in range(groups):
        rows = head_rows(k * groups + g)
        query, grad = q_ref[rows, :], do_ref[rows, :]
        prob = probabilities(query, key, bias_ref[...])
        prob_grad = dot(grad, value, (0, 0))
        row_dot = jnp.sum(prob * prob_grad, axis=1, keepdims=True)
        score_grad = (prob * (prob_grad - row_dot) * HEAD_SIZE ** (-0.5)).astype(BF16)
        dq_ref[rows, :] = dot(key, score_grad, (1, 1))
        dk = dot(query, score_grad, (1, 0))
        dv = dot(grad, prob.astype(BF16), (1, 0))
        key_grad = dk if g == 0 else key_grad + dk
        value_grad = dv if g == 0 else value_grad + dv
    tok = q_ref.shape[1]
    for head, grad in ((k, key_grad), (kv_heads + k, value_grad)):
        before = dkv_out.shape[0]
        for n in range(before):
            at = before - 1 - n
            dkv_out[n, head_rows(head), :] = grad[:, at * tok : (at + 1) * tok].astype(BF16)
        dkv_own[head_rows(head), :] = grad[:, before * tok :]


class Shift:
    def __init__(self, i, j, span, sign, n, send, recv):
        self.base, self.q, self.j, self.span, self.sign, self.n = i // span * span, i % span, j, span, sign, n
        self.send, self.recv = send, recv

    def copies(self, pick, land):
        for n in range(self.n):
            to = self.base + lax.rem(self.q + (self.sign * (n + 1)) % self.span, self.span)
            yield remote(pick(n), land(n), self.send.at[n], self.recv.at[n], (to, self.j))


def forward_kernel(
    grid, tok, plan, span, kv_heads, groups,
    q_ref, kv_ref, sq_ref, sw_ref, dy_ref, w_ref,
    o_ref, win, dyo, wo,
    bias, t_s, t_r, t_l, k_s, k_r, w_l, w_s, w_r,
):
    me = grid.here()
    i, j = lax.axis_index("gx"), lax.axis_index("gy")
    greet(gather_peers(grid, me, i, j))
    shift = list(Shift(i, j, span, 1, win.shape[0], k_s, k_r).copies(lambda n: kv_ref, lambda n: win.at[n]))
    for copy in shift:
        copy.start()
    tokens = Tokens(grid, i, j, tok, t_s, t_r, t_l)
    spread = Spread(grid, me, plan, w_ref, wo, w_s, w_r)
    own = pltpu.make_async_copy(w_ref, wo.at[j, i], w_l.at[0])
    own.start()
    spread.start()
    tokens.start(0, lambda p: tokens.of(dy_ref, p), lambda p: dyo.at[p])
    bias[...] = attention_bias(sq_ref[...], sw_ref[...])
    for copy in shift:
        copy.wait()

    def slot(t, carry):
        spread.slot(t)
        pl.when(t < kv_heads)(lambda: attend(t, kv_heads, groups, q_ref, win, kv_ref, bias, o_ref))
        return carry

    lax.fori_loop(0, max(plan.slots + 2, kv_heads), slot, 0)
    spread.finish()
    tokens.finish()
    own.wait()


def forward(grid, tok, span, before, heads, kv_heads, q, kv, seg_query, seg_window, dy, w):
    rows, cols = w.shape
    plan = Plan(grid, cols, GATHER_ORDERS)
    return pl.pallas_call(
        functools.partial(forward_kernel, grid, tok, plan, span, kv_heads, heads // kv_heads),
        out_shape=[
            jax.ShapeDtypeStruct(q.shape, BF16),
            jax.ShapeDtypeStruct((before,) + kv.shape, BF16),
            jax.ShapeDtypeStruct((grid.gx, dy.shape[0], tok), BF16),
            jax.ShapeDtypeStruct((grid.gy, grid.gx, rows, cols), BF16),
        ],
        in_specs=[VMEM_SPEC] * 6,
        out_specs=[VMEM_SPEC] * 2 + [HBM_SPEC] * 2,
        scratch_shapes=[pltpu.VMEM((tok, (before + 1) * tok), F32)]
        + Tokens.semaphores(grid, 1)
        + [pltpu.SemaphoreType.DMA((before,))] * 2
        + [pltpu.SemaphoreType.DMA((1,))]
        + Spread.semaphores(grid, plan),
        compiler_params=params(1),
        name="forward",
    )(q, kv, seg_query, seg_window, dy, w)


def slots_of(n):
    return 1 if n == 2 else max(1, 2 * (n - 1))


def over(ref, body):
    lead = ref.shape[:-2]
    total = math.prod(lead)

    def one(k, carry):
        place = []
        for n in reversed(lead):
            place.append(k % n)
            k = k // n
        body(tuple(reversed(place)))
        return carry

    if total == 1:
        body((0,) * len(lead))
    else:
        lax.fori_loop(0, total, one, 0)


def add_into(target, source):
    def one(place):
        where = place + (slice(None), slice(None))
        target[where] = target[where] + source[where]

    over(target, one)


DIMS = "xzy"


class Collect:
    def __init__(self, grid, me, plan, acc, from_core, lands, out, c_s, c_r, c_l, l_s, l_r):
        self.grid, self.me, self.plan = grid, me, plan
        self.acc, self.from_core, self.lands, self.out = acc, from_core, lands, out
        self.c_s, self.c_r, self.c_l, self.l_s, self.l_r = c_s, c_r, c_l, l_s, l_r
        self.actions = [self.actions_of(n, lane) for n, lane in enumerate(plan.lanes)]
        self.lags = max(len(actions) for actions in self.actions)

    @staticmethod
    def axes(grid, lane):
        return [axis for axis in lane.order if grid.size[axis] > 1]

    @staticmethod
    def scratch(grid, plan, rows, cols):
        size = (grid.X, grid.Z, grid.Y, rows, cols)
        shapes = [pltpu.VMEM(size, BF16), pltpu.VMEM(size, BF16)]
        for lane in plan.lanes:
            axes = Collect.axes(grid, lane)
            for level, axis in enumerate(axes):
                rest = tuple(grid.size[d] for d in DIMS if d in axes[level + 1 :])
                shapes.append(pltpu.VMEM((slots_of(grid.size[axis]),) + rest + (rows, lane.count * lane.width), BF16))
        sem = pltpu.SemaphoreType.DMA
        most = max(slots_of(n) for n in grid.size.values())
        levels = len(shapes) - 2
        return shapes, [sem((grid.X, plan.chunks))] * 3 + [sem((levels, most, plan.chunks))] * 2

    def own_copy(self, x, lane, m, g_ref, columns):
        src, chunk = g_ref.at[x * self.grid.C + self.me["c"], :, :, :, columns], lane.first + m
        return pltpu.make_async_copy(src, self.acc.at[x, :, :, :, lane.columns(m)], self.c_l.at[x, chunk])

    def core_copy(self, x, lane, m, g_ref, columns):
        src, chunk = g_ref.at[x * self.grid.C + 1 - self.me["c"], :, :, :, columns], lane.first + m
        land = self.from_core.at[x, :, :, :, lane.columns(m)]
        return remote(src, land, self.c_s.at[x, chunk], self.c_r.at[x, chunk], other_core(self.grid, self.me))

    def start(self, source):
        self.source = source
        for slot in range(self.plan.slots):
            for lane in self.plan.lanes:

                def body(m, lane=lane):
                    first = lane.base + m * lane.step
                    ref, at = source(first, lane.width)
                    for x in range(self.grid.X):
                        self.own_copy(x, lane, m, ref, pl.ds(at, lane.width)).start()
                        if self.grid.C == 2:
                            self.core_copy(x, lane, m, ref, pl.ds(at, lane.width)).start()

                lane.at(slot, body)

    def core(self, lane, m):
        columns = lane.columns(m)
        ref, _ = self.source(0, 128)
        for x in range(self.grid.X):
            self.own_copy(x, lane, m, ref, pl.ds(0, lane.width)).wait()
            if self.grid.C == 2:
                self.core_copy(x, lane, m, ref, pl.ds(0, lane.width)).wait_recv()
                add_into(self.acc.at[x, :, :, :, columns], self.from_core.at[x, :, :, :, columns])

    def level(self, number, lane, level):
        axes = self.axes(self.grid, lane)
        axis = axes[level]
        index = sum(len(self.axes(self.grid, other)) for other in self.plan.lanes[:number]) + level
        free = len(axes) - level - 1

        def pick(t, m):
            place = []
            for d in DIMS:
                if d == axis:
                    place.append(t)
                elif d in axes[level + 1 :]:
                    place.append(slice(None))
                else:
                    place.append(self.me[d] if self.grid.size[d] > 1 else 0)
            return self.acc.at[tuple(place) + (slice(None), lane.columns(m))]

        def land(slot, m):
            return self.lands[index].at[(slot,) + (slice(None),) * (free + 1) + (lane.own_columns(m),)]

        def copy(t, slot, m, step):
            device = self.grid.device({**self.me, axis: self.me[axis] + step})
            sems = self.l_s.at[index, slot, lane.first + m], self.l_r.at[index, slot, lane.first + m]
            return remote(pick(t, m), land(slot, m), *sems, device)

        def arrive(slot, m):
            where = land(slot, m)
            sems = self.l_s.at[index, slot, lane.first + m], self.l_r.at[index, slot, lane.first + m]
            remote(where, where, *sems, (0, 0)).wait_recv()

        return axis, self.grid.size[axis], self.me[axis], pick, land, copy, arrive

    def sends(self, number, lane, level):
        axis, n, p, pick, land, copy, arrive = self.level(number, lane, level)
        if n == 2:
            return [(None, 0, lambda m: copy(1 - p, 0, m, 1 - 2 * p), None)]
        found = []
        for step in range(n - 1):
            for t in range(n - 1, step, -1):
                found.append((p == step, step, lambda m, t=t: copy(t, t - 1, m, 1), (t - 1, t) if step else None))
            here = n - 1 - step
            for t in range(here):
                slot = n - 1 + t
                found.append((p == here, step, lambda m, t=t, slot=slot: copy(t, slot, m, -1), (slot, t) if step else None))
        return found

    def arrivals(self, number, lane, level):
        axis, n, p, pick, land, copy, arrive = self.level(number, lane, level)
        if n == 2:
            return [(None, 0)]
        return [(p == t, t - 1) for t in range(1, n)] + [(p == t, n - 1 + t) for t in range(n - 1)]

    def actions_of(self, number, lane):
        axes = self.axes(self.grid, lane)
        actions = [[functools.partial(self.core, lane)], []]
        for level, axis in enumerate(axes):
            _, n, p, pick, land, copy, arrive = self.level(number, lane, level)
            sends = self.sends(number, lane, level)

            def chain(m, step, sends=sends, pick=pick, land=land, arrive=arrive):
                for condition, at, copy_of, earlier in sends:
                    if at != step:
                        continue

                    def body(copy_of=copy_of, earlier=earlier):
                        if earlier is not None:
                            slot, t = earlier
                            arrive(slot, m)
                            add_into(pick(t, m), land(slot, m))
                        copy_of(m).start()

                    when(condition, body)

            at = 0 if level == 0 else len(actions) - 1
            for step in range(n - 1):
                if step and (level > 0 or step > 1):
                    actions.append([])
                where = at if step == 0 else (1 if level == 0 and step == 1 else len(actions) - 1)
                actions[where].append(functools.partial(chain, step=step))
            actions.append([])
            last = level == len(axes) - 1

            def take(m, level=level, p=p, pick=pick, land=land, arrive=arrive, last=last):
                columns = lane.columns(m)
                if last:
                    self.out[:, columns] = pick(p, m)[...].astype(F32)
                for condition, slot in self.arrivals(number, lane, level):

                    def body(slot=slot):
                        arrive(slot, m)
                        if last:
                            self.out[:, columns] += land(slot, m)[...].astype(F32)
                        else:
                            add_into(pick(p, m), land(slot, m))

                    when(condition, body)

            actions[-1].append(take)
        return actions

    def slot(self, t):
        for lag in range(self.lags):
            for lane, actions in zip(self.plan.lanes, self.actions):
                if lag < len(actions):
                    for action in actions[lag]:
                        lane.at(t - lag, action)

    def finish(self):
        def end(t, carry):
            for number, lane in enumerate(self.plan.lanes):

                def body(m, number=number, lane=lane):
                    if self.grid.C == 2:
                        ref, _ = self.source(0, 128)
                        for x in range(self.grid.X):
                            self.core_copy(x, lane, m, ref, pl.ds(0, lane.width)).wait_send()
                    for level in range(len(self.axes(self.grid, lane))):
                        for condition, _, copy_of, _ in self.sends(number, lane, level):
                            when(condition, copy_of(m).wait_send)

                lane.at(t, body)
            return carry

        lax.fori_loop(0, self.plan.slots, end, 0)


def reduce_peers(grid, me, i, j):
    peers = [(None, (p, j)) for _, p in row_peers(grid.gx, i)]
    return peers + [(None, (i, p)) for _, p in row_peers(grid.gy, j)]


def backward_kernel(
    grid, tok, plan, span, kv_heads, groups, splits,
    q_ref, do_ref, kv_ref, win, sq_ref, sw_ref, *refs,
):
    g_refs, refs = refs[: len(splits)], refs[len(splits) :]
    (dq_ref, dkv_own, go), refs = refs[:3], refs[3:]
    (bias, dkv_out, dkv_in, acc, from_core), refs = refs[:5], refs[5:]
    lands, (k_s, k_r, *sems) = refs[:-7], refs[-7:]
    me = grid.here()
    i, j = lax.axis_index("gx"), lax.axis_index("gy")
    greet(reduce_peers(grid, me, i, j))
    collect = Collect(grid, me, plan, acc, from_core, lands, go, *sems)

    def source(first, width):
        for ref, start in zip(reversed(g_refs), reversed(splits)):
            if first >= start:
                return ref, first - start

    collect.start(source)
    bias[...] = attention_bias(sq_ref[...], sw_ref[...])
    shift = list(Shift(i, j, span, -1, win.shape[0], k_s, k_r).copies(lambda n: dkv_out.at[n], lambda n: dkv_in.at[n]))

    def slot(t, carry):
        collect.slot(t)
        pl.when(t < kv_heads)(
            lambda: attend_back(t, kv_heads, groups, q_ref, do_ref, win, kv_ref, bias, dq_ref, dkv_out, dkv_own)
        )

        @pl.when(t == kv_heads)
        def _():
            for copy in shift:
                copy.start()

        return carry

    lax.fori_loop(0, max(plan.slots + collect.lags - 1, kv_heads + 1), slot, 0)
    for n, copy in enumerate(shift):
        copy.wait()
        dkv_own[...] += dkv_in[n].astype(F32)
    collect.finish()


def backward(grid, tok, span, heads, kv_heads, q, do, kv, win, seg_query, seg_window, grads):
    rows = grads[0].shape[-2]
    splits, cols = [], 0
    for g in grads:
        splits.append(cols)
        cols += g.shape[-1]
    plan = Plan(grid, cols, REDUCE_ORDERS)
    shapes, sems = Collect.scratch(grid, plan, rows, cols)
    before = win.shape[0]
    return pl.pallas_call(
        functools.partial(backward_kernel, grid, tok, plan, span, kv_heads, heads // kv_heads, splits),
        out_shape=[
            jax.ShapeDtypeStruct(q.shape, F32),
            jax.ShapeDtypeStruct(kv.shape, F32),
            jax.ShapeDtypeStruct((rows, cols), F32),
        ],
        in_specs=[VMEM_SPEC] * 6 + [HBM_SPEC] * len(grads),
        out_specs=[VMEM_SPEC] * 3,
        scratch_shapes=[
            pltpu.VMEM((tok, (before + 1) * tok), F32),
            pltpu.VMEM((before,) + kv.shape, BF16),
            pltpu.VMEM((before,) + kv.shape, BF16),
        ]
        + shapes
        + [pltpu.SemaphoreType.DMA((before,))] * 2
        + sems,
        compiler_params=params(2),
        name="backward",
    )(q, do, kv, win, seg_query, seg_window, *[g.reshape(g.shape[0], grid.Z, grid.Y, rows, -1) for g in grads])


def reduce_kernel(
    grid, tok, plan, g_ref, bo_ref, ig_ref, gain_ref,
    bo, ig, go, gaino,
    gain_in, gain_row, gain_across, acc, from_core, *refs,
):
    lands, (t_s, t_r, t_l, g_s, g_r, h_s, h_r, *sems) = refs[:-12], refs[-12:]
    me = grid.here()
    i, j = lax.axis_index("gx"), lax.axis_index("gy")
    peers, across = row_peers(grid.gx, i), row_peers(grid.gy, j)
    greet(reduce_peers(grid, me, i, j))
    collect = Collect(grid, me, plan, acc, from_core, lands, go, *sems)
    collect.start(lambda first, width: (g_ref, first))
    tokens = Tokens(grid, i, j, tok, t_s, t_r, t_l)
    tokens.start(0, lambda p: bo_ref.at[p], lambda p: tokens.of(bo, p))
    tokens.start(1, lambda p: ig_ref.at[p], lambda p: tokens.of(ig, p))
    column = []
    for d, p in peers:
        copy = remote(gain_ref.at[p], gain_in.at[d - 1], g_s.at[d - 1], g_r.at[d - 1], (p, j))
        copy.start()
        column.append(copy)

    def slot(t, carry):
        collect.slot(t)
        return carry

    lax.fori_loop(0, 1, slot, 0)
    gain_row[...] = gain_ref[i]
    for (d, _), copy in zip(peers, column):
        copy.wait()
        gain_row[...] += gain_in[d - 1]
    row = []
    for d, p in across:
        copy = remote(gain_row, gain_across.at[d - 1], h_s.at[d - 1], h_r.at[d - 1], (i, p))
        copy.start()
        row.append(copy)
    lax.fori_loop(1, plan.slots + collect.lags - 1, slot, 0)
    gaino[...] = gain_row[...]
    for (d, _), copy in zip(across, row):
        copy.wait()
        gaino[...] += gain_across[d - 1]
    tokens.finish()
    collect.finish()


def reduce(grid, tok, g, bo, ig, gain):
    rows, cols = g.shape[-2:]
    width = bo.shape[1]
    plan = Plan(grid, cols, REDUCE_ORDERS)
    shapes, sems = Collect.scratch(grid, plan, rows, cols)
    sem = pltpu.SemaphoreType.DMA
    return pl.pallas_call(
        functools.partial(reduce_kernel, grid, tok, plan),
        out_shape=[
            jax.ShapeDtypeStruct((width, grid.gx * tok), BF16),
            jax.ShapeDtypeStruct((width, grid.gx * tok), BF16),
            jax.ShapeDtypeStruct((rows, cols), F32),
            jax.ShapeDtypeStruct((8, 128), F32),
        ],
        in_specs=[HBM_SPEC] + [VMEM_SPEC] * 3,
        out_specs=[VMEM_SPEC] * 4,
        scratch_shapes=[
            pltpu.VMEM((grid.gx - 1, 8, 128), F32),
            pltpu.VMEM((8, 128), F32),
            pltpu.VMEM((grid.gy - 1, 8, 128), F32),
        ]
        + shapes
        + Tokens.semaphores(grid, 2)
        + [sem((grid.gx - 1,))] * 2
        + [sem((grid.gy - 1,))] * 2
        + sems,
        compiler_params=params(3),
        name="reduce",
    )(g.reshape(grid.gy, grid.Z, grid.Y, rows, cols), bo, ig, gain)


def rotate(values, cos_table, sine_table, direction):
    half = HEAD_SIZE // 2
    heads = values.reshape(-1, 2, half, values.shape[1])
    lower, upper = heads[:, 0], heads[:, 1]
    turned = jnp.stack(
        [lower * cos_table - direction * upper * sine_table, upper * cos_table + direction * lower * sine_table], axis=1
    )
    return turned.reshape(values.shape)


def einsum(form, a, b):
    return jnp.einsum(form, a, b, preferred_element_type=F32)


def padded(a, axis, size):
    pads = [(0, 0)] * a.ndim
    pads[axis] = (0, size - a.shape[axis])
    return jnp.pad(a, pads) if size != a.shape[axis] else a


def norm_backward(values, scale, gain, grad):
    weighted = grad * gain[:, None]
    inner = jnp.sum(weighted * values, axis=0) / values.shape[0]
    back = scale * weighted - values * (scale * scale * scale * inner)
    return back, jnp.sum(grad * values * scale, axis=1)


def shards(
    grid,
    block_input,
    attn_gain,
    query_weight,
    key_weight,
    value_weight,
    output_weight,
    ffn_gain,
    gate_weight,
    up_weight,
    down_weight,
    segment_ids,
    out_cotangent,
):
    GX, GY = grid.gx, grid.gy
    rows, row_tokens = block_input.shape
    tok = row_tokens // GX
    features = rows * GX
    span = PACKED_LENGTH // tok
    before = -(-(LONGEST_SEGMENT - 1) // tok)
    qc, kc, fc = query_weight.shape[1], key_weight.shape[1], gate_weight.shape[1]
    kv = kc * GY
    heads, kv_heads = qc * GY // HEAD_SIZE, kv // HEAD_SIZE
    i, j = lax.axis_index("gx"), lax.axis_index("gy")
    q = i % span

    attn_block = jnp.concatenate([query_weight, key_weight, value_weight, output_weight.T], axis=1)
    attn_block = padded(attn_block, 1, -(-attn_block.shape[1] // 128) * 128)
    ffn_block = jnp.concatenate([gate_weight, up_weight, down_weight.T], axis=1)
    ffn_block = padded(ffn_block, 1, -(-ffn_block.shape[1] // 128) * 128)
    segments_here = segment_ids.reshape(-1, 256).astype(F32)
    n_seg = segments_here.shape[0]
    small = padded(
        jnp.concatenate([segments_here, padded(jnp.stack([attn_gain, ffn_gain]), 1, 256)], axis=0), 0, -(-(n_seg + 2) // 8) * 8
    )
    x_parts, small_all, w_attn = gather(grid, tok, block_input, small, attn_block)

    x = x_parts.reshape(features, tok).astype(F32)
    w_attn = w_attn.reshape(GY, features, -1)
    w_qkv = w_attn[:, :, : qc + 2 * kc]
    w_out = w_attn[:, :, qc + 2 * kc : 2 * (qc + kc)]
    gain_one, gain_two = (small_all[:, n_seg + k, :rows].reshape(features) for k in range(2))

    sequence = j * (row_tokens // PACKED_LENGTH) + i // span
    segments = lax.dynamic_index_in_dim(small_all[:, :n_seg].reshape(GX, PACKED_LENGTH), sequence, 0, keepdims=False)
    window = (before + 1) * tok
    seg_window = lax.dynamic_slice_in_dim(
        jnp.concatenate([jnp.full((before * tok,), -1.0, F32), segments]), q * tok, window, 0
    )
    seg_query = seg_window[before * tok :]
    first = jnp.sum((segments[None, :] < seg_query[:, None]).astype(F32), axis=1)
    positions = (q * tok).astype(F32) + jnp.arange(tok, dtype=F32) - first
    half = HEAD_SIZE // 2
    frequency = jnp.exp(-math.log(THETA) * jnp.arange(half, dtype=F32) / half)
    angles = frequency[:, None] * positions[None, :]
    cos_table, sine_table = jnp.cos(angles), jnp.sin(angles)

    scale_one = lax.rsqrt(jnp.mean(x * x, axis=0) + EPS)
    normed_one = (x * scale_one * gain_one[:, None]).astype(BF16)
    qkv = einsum("jdc,dt->jct", w_qkv, normed_one).astype(BF16)
    query = rotate(qkv[:, :qc].reshape(-1, tok).astype(F32), cos_table, sine_table, 1.0).astype(BF16)
    key = rotate(qkv[:, qc : qc + kc].reshape(-1, tok).astype(F32), cos_table, sine_table, 1.0).astype(BF16)
    key_value = jnp.concatenate([key, qkv[:, qc + kc :].reshape(-1, tok)], axis=0)
    mixed, earlier, dy_parts, w_ffn = forward(
        grid, tok, span, before, heads, kv_heads,
        query, key_value, seg_query[:, None], seg_window[None, :], out_cotangent, ffn_block,
    )
    dy_half = dy_parts.reshape(features, tok)
    w_ffn = w_ffn.reshape(GY, features, -1)
    w_gate, w_up, w_down = (w_ffn[:, :, k * fc : (k + 1) * fc] for k in range(3))
    mixed = mixed.reshape(GY, qc, tok)
    hidden_in = x + einsum("jdc,jct->dt", w_out, mixed)
    scale_two = lax.rsqrt(jnp.mean(hidden_in * hidden_in, axis=0) + EPS)
    normed_two = (hidden_in * scale_two * gain_two[:, None]).astype(BF16)
    gate = einsum("dt,jdf->jtf", normed_two, w_gate)
    up = einsum("dt,jdf->jtf", normed_two, w_up)
    sigmoid = jax.nn.sigmoid(gate)
    hidden = (jax.nn.silu(gate) * up).astype(BF16)
    block_output = (hidden_in + einsum("jdf,jtf->dt", w_down, hidden)).astype(BF16)

    hidden_grad = einsum("dt,jdf->jtf", dy_half, w_down)
    gate_back = (hidden_grad * up * sigmoid * (1.0 + gate * (1.0 - sigmoid))).astype(BF16)
    up_back = (hidden_grad * gate * sigmoid).astype(BF16)
    both_back = jnp.concatenate([gate_back, up_back], axis=2)
    grad_both = einsum("dt,jtf->jdf", normed_two, both_back).astype(BF16)
    grad_down = padded(einsum("dt,jtf->jdf", dy_half, hidden).astype(BF16), 2, ffn_block.shape[1] - 2 * fc)
    normed_two_grad = einsum("jdf,jtf->dt", w_ffn[:, :, : 2 * fc], both_back)
    hidden_in_grad, gain_two_part = norm_backward(hidden_in, scale_two, gain_two, normed_two_grad)
    hidden_in_grad = hidden_in_grad + dy_half.astype(F32)
    hidden_in_half = hidden_in_grad.astype(BF16)
    head_grad = einsum("jdc,dt->jct", w_out, hidden_in_half).astype(BF16).reshape(-1, tok)
    grad_both, grad_down = (g.reshape(GY, GX, rows, -1) for g in (grad_both, grad_down))
    query_grad, key_value_grad, grad_ffn = backward(
        grid, tok, span, heads, kv_heads,
        query, head_grad, key_value, earlier, seg_query[:, None], seg_window[None, :], aligned(grid, grad_both, grad_down),
    )
    query_back = rotate(query_grad, cos_table, sine_table, -1.0).astype(BF16).reshape(GY, qc, tok)
    key_back = rotate(key_value_grad[:kv], cos_table, sine_table, -1.0).astype(BF16).reshape(GY, kc, tok)
    qkv_back = jnp.concatenate([query_back, key_back, key_value_grad[kv:].astype(BF16).reshape(GY, kc, tok)], axis=1)
    grad_qkv = einsum("dt,jct->jdc", normed_one, qkv_back).astype(BF16)
    grad_out = einsum("dt,jct->jdc", hidden_in_half, mixed).astype(BF16)
    normed_one_grad = einsum("jdc,jct->dt", w_qkv, qkv_back)
    input_grad, gain_one_part = norm_backward(x, scale_one, gain_one, normed_one_grad)
    input_grad = (input_grad + hidden_in_grad).astype(BF16)

    grads = padded(jnp.concatenate([grad_qkv, grad_out], axis=2), 2, attn_block.shape[1]).reshape(GY, GX, rows, -1)
    gains = padded(padded(jnp.stack([gain_one_part, gain_two_part]).reshape(2, GX, rows).transpose(1, 0, 2), 1, 8), 2, 128)
    block_output, input_grad, grads, gains = reduce(
        grid, tok, grads, block_output.reshape(GX, rows, tok), input_grad.reshape(GX, rows, tok), gains
    )
    grad_query, grad_key, grad_value, grad_out = jnp.split(
        grads[:, : 2 * (qc + kc)], [qc, qc + kc, qc + 2 * kc], axis=1
    )
    grad_gate, grad_up, grad_down = (grad_ffn[:, k * fc : (k + 1) * fc] for k in range(3))
    return (
        block_output,
        input_grad.astype(F32),
        gains[0, :rows],
        grad_query,
        grad_key,
        grad_value,
        grad_out.T,
        gains[1, :rows],
        grad_gate,
        grad_up,
        grad_down.T,
    )


def aligned(grid, both, down):
    first, cols = both.shape[-1], both.shape[-1] + down.shape[-1]
    lanes = Plan(grid, cols, REDUCE_ORDERS).lanes
    starts = [(lane.base + m * lane.step, lane.width) for lane in lanes for m in range(lane.count)]
    if first % 128 or any(start < first < start + width for start, width in starts):
        return [jnp.concatenate([both, down], axis=-1)]
    return [both, down]


def solution(mesh):
    grid = Grid(mesh.shape["gx"], mesh.shape["gy"])
    return jax.shard_map(
        functools.partial(shards, grid),
        mesh=mesh,
        in_specs=(
            P("gx", "gy"),
            P("gx"),
            P("gx", "gy"),
            P("gx", "gy"),
            P("gx", "gy"),
            P("gy", "gx"),
            P("gx"),
            P("gx", "gy"),
            P("gx", "gy"),
            P("gy", "gx"),
            P("gx", None),
            P("gx", "gy"),
        ),
        out_specs=(
            P("gx", "gy"),
            P("gx", "gy"),
            P("gx"),
            P("gx", "gy"),
            P("gx", "gy"),
            P("gx", "gy"),
            P("gy", "gx"),
            P("gx"),
            P("gx", "gy"),
            P("gx", "gy"),
            P("gy", "gx"),
        ),
        check_vma=False,
    )
```

```python
import functools
import math

import jax
import jax.numpy as jnp
from jax import lax
from jax.experimental import pallas as pl
from jax.experimental.pallas import tpu as pltpu
from jax.sharding import PartitionSpec as P

QUERY_HEADS = 15
KEY_VALUE_HEADS = 5
HEAD_SIZE = 64
PACKED_LENGTH = 1024
LONGEST_SEGMENT = 512

EPS = 1e-05
THETA = 10000.0
MESH = pl.DeviceIdType.MESH
F32 = jnp.float32
BF16 = jnp.bfloat16


class Grid:
    def __init__(self, gx, gy):
        self.gx, self.gy = gx, gy
        self.C = 2 if gy % 2 == 0 else 1
        self.X = gy // self.C
        self.Y = self.X if gx % self.X == 0 else 1
        self.Z = gx // self.Y
        self.size = {"z": self.Z, "y": self.Y, "x": self.X}

    def here(self):
        i, j = lax.axis_index("gx"), lax.axis_index("gy")
        return {"z": i // self.Y, "y": i % self.Y, "x": j // self.C, "c": j % self.C}

    def device(self, at):
        return (at["z"] * self.Y + at["y"], at["x"] * self.C + at["c"])


def remote(src, dst, send, recv, device):
    return pltpu.make_async_remote_copy(
        src_ref=src, dst_ref=dst, send_sem=send, recv_sem=recv, device_id=device, device_id_type=MESH
    )


def greet(devices):
    barrier = pltpu.get_barrier_semaphore()
    for device in devices:
        pl.semaphore_signal(barrier, inc=1, device_id=device, device_id_type=MESH)
    pl.semaphore_wait(barrier, len(devices))


def row_peers(n, me):
    return [(d, lax.rem(me + d, n)) for d in range(1, n)]


def line(n, here):
    found = []
    for k in range(1, n):
        if n & (n - 1):
            found.append((lax.rem(here + k, n), lax.rem(here + n - k, n)))
            continue
        place, bit = 0, 1
        while bit < n:
            digit = (here // bit) % 2
            place = place + bit * ((1 - digit) if k & bit else digit)
            bit *= 2
        found.append((place, place))
    return found


def places(n, here):
    return [here] + [origin for _, origin in line(n, here)]


def gather_sites(grid, me, order):
    other = [grid.device({**me, "c": 1 - me["c"]})] if grid.C == 2 else []
    onward = [[grid.device({**me, axis: to}) for to, _ in line(grid.size[axis], me[axis])] for axis in order]
    yield 0, dict(me), sum(onward, []) + other
    for stage, axis in enumerate(order, 1):
        earlier = [dict(me)]
        for done in order[: stage - 1]:
            earlier = [{**e, done: place} for place in places(grid.size[done], me[done]) for e in earlier]
        for _, origin in line(grid.size[axis], me[axis]):
            for e in earlier:
                yield stage, {**e, axis: origin}, sum(onward[stage:], []) + other


def core_sites(grid, me):
    found = [{"c": 1 - me["c"]}]
    for axis in "xyz":
        found = [{**f, axis: place} for place in places(grid.size[axis], me[axis]) for f in found]
    return found


class Lane:
    def __init__(self, order, first, count, width, base, step):
        self.order, self.first, self.count, self.width = order, first, count, width
        self.base, self.step = base, step

    def columns(self, m):
        return pl.ds(pl.multiple_of(self.base + m * self.step, 128), self.width)

    def own_columns(self, m):
        return pl.ds(pl.multiple_of(m * self.width, 128), self.width)

    def at(self, slot, body):
        if isinstance(slot, int):
            if 0 <= slot < self.count:
                body(slot)
        else:
            pl.when((slot >= 0) & (slot < self.count))(lambda: body(slot))

    def at_late(self, slot, body):
        pl.when((slot >= 0) & (slot <= self.count) & (slot != self.count - 1))(lambda: body(slot - slot // self.count))


GROUPS = 4


class Plan:
    def __init__(self, cols, orders):
        self.slots = GROUPS
        tiles = cols // 128 // GROUPS
        most = -(-tiles * 3 // 5)
        least = tiles - most
        self.lanes = [
            Lane(orders[0], 0, GROUPS, most * 128, 0, tiles * 128),
            Lane(orders[1], GROUPS, GROUPS, least * 128, most * 128, tiles * 128),
        ]
        self.chunks = 2 * GROUPS


GATHER_ORDERS = ("zyx", "zxy")
REDUCE_ORDERS = ("xyz", "yxz")


def place_of(grid, piece):
    return piece["x"] * grid.C + piece["c"], piece["z"] * grid.Y + piece["y"]


def other_core(grid, me):
    return grid.device({**me, "c": 1 - me["c"]})


def peers_of(grid, i, j):
    return [(p, j) for _, p in row_peers(grid.gx, i)] + [(i, p) for _, p in row_peers(grid.gy, j)]


class Spread:
    def __init__(self, grid, me, plan, w_ref, out, send, recv):
        self.grid, self.me, self.plan = grid, me, plan
        self.w_ref, self.out, self.send, self.recv = w_ref, out, send, recv
        self.sites = [list(gather_sites(grid, me, lane.order)) for lane in plan.lanes]

    @staticmethod
    def count(grid):
        me = {"z": 0, "y": 0, "x": 0, "c": 0}
        return max(sum(len(sends) for _, _, sends in gather_sites(grid, me, order)) for order in GATHER_ORDERS)

    @staticmethod
    def semaphores(grid, plan):
        return [
            pltpu.SemaphoreType.DMA((Spread.count(grid), plan.chunks)),
            pltpu.SemaphoreType.DMA((grid.gy, grid.gx, plan.chunks)),
        ]

    def stage(self, stage, slot, finish=False):
        for lane, sites in zip(self.plan.lanes, self.sites):
            lane.at(slot, lambda m, lane=lane, sites=sites: self.chunk(lane, sites, stage, m, finish))

    def chunk(self, lane, sites, stage, m, finish):
        number, chunk = 0, lane.first + m
        for at, piece, sends in sites:
            first = number
            number += len(sends)
            if at != stage:
                continue
            j, i = place_of(self.grid, piece)
            land = self.out.at[j, i, :, lane.columns(m)]
            src = self.w_ref.at[:, lane.columns(m)] if at == 0 else land
            arrived = self.recv.at[j, i, chunk]
            if at and not finish:
                remote(land, land, self.send.at[first, chunk], arrived, (0, 0)).wait_recv()
            for n, device in enumerate(sends):
                copy = remote(src, land, self.send.at[first + n, chunk], arrived, device)
                if finish:
                    copy.wait_send()
                else:
                    copy.start()

    def start(self):
        self.stage(0, 0)

    def slot(self, t):
        self.stage(0, t + 1)
        for stage in (1, 2, 3):
            self.stage(stage, t - (stage - 1))
        for lane in self.plan.lanes:
            lane.at(t - 2, functools.partial(self.core, lane))

    def core(self, lane, m):
        if self.grid.C == 2:
            for piece in core_sites(self.grid, self.me):
                j, i = place_of(self.grid, piece)
                land, chunk = self.out.at[j, i, :, lane.columns(m)], lane.first + m
                remote(land, land, self.send.at[0, chunk], self.recv.at[j, i, chunk], (0, 0)).wait_recv()

    def finish(self):
        def end(t, carry):
            for stage in range(4):
                self.stage(stage, t, True)
            return carry

        lax.fori_loop(0, self.plan.slots, end, 0)


class Tokens:
    def __init__(self, grid, i, j, tok, send, recv, local, pairs):
        self.grid, self.i, self.j, self.tok = grid, i, j, tok
        self.send, self.recv, self.local, self.pairs = send, recv, local, pairs

    @staticmethod
    def semaphores(grid, n):
        return [
            pltpu.SemaphoreType.DMA((n, grid.gx - 1)),
            pltpu.SemaphoreType.DMA((n, grid.gx - 1)),
            pltpu.SemaphoreType.DMA((n,)),
        ]

    def of(self, ref, p):
        return ref.at[:, pl.ds(pl.multiple_of(p * self.tok, self.tok), self.tok)]

    def own(self, n):
        pick, land = self.pairs[n]
        return pltpu.make_async_copy(pick(self, self.i), land(self, self.i), self.local.at[n])

    def start(self, n):
        pick, land = self.pairs[n]
        for d, p in row_peers(self.grid.gx, self.i):
            remote(pick(self, p), land(self, self.i), self.send.at[n, d - 1], self.recv.at[n, d - 1], (p, self.j)).start()
        self.own(n).start()

    def finish(self, n):
        pick, land = self.pairs[n]
        for d, p in row_peers(self.grid.gx, self.i):
            sems = self.send.at[n, d - 1], self.recv.at[n, d - 1]
            remote(pick(self, p), land(self, self.i), *sems, (p, self.j)).wait_send()
            back = land(self, lax.rem(self.i + self.grid.gx - d, self.grid.gx))
            remote(back, back, *sems, (p, self.j)).wait_recv()
        self.own(n).wait()


def dot(a, b, contract):
    return lax.dot_general(a, b, ((contract[:1], contract[1:]), ((), ())), preferred_element_type=F32)


def attention_bias(seg_query, seg_window):
    tok, window = seg_query.shape[0], seg_window.shape[1]
    row = lax.broadcasted_iota(jnp.int32, (tok, window), 0) + (window - tok)
    column = lax.broadcasted_iota(jnp.int32, (tok, window), 1)
    return jnp.where((seg_query == seg_window) & (column <= row), 0.0, -jnp.inf).astype(F32)


def head_rows(head):
    return pl.ds(pl.multiple_of(head * HEAD_SIZE, HEAD_SIZE), HEAD_SIZE)


def in_window(win_ref, own_ref, head):
    parts = [win_ref[n, head_rows(head), :] for n in reversed(range(win_ref.shape[0]))]
    return jnp.concatenate(parts + [own_ref[head_rows(head), :]], axis=1)


def probabilities(query, key, bias):
    scores = dot(query, key, (0, 0)) * HEAD_SIZE ** (-0.5) + bias
    raised = jnp.exp(scores - jnp.max(scores, axis=1, keepdims=True))
    return raised * (1.0 / jnp.sum(raised, axis=1, keepdims=True))


def attend(k, kv_heads, groups, q_ref, win_ref, own_ref, bias_ref, o_ref):
    key, value = in_window(win_ref, own_ref, k), in_window(win_ref, own_ref, kv_heads + k)
    for g in range(groups):
        rows = head_rows(k * groups + g)
        prob = probabilities(q_ref[rows, :], key, bias_ref[...]).astype(BF16)
        o_ref[rows, :] = dot(value, prob, (1, 1)).astype(BF16).astype(F32)


def attend_back(k, kv_heads, groups, q_ref, do_ref, win_ref, own_ref, bias_ref, dq_ref, dkv_out, dkv_own):
    key, value = in_window(win_ref, own_ref, k), in_window(win_ref, own_ref, kv_heads + k)
    key_grad = value_grad = None
    for g in range(groups):
        rows = head_rows(k * groups + g)
        query, grad = q_ref[rows, :], do_ref[rows, :]
        prob = probabilities(query, key, bias_ref[...])
        prob_grad = dot(grad, value, (0, 0))
        row_dot = jnp.sum(prob * prob_grad, axis=1, keepdims=True)
        score_grad = (prob * (prob_grad - row_dot) * HEAD_SIZE ** (-0.5)).astype(BF16)
        dq_ref[rows, :] = dot(key, score_grad, (1, 1))
        dk = dot(query, score_grad, (1, 0))
        dv = dot(grad, prob.astype(BF16), (1, 0))
        key_grad = dk if g == 0 else key_grad + dk
        value_grad = dv if g == 0 else value_grad + dv
    tok = q_ref.shape[1]
    for head, grad in ((k, key_grad), (kv_heads + k, value_grad)):
        before = dkv_out.shape[0]
        for n in range(before):
            at = before - 1 - n
            dkv_out[n, head_rows(head), :] = grad[:, at * tok : (at + 1) * tok].astype(BF16)
        dkv_own[head_rows(head), :] = grad[:, before * tok :]


def over(ref, body):
    lead = ref.shape[:-2]
    total = math.prod(lead)

    def one(k, carry):
        place = []
        for n in reversed(lead):
            place.append(k % n)
            k = k // n
        body(tuple(reversed(place)))
        return carry

    if total == 1:
        body((0,) * len(lead))
    else:
        lax.fori_loop(0, total, one, 0)


def add_into(target, source):
    def one(place):
        where = place + (slice(None), slice(None))
        target[where] = target[where] + source[where]

    over(target, one)


DIMS = "xzy"


class Collect:
    def __init__(self, grid, me, plan, acc, from_core, lands, out, c_s, c_r, c_l, l_s, l_r):
        self.grid, self.me, self.plan = grid, me, plan
        self.acc, self.from_core, self.lands, self.out = acc, from_core, lands, out
        self.c_s, self.c_r, self.c_l, self.l_s, self.l_r = c_s, c_r, c_l, l_s, l_r
        self.actions = [self.actions_of(n, lane) for n, lane in enumerate(plan.lanes)]
        self.lags = max(len(actions) for actions in self.actions)

    @staticmethod
    def axes(grid, lane):
        return [axis for axis in lane.order if grid.size[axis] > 1]

    @staticmethod
    def scratch(grid, plan, rows, cols):
        size = (grid.X, grid.Z, grid.Y, rows, cols)
        shapes = [pltpu.VMEM(size, BF16), pltpu.VMEM(size, BF16)]
        for lane in plan.lanes:
            axes = Collect.axes(grid, lane)
            for level, axis in enumerate(axes):
                rest = tuple(grid.size[d] for d in DIMS if d in axes[level + 1 :])
                shapes.append(pltpu.VMEM((grid.size[axis] - 1,) + rest + (rows, lane.count * lane.width), BF16))
        sem = pltpu.SemaphoreType.DMA
        most = max(n - 1 for n in grid.size.values())
        levels = len(shapes) - 2
        return shapes, [sem((grid.X, plan.chunks))] * 3 + [sem((levels, most, plan.chunks))] * 2

    def own_copy(self, x, lane, m, g_ref, columns):
        src, chunk = g_ref.at[x * self.grid.C + self.me["c"], :, :, :, columns], lane.first + m
        return pltpu.make_async_copy(src, self.acc.at[x, :, :, :, lane.columns(m)], self.c_l.at[x, chunk])

    def core_copy(self, x, lane, m, g_ref, columns):
        src, chunk = g_ref.at[x * self.grid.C + 1 - self.me["c"], :, :, :, columns], lane.first + m
        land = self.from_core.at[x, :, :, :, lane.columns(m)]
        return remote(src, land, self.c_s.at[x, chunk], self.c_r.at[x, chunk], other_core(self.grid, self.me))

    def start(self, source):
        self.source = source
        for slot in range(self.plan.slots - 1):
            self.load(slot)

    def load(self, slot):
        for lane in self.plan.lanes:
            ref, at = self.source(lane.base + slot * lane.step)
            for x in range(self.grid.X):
                self.own_copy(x, lane, slot, ref, pl.ds(at, lane.width)).start()
                if self.grid.C == 2:
                    self.core_copy(x, lane, slot, ref, pl.ds(at, lane.width)).start()

    def core(self, lane, m):
        columns = lane.columns(m)
        ref, _ = self.source(0)
        for x in range(self.grid.X):
            self.own_copy(x, lane, m, ref, pl.ds(0, lane.width)).wait()
            if self.grid.C == 2:
                self.core_copy(x, lane, m, ref, pl.ds(0, lane.width)).wait_recv()
                add_into(self.acc.at[x, :, :, :, columns], self.from_core.at[x, :, :, :, columns])

    def level(self, number, lane, level):
        axes = self.axes(self.grid, lane)
        axis = axes[level]
        index = sum(len(self.axes(self.grid, other)) for other in self.plan.lanes[:number]) + level
        free = len(axes) - level - 1

        def pick(t, m):
            place = []
            for d in DIMS:
                if d == axis:
                    place.append(t)
                elif d in axes[level + 1 :]:
                    place.append(slice(None))
                else:
                    place.append(self.me[d] if self.grid.size[d] > 1 else 0)
            return self.acc.at[tuple(place) + (slice(None), lane.columns(m))]

        def land(slot, m):
            return self.lands[index].at[(slot,) + (slice(None),) * (free + 1) + (lane.own_columns(m),)]

        def copies(m):
            for slot, (to, _) in enumerate(line(self.grid.size[axis], self.me[axis])):
                sems = self.l_s.at[index, slot, lane.first + m], self.l_r.at[index, slot, lane.first + m]
                yield slot, remote(pick(to, m), land(slot, m), *sems, self.grid.device({**self.me, axis: to}))

        return self.me[axis], pick, land, copies

    def actions_of(self, number, lane):
        levels = [self.level(number, lane, level) for level in range(len(self.axes(self.grid, lane)))]

        def send(m, copies):
            for _, copy in copies(m):
                copy.start()

        def take(m, p, pick, land, copies, last):
            columns = lane.columns(m)
            if last:
                self.out[:, columns] = pick(p, m)[...].astype(F32)
            for slot, copy in copies(m):
                copy.wait_recv()
                if last:
                    self.out[:, columns] += land(slot, m)[...].astype(F32)
                else:
                    add_into(pick(p, m), land(slot, m))

        actions = [[functools.partial(self.core, lane)]]
        for number, (p, pick, land, copies) in enumerate(levels):
            actions[-1].append(functools.partial(send, copies=copies))
            last = number == len(levels) - 1
            actions.append([functools.partial(take, p=p, pick=pick, land=land, copies=copies, last=last)])
        return actions

    def slot(self, t):
        for lag in range(self.lags):
            for lane, actions in zip(self.plan.lanes, self.actions):
                if lag < len(actions):
                    for action in actions[lag]:
                        lane.at_late(t - lag, action)

    def finish(self):
        def end(t, carry):
            for number, lane in enumerate(self.plan.lanes):

                def body(m, number=number, lane=lane):
                    if self.grid.C == 2:
                        ref, _ = self.source(0)
                        for x in range(self.grid.X):
                            self.core_copy(x, lane, m, ref, pl.ds(0, lane.width)).wait_send()
                    for level in range(len(self.axes(self.grid, lane))):
                        for _, copy in self.level(number, lane, level)[-1](m):
                            copy.wait_send()

                lane.at(t, body)
            return carry

        lax.fori_loop(0, self.plan.slots, end, 0)


class Shift:
    def __init__(self, span, i, j, sign, pick, land, send, recv):
        self.i, self.j, self.q, self.span, self.sign = i, j, i % span, span, sign
        self.pick, self.land, self.send, self.recv = pick, land, send, recv

    def copy(self, n):
        sems = self.send.at[n], self.recv.at[n]
        return remote(self.pick(n), self.land(n), *sems, (self.i + self.sign * (n + 1), self.j))

    def before(self, n):
        return self.q >= n + 1

    def after(self, n):
        return self.q + n + 1 < self.span

    def start(self, slots):
        for n in range(slots):
            pl.when(self.after(n) if self.sign > 0 else self.before(n))(lambda n=n: self.copy(n).start())

    def finish(self, slots, arrived, missing=None):
        for n in range(slots):
            there, goes = (self.before(n), self.after(n)) if self.sign > 0 else (self.after(n), self.before(n))

            def take(n=n):
                self.copy(n).wait_recv()
                arrived(n)

            pl.when(there)(take)
            if missing is not None:
                pl.when(jnp.logical_not(there))(lambda n=n: missing(n))
            pl.when(goes)(lambda n=n: self.copy(n).wait_send())


HBM_SPEC = pl.BlockSpec(memory_space=pl.ANY)
VMEM_SPEC = pl.BlockSpec(memory_space=pltpu.VMEM)


def params(collective_id):
    return pltpu.CompilerParams(
        collective_id=collective_id, has_side_effects=True, vmem_limit_bytes=63 * 1024 * 1024
    )


def column_of(row, size):
    n = row.shape[1]
    same = lax.broadcasted_iota(jnp.int32, (size, n), 0) == lax.broadcasted_iota(jnp.int32, (size, n), 1)
    return jnp.sum(jnp.where(same, row, 0.0), axis=1, keepdims=True)


def row_of(column, size):
    n = column.shape[0]
    same = lax.broadcasted_iota(jnp.int32, (n, size), 0) == lax.broadcasted_iota(jnp.int32, (n, size), 1)
    return jnp.sum(jnp.where(same, column, 0.0), axis=0, keepdims=True)


class Sizes:
    def __init__(self, grid, tok, rows, qc, kc):
        self.grid, self.tok, self.rows, self.qc, self.kc = grid, tok, rows, qc, kc
        self.features = rows * grid.gx
        self.q, self.kv = qc * grid.gy, kc * grid.gy
        self.heads, self.kv_heads = self.q // HEAD_SIZE, self.kv // HEAD_SIZE
        self.groups = self.heads // self.kv_heads
        self.span = PACKED_LENGTH // tok
        self.before = -(-(LONGEST_SEGMENT - 1) // tok)
        self.window = (self.before + 1) * tok
        self.qkv = qc + 2 * kc


def turn(ref, row, cos_table, sine_table, direction):
    half = HEAD_SIZE // 2
    lower = ref[pl.ds(row, half), :]
    upper = ref[pl.ds(pl.multiple_of(row + half, half), half), :]
    if direction > 0:
        lower, upper = lower.astype(BF16).astype(F32), upper.astype(BF16).astype(F32)
    return jnp.concatenate(
        [lower * cos_table - direction * upper * sine_table, upper * cos_table + direction * lower * sine_table], axis=0
    )


def first_kernel(
    sz, plan, width, row_sequences, x_ref, dy_ref, small_ref, w_ref,
    xo, dyo, wo, w_attn, smallo, xn_ref, scale_ref, q_ref, kv_ref, win, o_ref, bias, tables, gains, h_ref, xn2_ref, scale2_ref,
    raw, o_full, t_s, t_r, t_l, k_s, k_r, w_l, w_s, w_r,
):
    grid, tok = sz.grid, sz.tok
    me = grid.here()
    i, j = lax.axis_index("gx"), lax.axis_index("gy")
    greet(peers_of(grid, i, j))
    pairs = [
        (lambda c, p: small_ref, lambda c, p: smallo.at[p]),
        (lambda c, p: c.of(x_ref, p), lambda c, p: xo.at[p]),
        (lambda c, p: c.of(dy_ref, p), lambda c, p: dyo.at[p]),
    ]
    tokens = Tokens(grid, i, j, tok, t_s, t_r, t_l, pairs)
    spread = Spread(grid, me, plan, w_ref, wo, w_s, w_r)
    tokens.start(0)
    tokens.start(1)
    pltpu.make_async_copy(w_ref, wo.at[j, i], w_l.at[0]).start()
    spread.start()
    shift = Shift(sz.span, i, j, 1, lambda n: kv_ref, lambda n: win.at[n], k_s, k_r)
    sequence, q = j * row_sequences + i // sz.span, i % sz.span
    half = HEAD_SIZE // 2

    def norm(parts, scale_out, gain, out):
        total = None
        for k in range(grid.gx):
            value = parts(k)
            part = jnp.sum(value * value, axis=0, keepdims=True)
            total = part if k == 0 else total + part
        scale = lax.rsqrt(total / sz.features + EPS)
        scale_out[...] = scale
        for k in range(grid.gx):
            out[k] = (parts(k) * scale * gains[k, :, gain : gain + 1]).astype(BF16)

    def prepare():
        tokens.finish(0)
        tokens.start(2)

        def segments(place):
            row = smallo[sequence, pl.ds(jnp.maximum(place, 0), 1), :][:, :tok]
            return jnp.where(place >= 0, row, -1.0)

        here = segments(q)
        bias[...] = attention_bias(
            column_of(here, tok), jnp.concatenate([segments(q - n) for n in range(sz.before, 0, -1)] + [here], axis=1)
        )
        first = jnp.zeros((1, tok), F32)
        for n in range(sz.span):
            other = column_of(smallo[sequence, n : n + 1, :][:, :tok], tok)
            first = first + jnp.sum(jnp.where(other < here, 1.0, 0.0), axis=0, keepdims=True)
        positions = (q * tok).astype(F32) + lax.broadcasted_iota(jnp.int32, (1, tok), 1).astype(F32) - first
        frequency = jnp.exp(
            -math.log(THETA) * lax.broadcasted_iota(jnp.int32, (half, 1), 0).astype(F32) / half
        )
        angles = frequency * positions
        tables[0] = jnp.cos(angles)
        tables[1] = jnp.sin(angles)
        for k in range(grid.gx):
            columns = [column_of(smallo[k, sz.span + n : sz.span + n + 1, :][:, :tok], sz.rows) for n in range(2)]
            gains[k] = jnp.concatenate(columns, axis=1)
        tokens.finish(1)
        norm(lambda k: xo[k].astype(F32), scale_ref, 0, xn_ref)

    def project():
        pltpu.make_async_copy(w_ref, wo.at[j, i], w_l.at[0]).wait()
        copy = pltpu.make_async_copy(wo.at[:, :, :, pl.ds(0, width)], w_attn, w_l.at[0])
        copy.start()
        copy.wait()

        def column(b, carry):
            total = None
            for k in range(grid.gx):
                part = dot(w_attn[b, k][:, : sz.qkv], xn_ref[k], (0, 0))
                total = part if k == 0 else total + part
            for part, at, size in ((0, 0, sz.qc), (sz.qc, sz.q, sz.kc), (sz.qc + sz.kc, sz.q + sz.kv, sz.kc)):
                raw[pl.ds(pl.multiple_of(at + b * size, 8), size), :] = total[part : part + size]
            return carry

        lax.fori_loop(0, grid.gy, column, 0)

        def key(k, carry):
            kv_ref[head_rows(k), :] = turn(raw, pl.multiple_of(sz.q + k * HEAD_SIZE, HEAD_SIZE), tables[0], tables[1], 1).astype(BF16)
            kv_ref[head_rows(sz.kv_heads + k), :] = raw[head_rows(sz.heads + sz.kv_heads + k), :].astype(BF16)
            return carry

        lax.fori_loop(0, sz.kv_heads, key, 0)
        shift.start(sz.before)

        def query(k, carry):
            q_ref[head_rows(k), :] = turn(raw, pl.multiple_of(k * HEAD_SIZE, HEAD_SIZE), tables[0], tables[1], 1).astype(BF16)
            return carry

        lax.fori_loop(0, sz.heads, query, 0)

    def zero(n):
        win[n] = jnp.zeros(win.shape[1:], BF16)

    def mix():
        def block(k, carry):
            total = xo[k].astype(F32)
            for b in range(grid.gy):
                mixed = o_full[pl.ds(b * sz.qc, sz.qc), :].astype(BF16)
                total = total + dot(w_attn[b, k][:, sz.qkv : sz.qkv + sz.qc], mixed, (1, 0))
            h_ref[k] = total
            return carry

        lax.fori_loop(0, grid.gx, block, 0)
        norm(lambda k: h_ref[k], scale2_ref, 1, xn2_ref)
        o_ref[...] = o_full[...].astype(BF16)

    each = -(-sz.kv_heads // 2)

    def slot(t, carry):
        spread.slot(t)
        pl.when(t == 0)(prepare)
        pl.when(t == 2)(project)
        pl.when(t == 3)(lambda: shift.finish(sz.before, lambda n: None, zero))

        @pl.when((t == 3) | (t == 4))
        def _():
            def one(k, carry):
                attend(k, sz.kv_heads, sz.groups, q_ref, win, kv_ref, bias, o_full)
                return carry

            lax.fori_loop((t - 3) * each, jnp.minimum((t - 2) * each, sz.kv_heads), one, 0)

        pl.when(t == 5)(mix)
        return carry

    lax.fori_loop(0, plan.slots + 2, slot, 0)
    spread.finish()
    tokens.finish(2)


def first_half(sz, row_sequences, x, dy, small, w):
    grid, tok = sz.grid, sz.tok
    rows, cols = w.shape
    width = cols // GROUPS
    plan = Plan(cols, GATHER_ORDERS)
    parts = (grid.gx, sz.rows, tok)
    outs = [
        (parts, BF16, VMEM_SPEC),
        (parts, BF16, HBM_SPEC),
        ((grid.gy, grid.gx, rows, cols), BF16, HBM_SPEC),
        ((grid.gy, grid.gx, rows, width), BF16, VMEM_SPEC),
        ((grid.gx,) + small.shape, F32, VMEM_SPEC),
        (parts, BF16, VMEM_SPEC),
        ((1, tok), F32, VMEM_SPEC),
        ((sz.q, tok), BF16, VMEM_SPEC),
        ((2 * sz.kv, tok), BF16, VMEM_SPEC),
        ((sz.before, 2 * sz.kv, tok), BF16, VMEM_SPEC),
        ((sz.q, tok), BF16, VMEM_SPEC),
        ((tok, sz.window), F32, VMEM_SPEC),
        ((2, HEAD_SIZE // 2, tok), F32, VMEM_SPEC),
        ((grid.gx, sz.rows, 2), F32, VMEM_SPEC),
        (parts, F32, VMEM_SPEC),
        (parts, BF16, VMEM_SPEC),
        ((1, tok), F32, VMEM_SPEC),
    ]
    return pl.pallas_call(
        functools.partial(first_kernel, sz, plan, width, row_sequences),
        out_shape=[jax.ShapeDtypeStruct(shape, dtype) for shape, dtype, _ in outs],
        in_specs=[VMEM_SPEC] * 4,
        out_specs=[spec for _, _, spec in outs],
        scratch_shapes=[pltpu.VMEM((sz.q + 2 * sz.kv, tok), F32), pltpu.VMEM((sz.q, tok), F32)]
        + Tokens.semaphores(grid, 3)
        + [pltpu.SemaphoreType.DMA((sz.before,))] * 2
        + [pltpu.SemaphoreType.DMA((1,))]
        + Spread.semaphores(grid, plan),
        compiler_params=params(0),
        name="first_half",
    )(x, dy, small, w)


def last_kernel(
    sz, plan, width, both_ref, down_ref, w_attn, xo, xn_ref, scale_ref, q_ref, kv_ref, win, o_ref, bias, tables, gains,
    do_ref, dh_ref, dh_half, bo_ref, gain_two,
    bo, ig, go, gaino,
    dq, dkv_out, dkv_in, dkv, g_attn, dx, ig_parts, gain_parts, gain_in, gain_row, gain_across, acc, from_core, *refs,
):
    lands, (t_s, t_r, t_l, k_s, k_r, g_s, g_r, h_s, h_r, *sems) = refs[:-14], refs[-14:]
    grid, tok = sz.grid, sz.tok
    me = grid.here()
    i, j = lax.axis_index("gx"), lax.axis_index("gy")
    peers, across = row_peers(grid.gx, i), row_peers(grid.gy, j)
    greet(peers_of(grid, i, j))
    collect = Collect(grid, me, plan, acc, from_core, lands, go, *sems)

    def source(first):
        if first < 2 * width:
            return both_ref, first
        return (down_ref, first - 2 * width) if first < 3 * width else (g_attn, first - 3 * width)

    collect.start(source)
    pairs = [
        (lambda c, p: bo_ref.at[p], lambda c, p: c.of(bo, p)),
        (lambda c, p: ig_parts.at[p], lambda c, p: c.of(ig, p)),
    ]
    tokens = Tokens(grid, i, j, tok, t_s, t_r, t_l, pairs)
    shift = Shift(sz.span, i, j, -1, lambda n: dkv_out.at[n], lambda n: dkv_in.at[n], k_s, k_r)

    def column_copies():
        for d, p in peers:
            yield d, remote(gain_parts.at[p], gain_in.at[d - 1], g_s.at[d - 1], g_r.at[d - 1], (p, j))

    def across_copies():
        for d, p in across:
            yield d, remote(gain_row, gain_across.at[d - 1], h_s.at[d - 1], h_r.at[d - 1], (i, p))

    def heads_of(part):
        def one(k, carry):
            attend_back(k, sz.kv_heads, sz.groups, q_ref, do_ref, win, kv_ref, bias, dq, dkv_out, dkv)
            return carry

        each = -(-sz.kv_heads // 3)
        lax.fori_loop(part * each, jnp.minimum((part + 1) * each, sz.kv_heads), one, 0)

    def turn_back(ref, heads):
        def one(k, carry):
            row = pl.multiple_of(k * HEAD_SIZE, HEAD_SIZE)
            ref[head_rows(k), :] = turn(ref, row, tables[0], tables[1], -1)
            return carry

        lax.fori_loop(0, heads, one, 0)

    def back_of(b):
        parts = [
            dq[pl.ds(pl.multiple_of(b * sz.qc, 8), sz.qc), :],
            dkv[pl.ds(pl.multiple_of(b * sz.kc, 8), sz.kc), :],
            dkv[pl.ds(pl.multiple_of(sz.kv + b * sz.kc, 8), sz.kc), :],
        ]
        return jnp.concatenate(parts, axis=0).astype(BF16)

    def block_grads():
        turn_back(dq, sz.heads)

        def arrived(n):
            dkv[...] += dkv_in[n].astype(F32)

        shift.finish(sz.before, arrived)
        turn_back(dkv, sz.kv_heads)

        def column(b, carry):
            back = back_of(b)
            mixed = o_ref[pl.ds(pl.multiple_of(b * sz.qc, 8), sz.qc), :]
            for k in range(grid.gx):
                parts = [dot(xn_ref[k], back, (1, 1)), dot(dh_half[k], mixed, (1, 1))]
                left = width - sz.qkv - sz.qc
                if left:
                    parts.append(jnp.zeros((sz.rows, left), F32))
                g_attn[b, k // grid.Y, k % grid.Y] = jnp.concatenate(parts, axis=1).astype(BF16)
            return carry

        lax.fori_loop(0, grid.gy, column, 0)
        collect.load(plan.slots - 1)

    def input_grads():
        backs = [back_of(b) for b in range(grid.gy)]
        inner = None
        for k in range(grid.gx):
            total = None
            for b in range(grid.gy):
                part = dot(w_attn[b, k][:, : sz.qkv], backs[b], (1, 0))
                total = part if b == 0 else total + part
            dx[k] = total
            value = xo[k].astype(F32)
            part = jnp.sum(total * gains[k, :, 0:1] * value, axis=0, keepdims=True)
            inner = part if k == 0 else inner + part
            gain_parts[k] = gain_two[k]
            gain_parts[k, 0:1, :] = row_of(jnp.sum(total * value * scale_ref[...], axis=1, keepdims=True), 128)
        scale = scale_ref[...]
        inner = scale * scale * scale * inner / sz.features
        for k in range(grid.gx):
            value = xo[k].astype(F32)
            ig_parts[k] = (dh_ref[k] + scale * (dx[k] * gains[k, :, 0:1]) - value * inner).astype(BF16)
        tokens.start(1)
        for _, copy in column_copies():
            copy.start()

    def gain_sums():
        gain_row[...] = gain_parts[i]
        for d, copy in column_copies():
            copy.wait()
            gain_row[...] += gain_in[d - 1]
        for _, copy in across_copies():
            copy.start()

    def slot(t, carry):
        collect.slot(t)
        pl.when(t < 3)(lambda: heads_of(t))

        @pl.when(t == 2)
        def _():
            shift.start(sz.before)
            tokens.start(0)

        pl.when(t == 3)(block_grads)
        pl.when(t == 4)(input_grads)
        pl.when(t == 5)(gain_sums)
        return carry

    lax.fori_loop(0, plan.slots + collect.lags, slot, 0)
    gaino[...] = gain_row[...]
    for d, copy in across_copies():
        copy.wait()
        gaino[...] += gain_across[d - 1]
    tokens.finish(0)
    tokens.finish(1)
    collect.finish()


def last_half(sz, both, down, w_attn, kept, do, dh, dh_half, bo, gain_two):
    grid, tok = sz.grid, sz.tok
    rows, width = w_attn.shape[-2:]
    cols = GROUPS * width
    plan = Plan(cols, REDUCE_ORDERS)
    shapes, sems = Collect.scratch(grid, plan, rows, cols)
    sem = pltpu.SemaphoreType.DMA
    parts = (grid.gx, sz.rows, tok)
    shape = lambda g: g.reshape(grid.gy, grid.Z, grid.Y, rows, -1)
    return pl.pallas_call(
        functools.partial(last_kernel, sz, plan, width),
        out_shape=[
            jax.ShapeDtypeStruct((sz.rows, grid.gx * tok), BF16),
            jax.ShapeDtypeStruct((sz.rows, grid.gx * tok), BF16),
            jax.ShapeDtypeStruct((rows, cols), F32),
            jax.ShapeDtypeStruct((8, 128), F32),
        ],
        in_specs=[HBM_SPEC] * 2 + [VMEM_SPEC] * 16,
        out_specs=[VMEM_SPEC] * 4,
        scratch_shapes=[
            pltpu.VMEM((sz.q, tok), F32),
            pltpu.VMEM((sz.before, 2 * sz.kv, tok), BF16),
            pltpu.VMEM((sz.before, 2 * sz.kv, tok), BF16),
            pltpu.VMEM((2 * sz.kv, tok), F32),
            pltpu.VMEM((grid.gy, grid.Z, grid.Y, rows, width), BF16),
            pltpu.VMEM(parts, F32),
            pltpu.VMEM(parts, BF16),
            pltpu.VMEM((grid.gx, 8, 128), F32),
            pltpu.VMEM((grid.gx - 1, 8, 128), F32),
            pltpu.VMEM((8, 128), F32),
            pltpu.VMEM((grid.gy - 1, 8, 128), F32),
        ]
        + shapes
        + Tokens.semaphores(grid, 2)
        + [sem((sz.before,))] * 2
        + [sem((grid.gx - 1,))] * 2
        + [sem((grid.gy - 1,))] * 2
        + sems,
        compiler_params=params(1),
        name="last_half",
    )(shape(both), shape(down), w_attn, *kept, do, dh, dh_half, bo, gain_two)


def einsum(form, a, b):
    return jnp.einsum(form, a, b, preferred_element_type=F32)


def padded(a, axis, size):
    pads = [(0, 0)] * a.ndim
    pads[axis] = (0, size - a.shape[axis])
    return jnp.pad(a, pads) if size != a.shape[axis] else a


def norm_backward(values, scale, gain, grad):
    weighted = grad * gain[:, None]
    inner = jnp.sum(weighted * values, axis=0) / values.shape[0]
    back = scale * weighted - values * (scale * scale * scale * inner)
    return back, jnp.sum(grad * values * scale, axis=1)


def shards(
    grid,
    block_input,
    attn_gain,
    query_weight,
    key_weight,
    value_weight,
    output_weight,
    ffn_gain,
    gate_weight,
    up_weight,
    down_weight,
    segment_ids,
    out_cotangent,
):
    GX, GY = grid.gx, grid.gy
    rows, row_tokens = block_input.shape
    tok = row_tokens // GX
    sz = Sizes(grid, tok, rows, query_weight.shape[1], key_weight.shape[1])
    fc, features = gate_weight.shape[1], sz.features
    groups = [
        jnp.concatenate([query_weight, key_weight, value_weight, output_weight.T], axis=1), gate_weight, up_weight, down_weight.T
    ]
    width = -(-max(g.shape[1] for g in groups) // 128) * 128
    block = jnp.concatenate([padded(g, 1, width) for g in groups], axis=1)
    small = jnp.concatenate(
        [segment_ids.reshape(sz.span, tok).astype(F32), padded(jnp.stack([attn_gain, ffn_gain]), 1, tok)], axis=0
    )
    small = padded(small, 0, -(-small.shape[0] // 8) * 8)
    (
        x_parts, dy_parts, w_all, w_attn, _, normed_one, scale_one, query, key_value, earlier, mixed, bias, tables, gains,
        hidden_in, normed_two, scale_two,
    ) = first_half(sz, row_tokens // PACKED_LENGTH, block_input, out_cotangent, small, block)
    dy_half = dy_parts.reshape(features, tok)
    w_all = w_all.reshape(GY, features, -1)
    w_gate, w_up, w_down = (w_all[:, :, k * width : k * width + fc] for k in range(1, 4))
    w_out = w_attn.reshape(GY, features, -1)[:, :, sz.qkv : sz.qkv + sz.qc]
    hidden_in, normed_two = hidden_in.reshape(features, tok), normed_two.reshape(features, tok)
    scale_two, gain_two = scale_two[0], gains[:, :, 1].reshape(features)

    gate = einsum("dt,jdf->jtf", normed_two, w_gate)
    up = einsum("dt,jdf->jtf", normed_two, w_up)
    sigmoid = jax.nn.sigmoid(gate)
    hidden = (jax.nn.silu(gate) * up).astype(BF16)
    block_output = (hidden_in + einsum("jdf,jtf->dt", w_down, hidden)).astype(BF16)
    hidden_grad = einsum("dt,jdf->jtf", dy_half, w_down)
    gate_back = (hidden_grad * up * sigmoid * (1.0 + gate * (1.0 - sigmoid))).astype(BF16)
    up_back = (hidden_grad * gate * sigmoid).astype(BF16)
    both_back = jnp.concatenate([padded(gate_back, 2, width), padded(up_back, 2, width)], axis=2)
    grad_both = einsum("dt,jtf->jdf", normed_two, both_back).astype(BF16)
    grad_down = padded(einsum("dt,jtf->jdf", dy_half, hidden).astype(BF16), 2, width)
    normed_two_grad = einsum("jdf,jtf->dt", w_all[:, :, width : 3 * width], both_back)
    hidden_in_grad, gain_two_part = norm_backward(hidden_in, scale_two, gain_two, normed_two_grad)
    hidden_in_grad = hidden_in_grad + dy_half.astype(F32)
    hidden_in_half = hidden_in_grad.astype(BF16)
    head_grad = einsum("jdc,dt->jct", w_out, hidden_in_half).astype(BF16).reshape(-1, tok)

    gain_part = jnp.pad(gain_two_part.reshape(GX, 1, rows), ((0, 0), (1, 6), (0, 128 - rows)))
    parts = (GX, rows, tok)
    block_output, input_grad, grads, gains = last_half(
        sz, grad_both, grad_down, w_attn,
        (x_parts, normed_one, scale_one, query, key_value, earlier, mixed, bias, tables, gains),
        head_grad, hidden_in_grad.reshape(parts), hidden_in_half.reshape(parts), block_output.reshape(parts), gain_part,
    )
    grad_gate, grad_up, grad_down, grad_attn = (grads[:, k * width : (k + 1) * width] for k in range(GROUPS))
    qc, kc = sz.qc, sz.kc
    return (
        block_output,
        input_grad.astype(F32),
        gains[0, :rows],
        grad_attn[:, :qc],
        grad_attn[:, qc : qc + kc],
        grad_attn[:, qc + kc : sz.qkv],
        grad_attn[:, sz.qkv : sz.qkv + qc].T,
        gains[1, :rows],
        grad_gate[:, :fc],
        grad_up[:, :fc],
        grad_down[:, :fc].T,
    )


def solution(mesh):
    grid = Grid(mesh.shape["gx"], mesh.shape["gy"])
    return jax.shard_map(
        functools.partial(shards, grid),
        mesh=mesh,
        in_specs=(
            P("gx", "gy"),
            P("gx"),
            P("gx", "gy"),
            P("gx", "gy"),
            P("gx", "gy"),
            P("gy", "gx"),
            P("gx"),
            P("gx", "gy"),
            P("gx", "gy"),
            P("gy", "gx"),
            P("gx", None),
            P("gx", "gy"),
        ),
        out_specs=(
            P("gx", "gy"),
            P("gx", "gy"),
            P("gx"),
            P("gx", "gy"),
            P("gx", "gy"),
            P("gx", "gy"),
            P("gy", "gx"),
            P("gx"),
            P("gx", "gy"),
            P("gx", "gy"),
            P("gy", "gx"),
        ),
        check_vma=False,
    )
```

```python
import functools
import math

import jax
import jax.numpy as jnp
from jax import lax
from jax.experimental import pallas as pl
from jax.experimental.pallas import tpu as pltpu
from jax.sharding import PartitionSpec as P

QUERY_HEADS = 15
KEY_VALUE_HEADS = 5
HEAD_SIZE = 64
PACKED_LENGTH = 1024
LONGEST_SEGMENT = 512

EPS = 1e-05
THETA = 10000.0
MESH = pl.DeviceIdType.MESH
F32 = jnp.float32
BF16 = jnp.bfloat16


class Grid:
    def __init__(self, gx, gy):
        self.gx, self.gy = gx, gy
        self.C = 2 if gy % 2 == 0 else 1
        self.X = gy // self.C
        self.Y = self.X if gx % self.X == 0 else 1
        self.Z = gx // self.Y
        self.size = {"z": self.Z, "y": self.Y, "x": self.X}

    def here(self):
        i, j = lax.axis_index("gx"), lax.axis_index("gy")
        return {"z": i // self.Y, "y": i % self.Y, "x": j // self.C, "c": j % self.C}

    def device(self, at):
        return (at["z"] * self.Y + at["y"], at["x"] * self.C + at["c"])


def remote(src, dst, send, recv, device):
    return pltpu.make_async_remote_copy(
        src_ref=src, dst_ref=dst, send_sem=send, recv_sem=recv, device_id=device, device_id_type=MESH
    )


def greet(devices):
    barrier = pltpu.get_barrier_semaphore()
    for device in devices:
        pl.semaphore_signal(barrier, inc=1, device_id=device, device_id_type=MESH)
    pl.semaphore_wait(barrier, len(devices))


def row_peers(n, me):
    return [(d, lax.rem(me + d, n)) for d in range(1, n)]


def line(n, here):
    found = []
    for k in range(1, n):
        if n & (n - 1):
            found.append((lax.rem(here + k, n), lax.rem(here + n - k, n)))
            continue
        place, bit = 0, 1
        while bit < n:
            digit = (here // bit) % 2
            place = place + bit * ((1 - digit) if k & bit else digit)
            bit *= 2
        found.append((place, place))
    return found


def places(n, here):
    return [here] + [origin for _, origin in line(n, here)]


def gather_sites(grid, me, order):
    other = [grid.device({**me, "c": 1 - me["c"]})] if grid.C == 2 else []
    onward = [[grid.device({**me, axis: to}) for to, _ in line(grid.size[axis], me[axis])] for axis in order]
    yield 0, dict(me), sum(onward, []) + other
    for stage, axis in enumerate(order, 1):
        earlier = [dict(me)]
        for done in order[: stage - 1]:
            earlier = [{**e, done: place} for place in places(grid.size[done], me[done]) for e in earlier]
        for _, origin in line(grid.size[axis], me[axis]):
            for e in earlier:
                yield stage, {**e, axis: origin}, sum(onward[stage:], []) + other


def core_sites(grid, me):
    found = [{"c": 1 - me["c"]}]
    for axis in "xyz":
        found = [{**f, axis: place} for place in places(grid.size[axis], me[axis]) for f in found]
    return found


GROUPS = 4


class Lane:
    def __init__(self, order, first, part, parts, width, base, step):
        self.order, self.first, self.part, self.parts, self.width = order, first, part, parts, width
        self.base, self.step, self.count = base, step, GROUPS

    def columns(self, m):
        return pl.ds(pl.multiple_of(self.base + m * self.step, 128), self.width)

    def own_columns(self, m):
        return pl.ds(pl.multiple_of(m * self.width, 128), self.width)

    def at(self, slot, body):
        slots = self.count * self.parts
        if isinstance(slot, int):
            if 0 <= slot < slots and slot % self.parts == self.part:
                body(slot // self.parts)
            return
        active = (slot >= 0) & (slot < slots)
        if self.parts > 1:
            active = active & (slot % self.parts == self.part)
        pl.when(active)(lambda: body(slot // self.parts))


class Plan:
    def __init__(self, cols, orders, parts):
        tiles = cols // 128 // GROUPS
        most = -(-tiles * 3 // 5)
        self.lanes, self.parts, self.slots, at = [], parts, GROUPS * parts, 0
        for part in range(parts):
            for order, total in zip(orders, (most, tiles - most)):
                width = total // parts + (part < total % parts)
                if width:
                    self.lanes.append(Lane(order, GROUPS * len(self.lanes), part, parts, width * 128, at * 128, tiles * 128))
                    at += width
        self.chunks = GROUPS * len(self.lanes)


GATHER_ORDERS = ("zyx", "zxy")
REDUCE_ORDERS = ("xyz", "yxz")
GATHER_PARTS, REDUCE_PARTS = 1, 1


def place_of(grid, piece):
    return piece["x"] * grid.C + piece["c"], piece["z"] * grid.Y + piece["y"]


def other_core(grid, me):
    return grid.device({**me, "c": 1 - me["c"]})


def peers_of(grid, i, j):
    return [(p, j) for _, p in row_peers(grid.gx, i)] + [(i, p) for _, p in row_peers(grid.gy, j)]


class Spread:
    def __init__(self, grid, me, plan, w_ref, out, send, recv):
        self.grid, self.me, self.plan = grid, me, plan
        self.w_ref, self.out, self.send, self.recv = w_ref, out, send, recv
        self.sites = [list(gather_sites(grid, me, lane.order)) for lane in plan.lanes]

    @staticmethod
    def count(grid):
        me = {"z": 0, "y": 0, "x": 0, "c": 0}
        return max(sum(len(sends) for _, _, sends in gather_sites(grid, me, order)) for order in GATHER_ORDERS)

    @staticmethod
    def semaphores(grid, plan):
        return [
            pltpu.SemaphoreType.DMA((Spread.count(grid), plan.chunks)),
            pltpu.SemaphoreType.DMA((grid.gy, grid.gx, plan.chunks)),
        ]

    def stage(self, stage, slot, finish=False):
        for lane, sites in zip(self.plan.lanes, self.sites):
            lane.at(slot, lambda m, lane=lane, sites=sites: self.chunk(lane, sites, stage, m, finish))

    def chunk(self, lane, sites, stage, m, finish):
        number, chunk = 0, lane.first + m
        for at, piece, sends in sites:
            first = number
            number += len(sends)
            if at != stage:
                continue
            j, i = place_of(self.grid, piece)
            land = self.out.at[j, i, :, lane.columns(m)]
            src = self.w_ref.at[:, lane.columns(m)] if at == 0 else land
            arrived = self.recv.at[j, i, chunk]
            if at and not finish:
                remote(land, land, self.send.at[first, chunk], arrived, (0, 0)).wait_recv()
            for n, device in enumerate(sends):
                copy = remote(src, land, self.send.at[first + n, chunk], arrived, device)
                if finish:
                    copy.wait_send()
                else:
                    copy.start()

    def start(self):
        self.stage(0, 0)
        self.stage(0, 1)

    def slot(self, t):
        self.stage(0, t + 2)
        for stage in (1, 2, 3):
            self.stage(stage, t - (stage - 1))
        for lane in self.plan.lanes:
            lane.at(t - 2, functools.partial(self.core, lane))

    def core(self, lane, m):
        if self.grid.C == 2:
            for piece in core_sites(self.grid, self.me):
                j, i = place_of(self.grid, piece)
                land, chunk = self.out.at[j, i, :, lane.columns(m)], lane.first + m
                remote(land, land, self.send.at[0, chunk], self.recv.at[j, i, chunk], (0, 0)).wait_recv()

    def finish(self):
        def end(t, carry):
            for stage in range(4):
                self.stage(stage, t, True)
            return carry

        lax.fori_loop(0, self.plan.slots, end, 0)


class Tokens:
    def __init__(self, grid, i, j, tok, send, recv, local, pairs):
        self.grid, self.i, self.j, self.tok = grid, i, j, tok
        self.send, self.recv, self.local, self.pairs = send, recv, local, pairs

    @staticmethod
    def semaphores(grid, n):
        return [
            pltpu.SemaphoreType.DMA((n, grid.gx - 1)),
            pltpu.SemaphoreType.DMA((n, grid.gx - 1)),
            pltpu.SemaphoreType.DMA((n,)),
        ]

    def of(self, ref, p):
        return ref.at[:, pl.ds(pl.multiple_of(p * self.tok, self.tok), self.tok)]

    def own(self, n):
        pick, land = self.pairs[n]
        return pltpu.make_async_copy(pick(self, self.i), land(self, self.i), self.local.at[n])

    def start(self, n):
        pick, land = self.pairs[n]
        for d, p in row_peers(self.grid.gx, self.i):
            remote(pick(self, p), land(self, self.i), self.send.at[n, d - 1], self.recv.at[n, d - 1], (p, self.j)).start()
        self.own(n).start()

    def finish(self, n):
        pick, land = self.pairs[n]
        for d, p in row_peers(self.grid.gx, self.i):
            sems = self.send.at[n, d - 1], self.recv.at[n, d - 1]
            remote(pick(self, p), land(self, self.i), *sems, (p, self.j)).wait_send()
            back = land(self, lax.rem(self.i + self.grid.gx - d, self.grid.gx))
            remote(back, back, *sems, (p, self.j)).wait_recv()
        self.own(n).wait()


def dot(a, b, contract):
    return lax.dot_general(a, b, ((contract[:1], contract[1:]), ((), ())), preferred_element_type=F32)


def attention_bias(seg_query, seg_window):
    tok, window = seg_query.shape[0], seg_window.shape[1]
    row = lax.broadcasted_iota(jnp.int32, (tok, window), 0) + (window - tok)
    column = lax.broadcasted_iota(jnp.int32, (tok, window), 1)
    return jnp.where((seg_query == seg_window) & (column <= row), 0.0, -jnp.inf).astype(F32)


def head_rows(head):
    return pl.ds(pl.multiple_of(head * HEAD_SIZE, HEAD_SIZE), HEAD_SIZE)


def in_window(win_ref, own_ref, head):
    parts = [win_ref[n, head_rows(head), :] for n in reversed(range(win_ref.shape[0]))]
    return jnp.concatenate(parts + [own_ref[head_rows(head), :]], axis=1)


def probabilities(query, key, bias):
    scores = dot(query, key, (0, 0)) * HEAD_SIZE ** (-0.5) + bias
    raised = jnp.exp(scores - jnp.max(scores, axis=1, keepdims=True))
    return raised * (1.0 / jnp.sum(raised, axis=1, keepdims=True))


def attend(k, kv_heads, groups, q_ref, win_ref, own_ref, bias_ref, o_ref):
    key, value = in_window(win_ref, own_ref, k), in_window(win_ref, own_ref, kv_heads + k)
    for g in range(groups):
        rows = head_rows(k * groups + g)
        prob = probabilities(q_ref[rows, :], key, bias_ref[...]).astype(BF16)
        o_ref[rows, :] = dot(value, prob, (1, 1)).astype(BF16).astype(F32)


def attend_back(k, kv_heads, groups, q_ref, do_ref, win_ref, own_ref, bias_ref, dq_ref, dkv_out, dkv_own):
    key, value = in_window(win_ref, own_ref, k), in_window(win_ref, own_ref, kv_heads + k)
    key_grad = value_grad = None
    for g in range(groups):
        rows = head_rows(k * groups + g)
        query, grad = q_ref[rows, :], do_ref[rows, :]
        prob = probabilities(query, key, bias_ref[...])
        prob_grad = dot(grad, value, (0, 0))
        row_dot = jnp.sum(prob * prob_grad, axis=1, keepdims=True)
        score_grad = (prob * (prob_grad - row_dot) * HEAD_SIZE ** (-0.5)).astype(BF16)
        dq_ref[rows, :] = dot(key, score_grad, (1, 1))
        dk = dot(query, score_grad, (1, 0))
        dv = dot(grad, prob.astype(BF16), (1, 0))
        key_grad = dk if g == 0 else key_grad + dk
        value_grad = dv if g == 0 else value_grad + dv
    tok = q_ref.shape[1]
    for head, grad in ((k, key_grad), (kv_heads + k, value_grad)):
        before = dkv_out.shape[0]
        for n in range(before):
            at = before - 1 - n
            dkv_out[n, head_rows(head), :] = grad[:, at * tok : (at + 1) * tok].astype(BF16)
        dkv_own[head_rows(head), :] = grad[:, before * tok :]


def over(ref, body):
    lead = ref.shape[:-2]
    total = math.prod(lead)

    def one(k, carry):
        place = []
        for n in reversed(lead):
            place.append(k % n)
            k = k // n
        body(tuple(reversed(place)))
        return carry

    if total == 1:
        body((0,) * len(lead))
    else:
        lax.fori_loop(0, total, one, 0)


def add_into(target, source):
    def one(place):
        where = place + (slice(None), slice(None))
        target[where] = target[where] + source[where]

    over(target, one)


DIMS = "xzy"


class Collect:
    def __init__(self, grid, me, plan, acc, from_core, lands, out, c_s, c_r, c_l, l_s, l_r):
        self.grid, self.me, self.plan = grid, me, plan
        self.acc, self.from_core, self.lands, self.out = acc, from_core, lands, out
        self.c_s, self.c_r, self.c_l, self.l_s, self.l_r = c_s, c_r, c_l, l_s, l_r
        self.actions = [self.actions_of(n, lane) for n, lane in enumerate(plan.lanes)]
        self.lags = max(len(actions) for actions in self.actions)

    @staticmethod
    def axes(grid, lane):
        return [axis for axis in lane.order if grid.size[axis] > 1]

    @staticmethod
    def scratch(grid, plan, rows, cols):
        size = (grid.X, grid.Z, grid.Y, rows, cols)
        shapes = [pltpu.VMEM(size, BF16), pltpu.VMEM(size, BF16)]
        for lane in plan.lanes:
            axes = Collect.axes(grid, lane)
            for level, axis in enumerate(axes):
                rest = tuple(grid.size[d] for d in DIMS if d in axes[level + 1 :])
                shapes.append(pltpu.VMEM((grid.size[axis] - 1,) + rest + (rows, lane.count * lane.width), BF16))
        sem = pltpu.SemaphoreType.DMA
        most = max(n - 1 for n in grid.size.values())
        levels = len(shapes) - 2
        return shapes, [sem((grid.X, plan.chunks))] * 3 + [sem((levels, most, plan.chunks))] * 2

    def own_copy(self, x, lane, m, g_ref, columns):
        src, chunk = g_ref.at[x * self.grid.C + self.me["c"], :, :, :, columns], lane.first + m
        return pltpu.make_async_copy(src, self.acc.at[x, :, :, :, lane.columns(m)], self.c_l.at[x, chunk])

    def core_copy(self, x, lane, m, g_ref, columns):
        src, chunk = g_ref.at[x * self.grid.C + 1 - self.me["c"], :, :, :, columns], lane.first + m
        land = self.from_core.at[x, :, :, :, lane.columns(m)]
        return remote(src, land, self.c_s.at[x, chunk], self.c_r.at[x, chunk], other_core(self.grid, self.me))

    def start(self, source):
        self.source = source
        for slot in range(self.plan.slots - self.plan.parts):
            self.load(slot)

    def load(self, slot):
        for lane in self.plan.lanes:

            def body(m, lane=lane):
                ref, at = self.source(lane.base + m * lane.step)
                for x in range(self.grid.X):
                    self.own_copy(x, lane, m, ref, pl.ds(at, lane.width)).start()
                    if self.grid.C == 2:
                        self.core_copy(x, lane, m, ref, pl.ds(at, lane.width)).start()

            lane.at(slot, body)

    def core(self, lane, m):
        columns = lane.columns(m)
        ref, _ = self.source(0)
        for x in range(self.grid.X):
            self.own_copy(x, lane, m, ref, pl.ds(0, lane.width)).wait()
            if self.grid.C == 2:
                self.core_copy(x, lane, m, ref, pl.ds(0, lane.width)).wait_recv()
                add_into(self.acc.at[x, :, :, :, columns], self.from_core.at[x, :, :, :, columns])

    def level(self, number, lane, level):
        axes = self.axes(self.grid, lane)
        axis = axes[level]
        index = sum(len(self.axes(self.grid, other)) for other in self.plan.lanes[:number]) + level
        free = len(axes) - level - 1

        def pick(t, m):
            place = []
            for d in DIMS:
                if d == axis:
                    place.append(t)
                elif d in axes[level + 1 :]:
                    place.append(slice(None))
                else:
                    place.append(self.me[d] if self.grid.size[d] > 1 else 0)
            return self.acc.at[tuple(place) + (slice(None), lane.columns(m))]

        def land(slot, m):
            return self.lands[index].at[(slot,) + (slice(None),) * (free + 1) + (lane.own_columns(m),)]

        def copies(m):
            for slot, (to, _) in enumerate(line(self.grid.size[axis], self.me[axis])):
                sems = self.l_s.at[index, slot, lane.first + m], self.l_r.at[index, slot, lane.first + m]
                yield slot, remote(pick(to, m), land(slot, m), *sems, self.grid.device({**self.me, axis: to}))

        return self.me[axis], pick, land, copies

    def actions_of(self, number, lane):
        levels = [self.level(number, lane, level) for level in range(len(self.axes(self.grid, lane)))]

        def send(m, copies):
            for _, copy in copies(m):
                copy.start()

        def take(m, p, pick, land, copies, last):
            columns = lane.columns(m)
            if last:
                self.out[:, columns] = pick(p, m)[...].astype(F32)
            for slot, copy in copies(m):
                copy.wait_recv()
                if last:
                    self.out[:, columns] += land(slot, m)[...].astype(F32)
                else:
                    add_into(pick(p, m), land(slot, m))

        actions = [[functools.partial(self.core, lane)]]
        for number, (p, pick, land, copies) in enumerate(levels):
            actions[-1].append(functools.partial(send, copies=copies))
            last = number == len(levels) - 1
            actions.append([functools.partial(take, p=p, pick=pick, land=land, copies=copies, last=last)])
        return actions

    def begin(self, slot):
        for lane, actions in zip(self.plan.lanes, self.actions):
            for action in actions[0]:
                lane.at(slot, action)

    def slot(self, t):
        for lag in range(1, self.lags):
            for lane, actions in zip(self.plan.lanes, self.actions):
                if lag < len(actions):
                    for action in actions[lag]:
                        lane.at(t - lag, action)

    def finish(self):
        def end(t, carry):
            for number, lane in enumerate(self.plan.lanes):

                def body(m, number=number, lane=lane):
                    if self.grid.C == 2:
                        ref, _ = self.source(0)
                        for x in range(self.grid.X):
                            self.core_copy(x, lane, m, ref, pl.ds(0, lane.width)).wait_send()
                    for level in range(len(self.axes(self.grid, lane))):
                        for _, copy in self.level(number, lane, level)[-1](m):
                            copy.wait_send()

                lane.at(t, body)
            return carry

        lax.fori_loop(0, self.plan.slots, end, 0)


class Shift:
    def __init__(self, span, i, j, sign, pick, land, send, recv):
        self.i, self.j, self.q, self.span, self.sign = i, j, i % span, span, sign
        self.pick, self.land, self.send, self.recv = pick, land, send, recv

    def copy(self, n):
        sems = self.send.at[n], self.recv.at[n]
        return remote(self.pick(n), self.land(n), *sems, (self.i + self.sign * (n + 1), self.j))

    def before(self, n):
        return self.q >= n + 1

    def after(self, n):
        return self.q + n + 1 < self.span

    def start(self, slots):
        for n in range(slots):
            pl.when(self.after(n) if self.sign > 0 else self.before(n))(lambda n=n: self.copy(n).start())

    def finish(self, slots, arrived, missing=None):
        for n in range(slots):
            there, goes = (self.before(n), self.after(n)) if self.sign > 0 else (self.after(n), self.before(n))

            def take(n=n):
                self.copy(n).wait_recv()
                arrived(n)

            pl.when(there)(take)
            if missing is not None:
                pl.when(jnp.logical_not(there))(lambda n=n: missing(n))
            pl.when(goes)(lambda n=n: self.copy(n).wait_send())


HBM_SPEC = pl.BlockSpec(memory_space=pl.ANY)
VMEM_SPEC = pl.BlockSpec(memory_space=pltpu.VMEM)


def params(collective_id):
    return pltpu.CompilerParams(
        collective_id=collective_id, has_side_effects=True, vmem_limit_bytes=63 * 1024 * 1024
    )


def column_of(row, size):
    n = row.shape[1]
    same = lax.broadcasted_iota(jnp.int32, (size, n), 0) == lax.broadcasted_iota(jnp.int32, (size, n), 1)
    return jnp.sum(jnp.where(same, row, 0.0), axis=1, keepdims=True)


def row_of(column, size):
    n = column.shape[0]
    same = lax.broadcasted_iota(jnp.int32, (n, size), 0) == lax.broadcasted_iota(jnp.int32, (n, size), 1)
    return jnp.sum(jnp.where(same, column, 0.0), axis=0, keepdims=True)


class Sizes:
    def __init__(self, grid, tok, rows, qc, kc):
        self.grid, self.tok, self.rows, self.qc, self.kc = grid, tok, rows, qc, kc
        self.features = rows * grid.gx
        self.q, self.kv = qc * grid.gy, kc * grid.gy
        self.heads, self.kv_heads = self.q // HEAD_SIZE, self.kv // HEAD_SIZE
        self.groups = self.heads // self.kv_heads
        self.span = PACKED_LENGTH // tok
        self.before = -(-(LONGEST_SEGMENT - 1) // tok)
        self.window = (self.before + 1) * tok
        self.qkv = qc + 2 * kc


def turn(ref, row, cos_table, sine_table, direction):
    half = HEAD_SIZE // 2
    lower = ref[pl.ds(row, half), :]
    upper = ref[pl.ds(pl.multiple_of(row + half, half), half), :]
    if direction > 0:
        lower, upper = lower.astype(BF16).astype(F32), upper.astype(BF16).astype(F32)
    return jnp.concatenate(
        [lower * cos_table - direction * upper * sine_table, upper * cos_table + direction * lower * sine_table], axis=0
    )


def first_kernel(
    sz, plan, width, row_sequences, x_ref, dy_ref, small_ref, w_ref,
    xo, dyo, wo, w_attn, smallo, xn_ref, scale_ref, q_ref, kv_ref, win, o_ref, bias, tables, gains, h_ref, xn2_ref, scale2_ref,
    raw, o_full, t_s, t_r, t_l, k_s, k_r, w_l, w_s, w_r,
):
    grid, tok = sz.grid, sz.tok
    me = grid.here()
    i, j = lax.axis_index("gx"), lax.axis_index("gy")
    greet(peers_of(grid, i, j))
    pairs = [
        (lambda c, p: small_ref, lambda c, p: smallo.at[p]),
        (lambda c, p: c.of(x_ref, p), lambda c, p: xo.at[p]),
        (lambda c, p: c.of(dy_ref, p), lambda c, p: dyo.at[p]),
    ]
    tokens = Tokens(grid, i, j, tok, t_s, t_r, t_l, pairs)
    spread = Spread(grid, me, plan, w_ref, wo, w_s, w_r)
    tokens.start(0)
    spread.start()
    tokens.start(1)
    pltpu.make_async_copy(w_ref, wo.at[j, i], w_l.at[0]).start()
    shift = Shift(sz.span, i, j, 1, lambda n: kv_ref, lambda n: win.at[n], k_s, k_r)
    sequence, q = j * row_sequences + i // sz.span, i % sz.span
    half = HEAD_SIZE // 2

    def norm(parts, scale_out, gain, out):
        total = None
        for k in range(grid.gx):
            value = parts(k)
            part = jnp.sum(value * value, axis=0, keepdims=True)
            total = part if k == 0 else total + part
        scale = lax.rsqrt(total / sz.features + EPS)
        scale_out[...] = scale
        for k in range(grid.gx):
            out[k] = (parts(k) * scale * gains[k, :, gain : gain + 1]).astype(BF16)

    def prepare():
        tokens.finish(0)

        def segments(place):
            row = smallo[sequence, pl.ds(jnp.maximum(place, 0), 1), :][:, :tok]
            return jnp.where(place >= 0, row, -1.0)

        here = segments(q)
        bias[...] = attention_bias(
            column_of(here, tok), jnp.concatenate([segments(q - n) for n in range(sz.before, 0, -1)] + [here], axis=1)
        )
        first = jnp.zeros((1, tok), F32)
        for n in range(sz.span):
            other = column_of(smallo[sequence, n : n + 1, :][:, :tok], tok)
            first = first + jnp.sum(jnp.where(other < here, 1.0, 0.0), axis=0, keepdims=True)
        positions = (q * tok).astype(F32) + lax.broadcasted_iota(jnp.int32, (1, tok), 1).astype(F32) - first
        frequency = jnp.exp(
            -math.log(THETA) * lax.broadcasted_iota(jnp.int32, (half, 1), 0).astype(F32) / half
        )
        angles = frequency * positions
        tables[0] = jnp.cos(angles)
        tables[1] = jnp.sin(angles)
        for k in range(grid.gx):
            columns = [column_of(smallo[k, sz.span + n : sz.span + n + 1, :][:, :tok], sz.rows) for n in range(2)]
            gains[k] = jnp.concatenate(columns, axis=1)

    def first_norm():
        tokens.finish(1)
        norm(lambda k: xo[k].astype(F32), scale_ref, 0, xn_ref)

    def project():
        pltpu.make_async_copy(w_ref, wo.at[j, i], w_l.at[0]).wait()
        copy = pltpu.make_async_copy(wo.at[:, :, :, pl.ds(0, width)], w_attn, w_l.at[0])
        copy.start()
        copy.wait()

        def column(b, carry):
            total = None
            for k in range(grid.gx):
                part = dot(w_attn[b, k][:, : sz.qkv], xn_ref[k], (0, 0))
                total = part if k == 0 else total + part
            for part, at, size in ((0, 0, sz.qc), (sz.qc, sz.q, sz.kc), (sz.qc + sz.kc, sz.q + sz.kv, sz.kc)):
                raw[pl.ds(pl.multiple_of(at + b * size, 8), size), :] = total[part : part + size]
            return carry

        lax.fori_loop(0, grid.gy, column, 0)

        def key(k, carry):
            kv_ref[head_rows(k), :] = turn(raw, pl.multiple_of(sz.q + k * HEAD_SIZE, HEAD_SIZE), tables[0], tables[1], 1).astype(BF16)
            kv_ref[head_rows(sz.kv_heads + k), :] = raw[head_rows(sz.heads + sz.kv_heads + k), :].astype(BF16)
            return carry

        lax.fori_loop(0, sz.kv_heads, key, 0)
        shift.start(sz.before)

        def query(k, carry):
            q_ref[head_rows(k), :] = turn(raw, pl.multiple_of(k * HEAD_SIZE, HEAD_SIZE), tables[0], tables[1], 1).astype(BF16)
            return carry

        lax.fori_loop(0, sz.heads, query, 0)

    def zero(n):
        win[n] = jnp.zeros(win.shape[1:], BF16)

    def mix():
        def block(k, carry):
            total = xo[k].astype(F32)
            for b in range(grid.gy):
                mixed = o_full[pl.ds(b * sz.qc, sz.qc), :].astype(BF16)
                total = total + dot(w_attn[b, k][:, sz.qkv : sz.qkv + sz.qc], mixed, (1, 0))
            h_ref[k] = total
            return carry

        lax.fori_loop(0, grid.gx, block, 0)
        norm(lambda k: h_ref[k], scale2_ref, 1, xn2_ref)
        o_ref[...] = o_full[...].astype(BF16)

    each = -(-sz.kv_heads // 2)

    def slot(t, carry):
        spread.slot(t)
        pl.when(t == 0)(prepare)
        pl.when(t == 1)(first_norm)
        pl.when(t == 2)(lambda: tokens.start(2))
        pl.when(t == 2)(project)
        pl.when(t == 3)(lambda: shift.finish(sz.before, lambda n: None, zero))

        @pl.when((t == 3) | (t == 4))
        def _():
            def one(k, carry):
                attend(k, sz.kv_heads, sz.groups, q_ref, win, kv_ref, bias, o_full)
                return carry

            lax.fori_loop((t - 3) * each, jnp.minimum((t - 2) * each, sz.kv_heads), one, 0)

        pl.when(t == 5)(mix)
        return carry

    lax.fori_loop(0, plan.slots + 2, slot, 0)
    spread.finish()
    tokens.finish(2)


def first_half(sz, row_sequences, x, dy, small, w):
    grid, tok = sz.grid, sz.tok
    rows, cols = w.shape
    width = cols // GROUPS
    plan = Plan(cols, GATHER_ORDERS, GATHER_PARTS)
    parts = (grid.gx, sz.rows, tok)
    outs = [
        (parts, BF16, VMEM_SPEC),
        (parts, BF16, HBM_SPEC),
        ((grid.gy, grid.gx, rows, cols), BF16, HBM_SPEC),
        ((grid.gy, grid.gx, rows, width), BF16, VMEM_SPEC),
        ((grid.gx,) + small.shape, F32, VMEM_SPEC),
        (parts, BF16, VMEM_SPEC),
        ((1, tok), F32, VMEM_SPEC),
        ((sz.q, tok), BF16, VMEM_SPEC),
        ((2 * sz.kv, tok), BF16, VMEM_SPEC),
        ((sz.before, 2 * sz.kv, tok), BF16, VMEM_SPEC),
        ((sz.q, tok), BF16, VMEM_SPEC),
        ((tok, sz.window), F32, VMEM_SPEC),
        ((2, HEAD_SIZE // 2, tok), F32, VMEM_SPEC),
        ((grid.gx, sz.rows, 2), F32, VMEM_SPEC),
        (parts, F32, VMEM_SPEC),
        (parts, BF16, VMEM_SPEC),
        ((1, tok), F32, VMEM_SPEC),
    ]
    return pl.pallas_call(
        functools.partial(first_kernel, sz, plan, width, row_sequences),
        out_shape=[jax.ShapeDtypeStruct(shape, dtype) for shape, dtype, _ in outs],
        in_specs=[VMEM_SPEC] * 4,
        out_specs=[spec for _, _, spec in outs],
        scratch_shapes=[pltpu.VMEM((sz.q + 2 * sz.kv, tok), F32), pltpu.VMEM((sz.q, tok), F32)]
        + Tokens.semaphores(grid, 3)
        + [pltpu.SemaphoreType.DMA((sz.before,))] * 2
        + [pltpu.SemaphoreType.DMA((1,))]
        + Spread.semaphores(grid, plan),
        compiler_params=params(0),
        name="first_half",
    )(x, dy, small, w)


def last_kernel(
    sz, plan, width, both_ref, down_ref, w_all, w_attn, xo, xn_ref, scale_ref, q_ref, kv_ref, win, o_ref, bias, tables, gains,
    back_ref, hidden_ref, h_ref, dy_ref, scale2_ref,
    bo, ig, go, gaino,
    do_ref, dh_ref, dh_half, bo_ref, dq, dkv_out, dkv_in, dkv, g_attn, dx, y_acc, ig_parts, gain_parts, gain_in, gain_row,
    gain_across, acc, from_core, b_l, *refs,
):
    lands, (t_s, t_r, t_l, k_s, k_r, g_s, g_r, h_s, h_r, *sems) = refs[:-14], refs[-14:]
    grid, tok = sz.grid, sz.tok
    me = grid.here()
    i, j = lax.axis_index("gx"), lax.axis_index("gy")
    peers, across = row_peers(grid.gx, i), row_peers(grid.gy, j)
    greet(peers_of(grid, i, j))
    collect = Collect(grid, me, plan, acc, from_core, lands, go, *sems)

    def source(first):
        if first < 2 * width:
            return both_ref, first
        return (down_ref, first - 2 * width) if first < 3 * width else (g_attn, first - 3 * width)

    collect.start(source)
    pairs = [
        (lambda c, p: bo_ref.at[p], lambda c, p: c.of(bo, p)),
        (lambda c, p: ig_parts.at[p], lambda c, p: c.of(ig, p)),
    ]
    tokens = Tokens(grid, i, j, tok, t_s, t_r, t_l, pairs)
    shift = Shift(sz.span, i, j, -1, lambda n: dkv_out.at[n], lambda n: dkv_in.at[n], k_s, k_r)

    def column_copies():
        for d, p in peers:
            yield d, remote(gain_parts.at[p], gain_in.at[d - 1], g_s.at[d - 1], g_r.at[d - 1], (p, j))

    def across_copies():
        for d, p in across:
            yield d, remote(gain_row, gain_across.at[d - 1], h_s.at[d - 1], h_r.at[d - 1], (i, p))

    def heads_of(part):
        def one(k, carry):
            attend_back(k, sz.kv_heads, sz.groups, q_ref, do_ref, win, kv_ref, bias, dq, dkv_out, dkv)
            return carry

        each = -(-sz.kv_heads // (2 * plan.parts))
        lax.fori_loop(part * each, jnp.minimum((part + 1) * each, sz.kv_heads), one, 0)

    def feed_back():
        dx[...] = jnp.zeros_like(dx)
        y_acc[...] = jnp.zeros_like(y_acc)

        def column(b, carry):
            copies = [
                pltpu.make_async_copy(w_all.at[b, :, :, :, pl.ds((n + 1) * width, width)], g_attn.at[n], b_l.at[n])
                for n in range(3)
            ]
            for copy in copies:
                copy.start()
            for copy in copies:
                copy.wait()
            for k in range(grid.gx):
                at = k // grid.Y, k % grid.Y
                dx[k] += dot(g_attn[(0,) + at], back_ref[b, :width, :], (1, 0)) + dot(
                    g_attn[(1,) + at], back_ref[b, width:, :], (1, 0)
                )
                y_acc[k] += dot(g_attn[(2,) + at], hidden_ref[b], (1, 0))
            return carry

        lax.fori_loop(0, grid.gy, column, 0)
        scale = scale2_ref[...]
        inner = None
        for k in range(grid.gx):
            part = jnp.sum(dx[k] * gains[k, :, 1:2] * h_ref[k], axis=0, keepdims=True)
            inner = part if k == 0 else inner + part
        inner = scale * scale * scale * inner / sz.features
        for k in range(grid.gx):
            value, grad = h_ref[k], dx[k]
            gain_parts[k] = jnp.zeros((8, 128), F32)
            gain_parts[k, 1:2, :] = row_of(jnp.sum(grad * value * scale, axis=1, keepdims=True), 128)
            bo_ref[k] = (value + y_acc[k]).astype(BF16)
            back = dy_ref[k].astype(F32) + (scale * (grad * gains[k, :, 1:2]) - value * inner)
            dh_ref[k] = back
            dh_half[k] = back.astype(BF16)

        def heads(b, carry):
            total = None
            for k in range(grid.gx):
                part = dot(w_attn[b, k][:, sz.qkv : sz.qkv + sz.qc], dh_half[k], (0, 0))
                total = part if k == 0 else total + part
            dq[pl.ds(pl.multiple_of(b * sz.qc, 8), sz.qc), :] = total
            return carry

        lax.fori_loop(0, grid.gy, heads, 0)
        do_ref[...] = dq[...].astype(BF16)
        tokens.start(0)

    def turn_back(ref, heads):
        def one(k, carry):
            row = pl.multiple_of(k * HEAD_SIZE, HEAD_SIZE)
            ref[head_rows(k), :] = turn(ref, row, tables[0], tables[1], -1)
            return carry

        lax.fori_loop(0, heads, one, 0)

    def back_of(b):
        parts = [
            dq[pl.ds(pl.multiple_of(b * sz.qc, 8), sz.qc), :],
            dkv[pl.ds(pl.multiple_of(b * sz.kc, 8), sz.kc), :],
            dkv[pl.ds(pl.multiple_of(sz.kv + b * sz.kc, 8), sz.kc), :],
        ]
        return jnp.concatenate(parts, axis=0).astype(BF16)

    def block_grads():
        turn_back(dq, sz.heads)

        def arrived(n):
            dkv[...] += dkv_in[n].astype(F32)

        shift.finish(sz.before, arrived)
        turn_back(dkv, sz.kv_heads)

        def column(b, carry):
            back = jnp.transpose(back_of(b).astype(F32)).astype(BF16)
            mixed = o_ref[pl.ds(pl.multiple_of(b * sz.qc, 8), sz.qc), :]
            mixed = jnp.transpose(mixed.astype(F32)).astype(BF16)
            for k in range(grid.gx):
                parts = [dot(xn_ref[k], back, (1, 0)), dot(dh_half[k], mixed, (1, 0))]
                left = width - sz.qkv - sz.qc
                if left:
                    parts.append(jnp.zeros((sz.rows, left), F32))
                g_attn[b, k // grid.Y, k % grid.Y] = jnp.concatenate(parts, axis=1).astype(BF16)
            return carry

        lax.fori_loop(0, grid.gy, column, 0)
        for part in range(plan.parts):
            collect.load(plan.slots - plan.parts + part)

    def input_grads():
        backs = [back_of(b) for b in range(grid.gy)]
        inner = None
        for k in range(grid.gx):
            total = None
            for b in range(grid.gy):
                part = dot(w_attn[b, k][:, : sz.qkv], backs[b], (1, 0))
                total = part if b == 0 else total + part
            dx[k] = total
            value = xo[k].astype(F32)
            part = jnp.sum(total * gains[k, :, 0:1] * value, axis=0, keepdims=True)
            inner = part if k == 0 else inner + part
            gain_parts[k, 0:1, :] = row_of(jnp.sum(total * value * scale_ref[...], axis=1, keepdims=True), 128)
        scale = scale_ref[...]
        inner = scale * scale * scale * inner / sz.features
        for k in range(grid.gx):
            value = xo[k].astype(F32)
            ig_parts[k] = (dh_ref[k] + scale * (dx[k] * gains[k, :, 0:1]) - value * inner).astype(BF16)
        tokens.start(1)
        for _, copy in column_copies():
            copy.start()

    def gain_sums():
        gain_row[...] = gain_parts[i]
        for d, copy in column_copies():
            copy.wait()
            gain_row[...] += gain_in[d - 1]
        for _, copy in across_copies():
            copy.start()

    def slot(t, carry):
        pl.when(t == plan.slots - 1)(lambda: collect.begin(t))
        collect.slot(t)
        pl.when(t < plan.slots - 2)(lambda: collect.begin(t + 1))
        pl.when(t == 0)(feed_back)

        @pl.when(t == 1)
        def _():
            heads_of(0)
            heads_of(1)
            shift.start(sz.before)

        pl.when(t == 2)(block_grads)
        pl.when(t == 3)(input_grads)
        pl.when(t == 4)(gain_sums)
        return carry

    collect.begin(0)
    lax.fori_loop(0, plan.slots + collect.lags - 1, slot, 0)
    gaino[...] = gain_row[...]
    for d, copy in across_copies():
        copy.wait()
        gaino[...] += gain_across[d - 1]
    tokens.finish(0)
    tokens.finish(1)
    collect.finish()


def last_half(sz, both, down, w_all, w_attn, kept, back, hidden, h, dy, scale_two):
    grid, tok = sz.grid, sz.tok
    rows, width = w_attn.shape[-2:]
    cols = GROUPS * width
    plan = Plan(cols, REDUCE_ORDERS, REDUCE_PARTS)
    shapes, sems = Collect.scratch(grid, plan, rows, cols)
    sem = pltpu.SemaphoreType.DMA
    parts = (grid.gx, sz.rows, tok)
    shape = lambda g: g.reshape(grid.gy, grid.Z, grid.Y, rows, -1)
    return pl.pallas_call(
        functools.partial(last_kernel, sz, plan, width),
        out_shape=[
            jax.ShapeDtypeStruct((sz.rows, grid.gx * tok), BF16),
            jax.ShapeDtypeStruct((sz.rows, grid.gx * tok), BF16),
            jax.ShapeDtypeStruct((rows, cols), F32),
            jax.ShapeDtypeStruct((8, 128), F32),
        ],
        in_specs=[HBM_SPEC] * 3 + [VMEM_SPEC] * 16,
        out_specs=[VMEM_SPEC] * 4,
        scratch_shapes=[
            pltpu.VMEM((sz.q, tok), BF16),
            pltpu.VMEM(parts, F32),
            pltpu.VMEM(parts, BF16),
            pltpu.VMEM(parts, BF16),
            pltpu.VMEM((sz.q, tok), F32),
            pltpu.VMEM((sz.before, 2 * sz.kv, tok), BF16),
            pltpu.VMEM((sz.before, 2 * sz.kv, tok), BF16),
            pltpu.VMEM((2 * sz.kv, tok), F32),
            pltpu.VMEM((grid.gy, grid.Z, grid.Y, rows, width), BF16),
            pltpu.VMEM(parts, F32),
            pltpu.VMEM(parts, F32),
            pltpu.VMEM(parts, BF16),
            pltpu.VMEM((grid.gx, 8, 128), F32),
            pltpu.VMEM((grid.gx - 1, 8, 128), F32),
            pltpu.VMEM((8, 128), F32),
            pltpu.VMEM((grid.gy - 1, 8, 128), F32),
        ]
        + shapes[:2]
        + [sem((3,))]
        + shapes[2:]
        + Tokens.semaphores(grid, 2)
        + [sem((sz.before,))] * 2
        + [sem((grid.gx - 1,))] * 2
        + [sem((grid.gy - 1,))] * 2
        + sems,
        compiler_params=params(1),
        name="last_half",
    )(shape(both), shape(down), shape(w_all), w_attn, *kept, back, hidden, h, dy, scale_two)


def einsum(form, a, b):
    return jnp.einsum(form, a, b, preferred_element_type=F32)


def padded(a, axis, size):
    pads = [(0, 0)] * a.ndim
    pads[axis] = (0, size - a.shape[axis])
    return jnp.pad(a, pads) if size != a.shape[axis] else a


def shards(
    grid,
    block_input,
    attn_gain,
    query_weight,
    key_weight,
    value_weight,
    output_weight,
    ffn_gain,
    gate_weight,
    up_weight,
    down_weight,
    segment_ids,
    out_cotangent,
):
    GX, GY = grid.gx, grid.gy
    rows, row_tokens = block_input.shape
    tok = row_tokens // GX
    sz = Sizes(grid, tok, rows, query_weight.shape[1], key_weight.shape[1])
    fc, features = gate_weight.shape[1], sz.features
    groups = [
        jnp.concatenate([query_weight, key_weight, value_weight, output_weight.T], axis=1), gate_weight, up_weight, down_weight.T
    ]
    width = -(-max(g.shape[1] for g in groups) // 128) * 128
    block = jnp.concatenate([padded(g, 1, width) for g in groups], axis=1)
    small = jnp.concatenate(
        [segment_ids.reshape(sz.span, tok).astype(F32), padded(jnp.stack([attn_gain, ffn_gain]), 1, tok)], axis=0
    )
    small = padded(small, 0, -(-small.shape[0] // 8) * 8)
    (
        x_parts, dy_parts, w_all, w_attn, _, normed_one, scale_one, query, key_value, earlier, mixed, bias, tables, gains,
        hidden_in, normed_two, scale_two,
    ) = first_half(sz, row_tokens // PACKED_LENGTH, block_input, out_cotangent, small, block)
    dy_half = dy_parts.reshape(features, tok)
    w_cols = w_all.reshape(GY, features, -1)
    w_gate, w_up, w_down = (w_cols[:, :, k * width : k * width + fc] for k in range(1, 4))
    normed_two = normed_two.reshape(features, tok)

    gate = einsum("jdf,dt->jft", w_gate, normed_two)
    up = einsum("jdf,dt->jft", w_up, normed_two)
    sigmoid = jax.nn.sigmoid(gate)
    hidden = padded((jax.nn.silu(gate) * up).astype(BF16), 1, width)
    hidden_grad = einsum("jdf,dt->jft", w_down, dy_half)
    gate_back = (hidden_grad * up * sigmoid * (1.0 + gate * (1.0 - sigmoid))).astype(BF16)
    up_back = (hidden_grad * gate * sigmoid).astype(BF16)
    both_back = jnp.concatenate([padded(gate_back, 1, width), padded(up_back, 1, width)], axis=1)
    grad_both = einsum("dt,jft->jdf", normed_two, both_back).astype(BF16)
    grad_down = einsum("dt,jft->jdf", dy_half, hidden).astype(BF16)
    block_output, input_grad, grads, gains = last_half(
        sz, grad_both, grad_down, w_all, w_attn,
        (x_parts, normed_one, scale_one, query, key_value, earlier, mixed, bias, tables, gains),
        both_back, hidden, hidden_in, dy_parts, scale_two,
    )
    grad_gate, grad_up, grad_down, grad_attn = (grads[:, k * width : (k + 1) * width] for k in range(GROUPS))
    qc, kc = sz.qc, sz.kc
    return (
        block_output,
        input_grad.astype(F32),
        gains[0, :rows],
        grad_attn[:, :qc],
        grad_attn[:, qc : qc + kc],
        grad_attn[:, qc + kc : sz.qkv],
        grad_attn[:, sz.qkv : sz.qkv + qc].T,
        gains[1, :rows],
        grad_gate[:, :fc],
        grad_up[:, :fc],
        grad_down[:, :fc].T,
    )


def solution(mesh):
    grid = Grid(mesh.shape["gx"], mesh.shape["gy"])
    return jax.shard_map(
        functools.partial(shards, grid),
        mesh=mesh,
        in_specs=(
            P("gx", "gy"),
            P("gx"),
            P("gx", "gy"),
            P("gx", "gy"),
            P("gx", "gy"),
            P("gy", "gx"),
            P("gx"),
            P("gx", "gy"),
            P("gx", "gy"),
            P("gy", "gx"),
            P("gx", None),
            P("gx", "gy"),
        ),
        out_specs=(
            P("gx", "gy"),
            P("gx", "gy"),
            P("gx"),
            P("gx", "gy"),
            P("gx", "gy"),
            P("gx", "gy"),
            P("gy", "gx"),
            P("gx"),
            P("gx", "gy"),
            P("gx", "gy"),
            P("gy", "gx"),
        ),
        check_vma=False,
    )
```

```python
import functools
import math

import jax
import jax.numpy as jnp
from jax import lax
from jax.experimental import pallas as pl
from jax.experimental.pallas import tpu as pltpu
from jax.sharding import PartitionSpec as P

QUERY_HEADS = 15
KEY_VALUE_HEADS = 5
HEAD_SIZE = 64
PACKED_LENGTH = 1024
LONGEST_SEGMENT = 512

EPS = 1e-05
THETA = 10000.0
MESH = pl.DeviceIdType.MESH
F32 = jnp.float32
BF16 = jnp.bfloat16


class Grid:
    def __init__(self, gx, gy):
        self.gx, self.gy = gx, gy
        self.C = 2 if gy % 2 == 0 else 1
        self.X = gy // self.C
        self.Y = self.X if gx % self.X == 0 else 1
        self.Z = gx // self.Y
        self.size = {"z": self.Z, "y": self.Y, "x": self.X}

    def here(self):
        i, j = lax.axis_index("gx"), lax.axis_index("gy")
        return {"z": i // self.Y, "y": i % self.Y, "x": j // self.C, "c": j % self.C}

    def device(self, at):
        return (at["z"] * self.Y + at["y"], at["x"] * self.C + at["c"])


def remote(src, dst, send, recv, device):
    return pltpu.make_async_remote_copy(
        src_ref=src, dst_ref=dst, send_sem=send, recv_sem=recv, device_id=device, device_id_type=MESH
    )


def greet(devices):
    barrier = pltpu.get_barrier_semaphore()
    for device in devices:
        pl.semaphore_signal(barrier, inc=1, device_id=device, device_id_type=MESH)
    pl.semaphore_wait(barrier, len(devices))


def row_peers(n, me):
    return [(d, lax.rem(me + d, n)) for d in range(1, n)]


def line(n, here):
    found = []
    for k in range(1, n):
        if n & (n - 1):
            found.append((lax.rem(here + k, n), lax.rem(here + n - k, n)))
            continue
        place, bit = 0, 1
        while bit < n:
            digit = (here // bit) % 2
            place = place + bit * ((1 - digit) if k & bit else digit)
            bit *= 2
        found.append((place, place))
    return found


def places(n, here):
    return [here] + [origin for _, origin in line(n, here)]


def gather_sites(grid, me, order):
    other = [grid.device({**me, "c": 1 - me["c"]})] if grid.C == 2 else []
    onward = [[grid.device({**me, axis: to}) for to, _ in line(grid.size[axis], me[axis])] for axis in order]
    yield 0, dict(me), sum(onward, []) + other
    for stage, axis in enumerate(order, 1):
        earlier = [dict(me)]
        for done in order[: stage - 1]:
            earlier = [{**e, done: place} for place in places(grid.size[done], me[done]) for e in earlier]
        for _, origin in line(grid.size[axis], me[axis]):
            for e in earlier:
                yield stage, {**e, axis: origin}, sum(onward[stage:], []) + other


def core_sites(grid, me):
    found = [{"c": 1 - me["c"]}]
    for axis in "xyz":
        found = [{**f, axis: place} for place in places(grid.size[axis], me[axis]) for f in found]
    return found


GROUPS = 4


class Lane:
    def __init__(self, order, first, part, parts, width, base, step):
        self.order, self.first, self.part, self.parts, self.width = order, first, part, parts, width
        self.base, self.step, self.count = base, step, GROUPS

    def columns(self, m):
        return pl.ds(pl.multiple_of(self.base + m * self.step, 128), self.width)

    def own_columns(self, m):
        return pl.ds(pl.multiple_of(m * self.width, 128), self.width)

    def at(self, slot, body):
        slots = self.count * self.parts
        if isinstance(slot, int):
            if 0 <= slot < slots and slot % self.parts == self.part:
                body(slot // self.parts)
            return
        active = (slot >= 0) & (slot < slots)
        if self.parts > 1:
            active = active & (slot % self.parts == self.part)
        pl.when(active)(lambda: body(slot // self.parts))


class Plan:
    def __init__(self, cols, orders, parts):
        tiles = cols // 128 // GROUPS
        most = -(-tiles * 3 // 5)
        self.lanes, self.parts, self.slots, at = [], parts, GROUPS * parts, 0
        for part in range(parts):
            for order, total in zip(orders, (most, tiles - most)):
                width = total // parts + (part < total % parts)
                if width:
                    self.lanes.append(Lane(order, GROUPS * len(self.lanes), part, parts, width * 128, at * 128, tiles * 128))
                    at += width
        self.chunks = GROUPS * len(self.lanes)


GATHER_ORDERS = ("zyx", "zxy")
REDUCE_ORDERS = ("xyz", "yxz")
GATHER_PARTS, REDUCE_PARTS = 1, 1


def place_of(grid, piece):
    return piece["x"] * grid.C + piece["c"], piece["z"] * grid.Y + piece["y"]


def other_core(grid, me):
    return grid.device({**me, "c": 1 - me["c"]})


def peers_of(grid, i, j):
    return [(p, j) for _, p in row_peers(grid.gx, i)] + [(i, p) for _, p in row_peers(grid.gy, j)]


class Spread:
    def __init__(self, grid, me, plan, w_ref, out, send, recv):
        self.grid, self.me, self.plan = grid, me, plan
        self.w_ref, self.out, self.send, self.recv = w_ref, out, send, recv
        self.sites = [list(gather_sites(grid, me, lane.order)) for lane in plan.lanes]

    @staticmethod
    def count(grid):
        me = {"z": 0, "y": 0, "x": 0, "c": 0}
        return max(sum(len(sends) for _, _, sends in gather_sites(grid, me, order)) for order in GATHER_ORDERS)

    @staticmethod
    def semaphores(grid, plan):
        return [
            pltpu.SemaphoreType.DMA((Spread.count(grid), plan.chunks)),
            pltpu.SemaphoreType.DMA((grid.gy, grid.gx, plan.chunks)),
        ]

    def stage(self, stage, slot, finish=False):
        for lane, sites in zip(self.plan.lanes, self.sites):
            lane.at(slot, lambda m, lane=lane, sites=sites: self.chunk(lane, sites, stage, m, finish))

    def chunk(self, lane, sites, stage, m, finish):
        number, chunk = 0, lane.first + m
        for at, piece, sends in sites:
            first = number
            number += len(sends)
            if at != stage:
                continue
            j, i = place_of(self.grid, piece)
            land = self.out.at[j, i, :, lane.columns(m)]
            src = self.w_ref.at[:, lane.columns(m)] if at == 0 else land
            arrived = self.recv.at[j, i, chunk]
            if at and not finish:
                remote(land, land, self.send.at[first, chunk], arrived, (0, 0)).wait_recv()
            for n, device in enumerate(sends):
                copy = remote(src, land, self.send.at[first + n, chunk], arrived, device)
                if finish:
                    copy.wait_send()
                else:
                    copy.start()

    def start(self):
        self.stage(0, 0)
        self.stage(0, 1)

    def slot(self, t):
        self.stage(0, t + 2)
        for stage in (2, 3, 1):
            self.stage(stage, t - (stage - 1))

        @pl.when(t == 2)
        def _():
            self.cores(0)

    def cores(self, slot):
        for lane in self.plan.lanes:
            lane.at(slot, functools.partial(self.core, lane))

    def core(self, lane, m):
        if self.grid.C == 2:
            for piece in core_sites(self.grid, self.me):
                j, i = place_of(self.grid, piece)
                land, chunk = self.out.at[j, i, :, lane.columns(m)], lane.first + m
                remote(land, land, self.send.at[0, chunk], self.recv.at[j, i, chunk], (0, 0)).wait_recv()

    def finish(self):
        def end(t, carry):
            pl.when(t > 0)(lambda: self.cores(t))
            for stage in range(4):
                self.stage(stage, t, True)
            return carry

        lax.fori_loop(0, self.plan.slots, end, 0)


class Tokens:
    def __init__(self, grid, i, j, tok, send, recv, local, pairs):
        self.grid, self.i, self.j, self.tok = grid, i, j, tok
        self.send, self.recv, self.local, self.pairs = send, recv, local, pairs

    @staticmethod
    def semaphores(grid, n):
        return [
            pltpu.SemaphoreType.DMA((n, grid.gx - 1)),
            pltpu.SemaphoreType.DMA((n, grid.gx - 1)),
            pltpu.SemaphoreType.DMA((n,)),
        ]

    def of(self, ref, p):
        return ref.at[:, pl.ds(pl.multiple_of(p * self.tok, self.tok), self.tok)]

    def own(self, n):
        pick, land = self.pairs[n]
        return pltpu.make_async_copy(pick(self, self.i), land(self, self.i), self.local.at[n])

    def start(self, n):
        pick, land = self.pairs[n]
        for d, p in row_peers(self.grid.gx, self.i):
            remote(pick(self, p), land(self, self.i), self.send.at[n, d - 1], self.recv.at[n, d - 1], (p, self.j)).start()
        self.own(n).start()

    def finish(self, n):
        pick, land = self.pairs[n]
        for d, p in row_peers(self.grid.gx, self.i):
            sems = self.send.at[n, d - 1], self.recv.at[n, d - 1]
            remote(pick(self, p), land(self, self.i), *sems, (p, self.j)).wait_send()
            back = land(self, lax.rem(self.i + self.grid.gx - d, self.grid.gx))
            remote(back, back, *sems, (p, self.j)).wait_recv()
        self.own(n).wait()


def dot(a, b, contract):
    return lax.dot_general(a, b, ((contract[:1], contract[1:]), ((), ())), preferred_element_type=F32)


def attention_bias(seg_query, seg_window):
    tok, window = seg_query.shape[0], seg_window.shape[1]
    row = lax.broadcasted_iota(jnp.int32, (tok, window), 0) + (window - tok)
    column = lax.broadcasted_iota(jnp.int32, (tok, window), 1)
    return jnp.where((seg_query == seg_window) & (column <= row), 0.0, -jnp.inf).astype(F32)


def head_rows(head):
    return pl.ds(pl.multiple_of(head * HEAD_SIZE, HEAD_SIZE), HEAD_SIZE)


def in_window(win_ref, own_ref, head):
    parts = [win_ref[n, head_rows(head), :] for n in reversed(range(win_ref.shape[0]))]
    return jnp.concatenate(parts + [own_ref[head_rows(head), :]], axis=1)


def probabilities(query, key, bias):
    scores = dot(query, key, (0, 0)) * HEAD_SIZE ** (-0.5) + bias
    raised = jnp.exp(scores - jnp.max(scores, axis=1, keepdims=True))
    return raised * (1.0 / jnp.sum(raised, axis=1, keepdims=True))


def attend(k, kv_heads, groups, q_ref, win_ref, own_ref, bias_ref, o_ref):
    key, value = in_window(win_ref, own_ref, k), in_window(win_ref, own_ref, kv_heads + k)
    for g in range(groups):
        rows = head_rows(k * groups + g)
        prob = probabilities(q_ref[rows, :], key, bias_ref[...]).astype(BF16)
        o_ref[rows, :] = dot(value, prob, (1, 1)).astype(BF16).astype(F32)


def attend_back(k, kv_heads, groups, q_ref, do_ref, win_ref, own_ref, bias_ref, dq_ref, dkv_out, dkv_own):
    key, value = in_window(win_ref, own_ref, k), in_window(win_ref, own_ref, kv_heads + k)
    key_grad = value_grad = None
    for g in range(groups):
        rows = head_rows(k * groups + g)
        query, grad = q_ref[rows, :], do_ref[rows, :]
        prob = probabilities(query, key, bias_ref[...])
        prob_grad = dot(grad, value, (0, 0))
        row_dot = jnp.sum(prob * prob_grad, axis=1, keepdims=True)
        score_grad = (prob * (prob_grad - row_dot) * HEAD_SIZE ** (-0.5)).astype(BF16)
        dq_ref[rows, :] = dot(key, score_grad, (1, 1))
        dk = dot(query, score_grad, (1, 0))
        dv = dot(grad, prob.astype(BF16), (1, 0))
        key_grad = dk if g == 0 else key_grad + dk
        value_grad = dv if g == 0 else value_grad + dv
    tok = q_ref.shape[1]
    for head, grad in ((k, key_grad), (kv_heads + k, value_grad)):
        before = dkv_out.shape[0]
        for n in range(before):
            at = before - 1 - n
            dkv_out[n, head_rows(head), :] = grad[:, at * tok : (at + 1) * tok].astype(BF16)
        dkv_own[head_rows(head), :] = grad[:, before * tok :]


def over(ref, body):
    lead = ref.shape[:-2]
    total = math.prod(lead)

    def one(k, carry):
        place = []
        for n in reversed(lead):
            place.append(k % n)
            k = k // n
        body(tuple(reversed(place)))
        return carry

    if total == 1:
        body((0,) * len(lead))
    else:
        lax.fori_loop(0, total, one, 0)


def add_into(target, source):
    def one(place):
        where = place + (slice(None), slice(None))
        target[where] = target[where] + source[where]

    over(target, one)


DIMS = "xzy"


class Collect:
    def __init__(self, grid, me, plan, acc, from_core, lands, out, c_s, c_r, c_l, l_s, l_r):
        self.grid, self.me, self.plan = grid, me, plan
        self.acc, self.from_core, self.lands, self.out = acc, from_core, lands, out
        self.c_s, self.c_r, self.c_l, self.l_s, self.l_r = c_s, c_r, c_l, l_s, l_r
        self.actions = [self.actions_of(n, lane) for n, lane in enumerate(plan.lanes)]
        self.lags = max(len(actions) for actions in self.actions)

    @staticmethod
    def axes(grid, lane):
        return [axis for axis in lane.order if grid.size[axis] > 1]

    @staticmethod
    def scratch(grid, plan, rows, cols):
        size = (grid.X, grid.Z, grid.Y, rows, cols)
        shapes = [pltpu.VMEM(size, BF16), pltpu.VMEM(size, BF16)]
        for lane in plan.lanes:
            axes = Collect.axes(grid, lane)
            for level, axis in enumerate(axes):
                rest = tuple(grid.size[d] for d in DIMS if d in axes[level + 1 :])
                shapes.append(pltpu.VMEM((grid.size[axis] - 1,) + rest + (rows, lane.count * lane.width), BF16))
        sem = pltpu.SemaphoreType.DMA
        most = max(n - 1 for n in grid.size.values())
        levels = len(shapes) - 2
        return shapes, [sem((grid.X, plan.chunks))] * 3 + [sem((levels, most, plan.chunks))] * 2

    def own_copy(self, x, lane, m, g_ref, columns):
        src, chunk = g_ref.at[x * self.grid.C + self.me["c"], :, :, :, columns], lane.first + m
        return pltpu.make_async_copy(src, self.acc.at[x, :, :, :, lane.columns(m)], self.c_l.at[x, chunk])

    def core_copy(self, x, lane, m, g_ref, columns):
        src, chunk = g_ref.at[x * self.grid.C + 1 - self.me["c"], :, :, :, columns], lane.first + m
        land = self.from_core.at[x, :, :, :, lane.columns(m)]
        return remote(src, land, self.c_s.at[x, chunk], self.c_r.at[x, chunk], other_core(self.grid, self.me))

    def start(self, source):
        self.source = source
        for slot in range(self.plan.slots - self.plan.parts):
            self.load(slot)

    def load(self, slot):
        for lane in self.plan.lanes:

            def body(m, lane=lane):
                ref, at = self.source(lane.base + m * lane.step)
                for x in range(self.grid.X):
                    self.own_copy(x, lane, m, ref, pl.ds(at, lane.width)).start()
                    if self.grid.C == 2:
                        self.core_copy(x, lane, m, ref, pl.ds(at, lane.width)).start()

            lane.at(slot, body)

    def core(self, lane, m):
        columns = lane.columns(m)
        ref, _ = self.source(0)
        for x in range(self.grid.X):
            self.own_copy(x, lane, m, ref, pl.ds(0, lane.width)).wait()
            if self.grid.C == 2:
                self.core_copy(x, lane, m, ref, pl.ds(0, lane.width)).wait_recv()
                add_into(self.acc.at[x, :, :, :, columns], self.from_core.at[x, :, :, :, columns])

    def level(self, number, lane, level):
        axes = self.axes(self.grid, lane)
        axis = axes[level]
        index = sum(len(self.axes(self.grid, other)) for other in self.plan.lanes[:number]) + level
        free = len(axes) - level - 1

        def pick(t, m):
            place = []
            for d in DIMS:
                if d == axis:
                    place.append(t)
                elif d in axes[level + 1 :]:
                    place.append(slice(None))
                else:
                    place.append(self.me[d] if self.grid.size[d] > 1 else 0)
            return self.acc.at[tuple(place) + (slice(None), lane.columns(m))]

        def land(slot, m):
            return self.lands[index].at[(slot,) + (slice(None),) * (free + 1) + (lane.own_columns(m),)]

        def copies(m):
            for slot, (to, _) in enumerate(line(self.grid.size[axis], self.me[axis])):
                sems = self.l_s.at[index, slot, lane.first + m], self.l_r.at[index, slot, lane.first + m]
                yield slot, remote(pick(to, m), land(slot, m), *sems, self.grid.device({**self.me, axis: to}))

        return self.me[axis], pick, land, copies

    def actions_of(self, number, lane):
        levels = [self.level(number, lane, level) for level in range(len(self.axes(self.grid, lane)))]

        def send(m, copies):
            for _, copy in copies(m):
                copy.start()

        def take(m, p, pick, land, copies, last):
            columns = lane.columns(m)
            if last:
                self.out[:, columns] = pick(p, m)[...].astype(F32)
            for slot, copy in copies(m):
                copy.wait_recv()
                if last:
                    self.out[:, columns] += land(slot, m)[...].astype(F32)
                else:
                    add_into(pick(p, m), land(slot, m))

        actions = [[functools.partial(self.core, lane)]]
        for number, (p, pick, land, copies) in enumerate(levels):
            actions[-1].append(functools.partial(send, copies=copies))
            last = number == len(levels) - 1
            actions.append([functools.partial(take, p=p, pick=pick, land=land, copies=copies, last=last)])
        return actions

    def begin(self, slot):
        for lane, actions in zip(self.plan.lanes, self.actions):
            for action in actions[0]:
                lane.at(slot, action)

    def slot(self, t):
        for lag in range(1, self.lags):
            for lane, actions in zip(self.plan.lanes, self.actions):
                if lag < len(actions):
                    for action in actions[lag]:
                        lane.at(t - lag, action)

    def finish(self):
        def end(t, carry):
            for number, lane in enumerate(self.plan.lanes):

                def body(m, number=number, lane=lane):
                    if self.grid.C == 2:
                        ref, _ = self.source(0)
                        for x in range(self.grid.X):
                            self.core_copy(x, lane, m, ref, pl.ds(0, lane.width)).wait_send()
                    for level in range(len(self.axes(self.grid, lane))):
                        for _, copy in self.level(number, lane, level)[-1](m):
                            copy.wait_send()

                lane.at(t, body)
            return carry

        lax.fori_loop(0, self.plan.slots, end, 0)


class Shift:
    def __init__(self, span, i, j, sign, pick, land, send, recv):
        self.i, self.j, self.q, self.span, self.sign = i, j, i % span, span, sign
        self.pick, self.land, self.send, self.recv = pick, land, send, recv

    def copy(self, n):
        sems = self.send.at[n], self.recv.at[n]
        return remote(self.pick(n), self.land(n), *sems, (self.i + self.sign * (n + 1), self.j))

    def before(self, n):
        return self.q >= n + 1

    def after(self, n):
        return self.q + n + 1 < self.span

    def start(self, slots):
        for n in range(slots):
            pl.when(self.after(n) if self.sign > 0 else self.before(n))(lambda n=n: self.copy(n).start())

    def finish(self, slots, arrived, missing=None):
        for n in range(slots):
            there, goes = (self.before(n), self.after(n)) if self.sign > 0 else (self.after(n), self.before(n))

            def take(n=n):
                self.copy(n).wait_recv()
                arrived(n)

            pl.when(there)(take)
            if missing is not None:
                pl.when(jnp.logical_not(there))(lambda n=n: missing(n))
            pl.when(goes)(lambda n=n: self.copy(n).wait_send())


HBM_SPEC = pl.BlockSpec(memory_space=pl.ANY)
VMEM_SPEC = pl.BlockSpec(memory_space=pltpu.VMEM)


def params(collective_id):
    return pltpu.CompilerParams(
        collective_id=collective_id, has_side_effects=True, vmem_limit_bytes=63 * 1024 * 1024
    )


def column_of(row, size):
    n = row.shape[1]
    same = lax.broadcasted_iota(jnp.int32, (size, n), 0) == lax.broadcasted_iota(jnp.int32, (size, n), 1)
    return jnp.sum(jnp.where(same, row, 0.0), axis=1, keepdims=True)


def row_of(column, size):
    n = column.shape[0]
    same = lax.broadcasted_iota(jnp.int32, (n, size), 0) == lax.broadcasted_iota(jnp.int32, (n, size), 1)
    return jnp.sum(jnp.where(same, column, 0.0), axis=0, keepdims=True)


class Sizes:
    def __init__(self, grid, tok, rows, qc, kc):
        self.grid, self.tok, self.rows, self.qc, self.kc = grid, tok, rows, qc, kc
        self.features = rows * grid.gx
        self.q, self.kv = qc * grid.gy, kc * grid.gy
        self.heads, self.kv_heads = self.q // HEAD_SIZE, self.kv // HEAD_SIZE
        self.groups = self.heads // self.kv_heads
        self.span = PACKED_LENGTH // tok
        self.before = -(-(LONGEST_SEGMENT - 1) // tok)
        self.window = (self.before + 1) * tok
        self.qkv = qc + 2 * kc


def turn(ref, row, cos_table, sine_table, direction):
    half = HEAD_SIZE // 2
    lower = ref[pl.ds(row, half), :]
    upper = ref[pl.ds(pl.multiple_of(row + half, half), half), :]
    if direction > 0:
        lower, upper = lower.astype(BF16).astype(F32), upper.astype(BF16).astype(F32)
    return jnp.concatenate(
        [lower * cos_table - direction * upper * sine_table, upper * cos_table + direction * lower * sine_table], axis=0
    )


def first_kernel(
    sz, plan, width, row_sequences, x_ref, dy_ref, small_ref, w_ref,
    xo, dyo, wo, w_attn, smallo, xn_ref, scale_ref, q_ref, kv_ref, win, o_ref, bias, tables, gains, h_ref, xn2_ref, scale2_ref,
    raw, o_full, t_s, t_r, t_l, k_s, k_r, w_l, w_s, w_r,
):
    grid, tok = sz.grid, sz.tok
    me = grid.here()
    i, j = lax.axis_index("gx"), lax.axis_index("gy")
    greet(peers_of(grid, i, j))
    pairs = [
        (lambda c, p: small_ref, lambda c, p: smallo.at[p]),
        (lambda c, p: c.of(x_ref, p), lambda c, p: xo.at[p]),
        (lambda c, p: c.of(dy_ref, p), lambda c, p: dyo.at[p]),
    ]
    tokens = Tokens(grid, i, j, tok, t_s, t_r, t_l, pairs)
    spread = Spread(grid, me, plan, w_ref, wo, w_s, w_r)
    tokens.start(0)
    spread.start()
    tokens.start(1)
    pltpu.make_async_copy(w_ref, wo.at[j, i], w_l.at[0]).start()
    shift = Shift(sz.span, i, j, 1, lambda n: kv_ref, lambda n: win.at[n], k_s, k_r)
    sequence, q = j * row_sequences + i // sz.span, i % sz.span
    half = HEAD_SIZE // 2

    def norm(parts, scale_out, gain, out):
        total = None
        for k in range(grid.gx):
            value = parts(k)
            part = jnp.sum(value * value, axis=0, keepdims=True)
            total = part if k == 0 else total + part
        scale = lax.rsqrt(total / sz.features + EPS)
        scale_out[...] = scale
        for k in range(grid.gx):
            out[k] = (parts(k) * scale * gains[k, :, gain : gain + 1]).astype(BF16)

    def prepare():
        tokens.finish(0)

        def segments(place):
            row = smallo[sequence, pl.ds(jnp.maximum(place, 0), 1), :][:, :tok]
            return jnp.where(place >= 0, row, -1.0)

        here = segments(q)
        bias[...] = attention_bias(
            column_of(here, tok), jnp.concatenate([segments(q - n) for n in range(sz.before, 0, -1)] + [here], axis=1)
        )
        first = jnp.zeros((1, tok), F32)
        for n in range(sz.span):
            other = column_of(smallo[sequence, n : n + 1, :][:, :tok], tok)
            first = first + jnp.sum(jnp.where(other < here, 1.0, 0.0), axis=0, keepdims=True)
        positions = (q * tok).astype(F32) + lax.broadcasted_iota(jnp.int32, (1, tok), 1).astype(F32) - first
        frequency = jnp.exp(
            -math.log(THETA) * lax.broadcasted_iota(jnp.int32, (half, 1), 0).astype(F32) / half
        )
        angles = frequency * positions
        tables[0] = jnp.cos(angles)
        tables[1] = jnp.sin(angles)
        for k in range(grid.gx):
            columns = [column_of(smallo[k, sz.span + n : sz.span + n + 1, :][:, :tok], sz.rows) for n in range(2)]
            gains[k] = jnp.concatenate(columns, axis=1)

    def first_norm():
        tokens.finish(1)
        norm(lambda k: xo[k].astype(F32), scale_ref, 0, xn_ref)

    def project():
        pltpu.make_async_copy(w_ref, wo.at[j, i], w_l.at[0]).wait()
        copy = pltpu.make_async_copy(wo.at[:, :, :, pl.ds(0, width)], w_attn, w_l.at[0])
        copy.start()
        copy.wait()

        def column(b, carry):
            total = None
            for k in range(grid.gx):
                part = dot(w_attn[b, k][:, : sz.qkv], xn_ref[k], (0, 0))
                total = part if k == 0 else total + part
            for part, at, size in ((0, 0, sz.qc), (sz.qc, sz.q, sz.kc), (sz.qc + sz.kc, sz.q + sz.kv, sz.kc)):
                raw[pl.ds(pl.multiple_of(at + b * size, 8), size), :] = total[part : part + size]
            return carry

        lax.fori_loop(0, grid.gy, column, 0)

        def key(k, carry):
            kv_ref[head_rows(k), :] = turn(raw, pl.multiple_of(sz.q + k * HEAD_SIZE, HEAD_SIZE), tables[0], tables[1], 1).astype(BF16)
            kv_ref[head_rows(sz.kv_heads + k), :] = raw[head_rows(sz.heads + sz.kv_heads + k), :].astype(BF16)
            return carry

        lax.fori_loop(0, sz.kv_heads, key, 0)
        shift.start(sz.before)

        def query(k, carry):
            q_ref[head_rows(k), :] = turn(raw, pl.multiple_of(k * HEAD_SIZE, HEAD_SIZE), tables[0], tables[1], 1).astype(BF16)
            return carry

        lax.fori_loop(0, sz.heads, query, 0)

    def zero(n):
        win[n] = jnp.zeros(win.shape[1:], BF16)

    def mix():
        def block(k, carry):
            total = xo[k].astype(F32)
            for b in range(grid.gy):
                mixed = o_full[pl.ds(b * sz.qc, sz.qc), :].astype(BF16)
                total = total + dot(w_attn[b, k][:, sz.qkv : sz.qkv + sz.qc], mixed, (1, 0))
            h_ref[k] = total
            return carry

        lax.fori_loop(0, grid.gx, block, 0)
        norm(lambda k: h_ref[k], scale2_ref, 1, xn2_ref)
        o_ref[...] = o_full[...].astype(BF16)

    each = -(-sz.kv_heads // 2)

    def slot(t, carry):
        spread.slot(t)
        pl.when(t == 0)(prepare)
        pl.when(t == 1)(first_norm)
        pl.when(t == 2)(lambda: tokens.start(2))
        pl.when(t == 2)(project)
        pl.when(t == 3)(lambda: shift.finish(sz.before, lambda n: None, zero))

        @pl.when((t == 3) | (t == 4))
        def _():
            def one(k, carry):
                attend(k, sz.kv_heads, sz.groups, q_ref, win, kv_ref, bias, o_full)
                return carry

            lax.fori_loop((t - 3) * each, jnp.minimum((t - 2) * each, sz.kv_heads), one, 0)

        pl.when(t == 5)(mix)
        return carry

    lax.fori_loop(0, plan.slots + 2, slot, 0)
    spread.finish()
    tokens.finish(2)


def first_half(sz, row_sequences, x, dy, small, w):
    grid, tok = sz.grid, sz.tok
    rows, cols = w.shape
    width = cols // GROUPS
    plan = Plan(cols, GATHER_ORDERS, GATHER_PARTS)
    parts = (grid.gx, sz.rows, tok)
    outs = [
        (parts, BF16, VMEM_SPEC),
        (parts, BF16, HBM_SPEC),
        ((grid.gy, grid.gx, rows, cols), BF16, HBM_SPEC),
        ((grid.gy, grid.gx, rows, width), BF16, VMEM_SPEC),
        ((grid.gx,) + small.shape, F32, VMEM_SPEC),
        (parts, BF16, VMEM_SPEC),
        ((1, tok), F32, VMEM_SPEC),
        ((sz.q, tok), BF16, VMEM_SPEC),
        ((2 * sz.kv, tok), BF16, VMEM_SPEC),
        ((sz.before, 2 * sz.kv, tok), BF16, VMEM_SPEC),
        ((sz.q, tok), BF16, VMEM_SPEC),
        ((tok, sz.window), F32, VMEM_SPEC),
        ((2, HEAD_SIZE // 2, tok), F32, VMEM_SPEC),
        ((grid.gx, sz.rows, 2), F32, VMEM_SPEC),
        (parts, F32, VMEM_SPEC),
        (parts, BF16, VMEM_SPEC),
        ((1, tok), F32, VMEM_SPEC),
    ]
    return pl.pallas_call(
        functools.partial(first_kernel, sz, plan, width, row_sequences),
        out_shape=[jax.ShapeDtypeStruct(shape, dtype) for shape, dtype, _ in outs],
        in_specs=[VMEM_SPEC] * 4,
        out_specs=[spec for _, _, spec in outs],
        scratch_shapes=[pltpu.VMEM((sz.q + 2 * sz.kv, tok), F32), pltpu.VMEM((sz.q, tok), F32)]
        + Tokens.semaphores(grid, 3)
        + [pltpu.SemaphoreType.DMA((sz.before,))] * 2
        + [pltpu.SemaphoreType.DMA((1,))]
        + Spread.semaphores(grid, plan),
        compiler_params=params(0),
        name="first_half",
    )(x, dy, small, w)


def last_kernel(
    sz, plan, width, both_ref, down_ref, w_all, w_attn, xo, xn_ref, scale_ref, q_ref, kv_ref, win, o_ref, bias, tables, gains,
    back_ref, hidden_ref, h_ref, dy_ref, scale2_ref,
    bo, ig, go, gaino,
    do_ref, dh_ref, dh_half, bo_ref, dq, dkv_out, dkv_in, dkv, g_attn, dx, y_acc, ig_parts, gain_parts, gain_in, gain_row,
    gain_across, acc, from_core, b_l, *refs,
):
    lands, (t_s, t_r, t_l, k_s, k_r, g_s, g_r, h_s, h_r, *sems) = refs[:-14], refs[-14:]
    grid, tok = sz.grid, sz.tok
    me = grid.here()
    i, j = lax.axis_index("gx"), lax.axis_index("gy")
    peers, across = row_peers(grid.gx, i), row_peers(grid.gy, j)
    greet(peers_of(grid, i, j))
    collect = Collect(grid, me, plan, acc, from_core, lands, go, *sems)

    def source(first):
        if first < 2 * width:
            return both_ref, first
        return (down_ref, first - 2 * width) if first < 3 * width else (g_attn, first - 3 * width)

    collect.start(source)
    pairs = [
        (lambda c, p: bo_ref.at[p], lambda c, p: c.of(bo, p)),
        (lambda c, p: ig_parts.at[p], lambda c, p: c.of(ig, p)),
    ]
    tokens = Tokens(grid, i, j, tok, t_s, t_r, t_l, pairs)
    shift = Shift(sz.span, i, j, -1, lambda n: dkv_out.at[n], lambda n: dkv_in.at[n], k_s, k_r)

    def column_copies():
        for d, p in peers:
            yield d, remote(gain_parts.at[p], gain_in.at[d - 1], g_s.at[d - 1], g_r.at[d - 1], (p, j))

    def across_copies():
        for d, p in across:
            yield d, remote(gain_row, gain_across.at[d - 1], h_s.at[d - 1], h_r.at[d - 1], (i, p))

    def heads_of(part):
        def one(k, carry):
            attend_back(k, sz.kv_heads, sz.groups, q_ref, do_ref, win, kv_ref, bias, dq, dkv_out, dkv)
            return carry

        each = -(-sz.kv_heads // (2 * plan.parts))
        lax.fori_loop(part * each, jnp.minimum((part + 1) * each, sz.kv_heads), one, 0)

    def feed_back():
        dx[...] = jnp.zeros_like(dx)
        y_acc[...] = jnp.zeros_like(y_acc)

        def column(b, carry):
            copies = [
                pltpu.make_async_copy(w_all.at[b, :, :, :, pl.ds((n + 1) * width, width)], g_attn.at[n], b_l.at[n])
                for n in range(3)
            ]
            for copy in copies:
                copy.start()
            for copy in copies:
                copy.wait()
            for k in range(grid.gx):
                at = k // grid.Y, k % grid.Y
                dx[k] += dot(g_attn[(0,) + at], back_ref[b, :width, :], (1, 0)) + dot(
                    g_attn[(1,) + at], back_ref[b, width:, :], (1, 0)
                )
                y_acc[k] += dot(g_attn[(2,) + at], hidden_ref[b], (1, 0))
            return carry

        lax.fori_loop(0, grid.gy, column, 0)
        scale = scale2_ref[...]
        inner = None
        for k in range(grid.gx):
            part = jnp.sum(dx[k] * gains[k, :, 1:2] * h_ref[k], axis=0, keepdims=True)
            inner = part if k == 0 else inner + part
        inner = scale * scale * scale * inner / sz.features
        for k in range(grid.gx):
            value, grad = h_ref[k], dx[k]
            gain_parts[k] = jnp.zeros((8, 128), F32)
            gain_parts[k, 1:2, :] = row_of(jnp.sum(grad * value * scale, axis=1, keepdims=True), 128)
            bo_ref[k] = (value + y_acc[k]).astype(BF16)
            back = dy_ref[k].astype(F32) + (scale * (grad * gains[k, :, 1:2]) - value * inner)
            dh_ref[k] = back
            dh_half[k] = back.astype(BF16)

        def heads(b, carry):
            total = None
            for k in range(grid.gx):
                part = dot(w_attn[b, k][:, sz.qkv : sz.qkv + sz.qc], dh_half[k], (0, 0))
                total = part if k == 0 else total + part
            dq[pl.ds(pl.multiple_of(b * sz.qc, 8), sz.qc), :] = total
            return carry

        lax.fori_loop(0, grid.gy, heads, 0)
        do_ref[...] = dq[...].astype(BF16)
        tokens.start(0)

    def turn_back(ref, heads):
        def one(k, carry):
            row = pl.multiple_of(k * HEAD_SIZE, HEAD_SIZE)
            ref[head_rows(k), :] = turn(ref, row, tables[0], tables[1], -1)
            return carry

        lax.fori_loop(0, heads, one, 0)

    def back_of(b):
        parts = [
            dq[pl.ds(pl.multiple_of(b * sz.qc, 8), sz.qc), :],
            dkv[pl.ds(pl.multiple_of(b * sz.kc, 8), sz.kc), :],
            dkv[pl.ds(pl.multiple_of(sz.kv + b * sz.kc, 8), sz.kc), :],
        ]
        return jnp.concatenate(parts, axis=0).astype(BF16)

    def block_grads():
        turn_back(dq, sz.heads)

        def arrived(n):
            dkv[...] += dkv_in[n].astype(F32)

        shift.finish(sz.before, arrived)
        turn_back(dkv, sz.kv_heads)

        def column(b, carry):
            back = jnp.transpose(back_of(b).astype(F32)).astype(BF16)
            mixed = o_ref[pl.ds(pl.multiple_of(b * sz.qc, 8), sz.qc), :]
            mixed = jnp.transpose(mixed.astype(F32)).astype(BF16)
            for k in range(grid.gx):
                parts = [dot(xn_ref[k], back, (1, 0)), dot(dh_half[k], mixed, (1, 0))]
                left = width - sz.qkv - sz.qc
                if left:
                    parts.append(jnp.zeros((sz.rows, left), F32))
                g_attn[b, k // grid.Y, k % grid.Y] = jnp.concatenate(parts, axis=1).astype(BF16)
            return carry

        lax.fori_loop(0, grid.gy, column, 0)
        for part in range(plan.parts):
            collect.load(plan.slots - plan.parts + part)

    def input_grads():
        backs = [back_of(b) for b in range(grid.gy)]
        inner = None
        for k in range(grid.gx):
            total = None
            for b in range(grid.gy):
                part = dot(w_attn[b, k][:, : sz.qkv], backs[b], (1, 0))
                total = part if b == 0 else total + part
            dx[k] = total
            value = xo[k].astype(F32)
            part = jnp.sum(total * gains[k, :, 0:1] * value, axis=0, keepdims=True)
            inner = part if k == 0 else inner + part
            gain_parts[k, 0:1, :] = row_of(jnp.sum(total * value * scale_ref[...], axis=1, keepdims=True), 128)
        scale = scale_ref[...]
        inner = scale * scale * scale * inner / sz.features
        for k in range(grid.gx):
            value = xo[k].astype(F32)
            ig_parts[k] = (dh_ref[k] + scale * (dx[k] * gains[k, :, 0:1]) - value * inner).astype(BF16)
        tokens.start(1)
        for _, copy in column_copies():
            copy.start()

    def gain_sums():
        gain_row[...] = gain_parts[i]
        for d, copy in column_copies():
            copy.wait()
            gain_row[...] += gain_in[d - 1]
        for _, copy in across_copies():
            copy.start()

    def slot(t, carry):
        pl.when(t == plan.slots - 1)(lambda: collect.begin(t))
        collect.slot(t)
        pl.when(t < plan.slots - 2)(lambda: collect.begin(t + 1))
        pl.when(t == 0)(feed_back)

        @pl.when(t == 1)
        def _():
            heads_of(0)
            heads_of(1)
            shift.start(sz.before)

        pl.when(t == 2)(block_grads)
        pl.when(t == 3)(input_grads)
        pl.when(t == 4)(gain_sums)
        return carry

    collect.begin(0)
    lax.fori_loop(0, plan.slots + collect.lags - 1, slot, 0)
    gaino[...] = gain_row[...]
    for d, copy in across_copies():
        copy.wait()
        gaino[...] += gain_across[d - 1]
    tokens.finish(0)
    tokens.finish(1)
    collect.finish()


def last_half(sz, both, down, w_all, w_attn, kept, back, hidden, h, dy, scale_two):
    grid, tok = sz.grid, sz.tok
    rows, width = w_attn.shape[-2:]
    cols = GROUPS * width
    plan = Plan(cols, REDUCE_ORDERS, REDUCE_PARTS)
    shapes, sems = Collect.scratch(grid, plan, rows, cols)
    sem = pltpu.SemaphoreType.DMA
    parts = (grid.gx, sz.rows, tok)
    shape = lambda g: g.reshape(grid.gy, grid.Z, grid.Y, rows, -1)
    return pl.pallas_call(
        functools.partial(last_kernel, sz, plan, width),
        out_shape=[
            jax.ShapeDtypeStruct((sz.rows, grid.gx * tok), BF16),
            jax.ShapeDtypeStruct((sz.rows, grid.gx * tok), BF16),
            jax.ShapeDtypeStruct((rows, cols), F32),
            jax.ShapeDtypeStruct((8, 128), F32),
        ],
        in_specs=[HBM_SPEC] * 3 + [VMEM_SPEC] * 16,
        out_specs=[VMEM_SPEC] * 4,
        scratch_shapes=[
            pltpu.VMEM((sz.q, tok), BF16),
            pltpu.VMEM(parts, F32),
            pltpu.VMEM(parts, BF16),
            pltpu.VMEM(parts, BF16),
            pltpu.VMEM((sz.q, tok), F32),
            pltpu.VMEM((sz.before, 2 * sz.kv, tok), BF16),
            pltpu.VMEM((sz.before, 2 * sz.kv, tok), BF16),
            pltpu.VMEM((2 * sz.kv, tok), F32),
            pltpu.VMEM((grid.gy, grid.Z, grid.Y, rows, width), BF16),
            pltpu.VMEM(parts, F32),
            pltpu.VMEM(parts, F32),
            pltpu.VMEM(parts, BF16),
            pltpu.VMEM((grid.gx, 8, 128), F32),
            pltpu.VMEM((grid.gx - 1, 8, 128), F32),
            pltpu.VMEM((8, 128), F32),
            pltpu.VMEM((grid.gy - 1, 8, 128), F32),
        ]
        + shapes[:2]
        + [sem((3,))]
        + shapes[2:]
        + Tokens.semaphores(grid, 2)
        + [sem((sz.before,))] * 2
        + [sem((grid.gx - 1,))] * 2
        + [sem((grid.gy - 1,))] * 2
        + sems,
        compiler_params=params(1),
        name="last_half",
    )(shape(both), shape(down), shape(w_all), w_attn, *kept, back, hidden, h, dy, scale_two)


def einsum(form, a, b):
    return jnp.einsum(form, a, b, preferred_element_type=F32)


def padded(a, axis, size):
    pads = [(0, 0)] * a.ndim
    pads[axis] = (0, size - a.shape[axis])
    return jnp.pad(a, pads) if size != a.shape[axis] else a


def shards(
    grid,
    block_input,
    attn_gain,
    query_weight,
    key_weight,
    value_weight,
    output_weight,
    ffn_gain,
    gate_weight,
    up_weight,
    down_weight,
    segment_ids,
    out_cotangent,
):
    GX, GY = grid.gx, grid.gy
    rows, row_tokens = block_input.shape
    tok = row_tokens // GX
    sz = Sizes(grid, tok, rows, query_weight.shape[1], key_weight.shape[1])
    fc, features = gate_weight.shape[1], sz.features
    groups = [
        jnp.concatenate([query_weight, key_weight, value_weight, output_weight.T], axis=1), gate_weight, up_weight, down_weight.T
    ]
    width = -(-max(g.shape[1] for g in groups) // 128) * 128
    block = jnp.concatenate([padded(g, 1, width) for g in groups], axis=1)
    small = jnp.concatenate(
        [segment_ids.reshape(sz.span, tok).astype(F32), padded(jnp.stack([attn_gain, ffn_gain]), 1, tok)], axis=0
    )
    small = padded(small, 0, -(-small.shape[0] // 8) * 8)
    (
        x_parts, dy_parts, w_all, w_attn, _, normed_one, scale_one, query, key_value, earlier, mixed, bias, tables, gains,
        hidden_in, normed_two, scale_two,
    ) = first_half(sz, row_tokens // PACKED_LENGTH, block_input, out_cotangent, small, block)
    dy_half = dy_parts.reshape(features, tok)
    w_cols = w_all.reshape(GY, features, -1)
    w_gate, w_up, w_down = (w_cols[:, :, k * width : k * width + fc] for k in range(1, 4))
    normed_two = normed_two.reshape(features, tok)

    gate = einsum("jdf,dt->jft", w_gate, normed_two)
    up = einsum("jdf,dt->jft", w_up, normed_two)
    sigmoid = jax.nn.sigmoid(gate)
    hidden = padded((jax.nn.silu(gate) * up).astype(BF16), 1, width)
    hidden_grad = einsum("jdf,dt->jft", w_down, dy_half)
    gate_back = (hidden_grad * up * sigmoid * (1.0 + gate * (1.0 - sigmoid))).astype(BF16)
    up_back = (hidden_grad * gate * sigmoid).astype(BF16)
    both_back = jnp.concatenate([padded(gate_back, 1, width), padded(up_back, 1, width)], axis=1)
    grad_both = einsum("dt,jft->jdf", normed_two, both_back).astype(BF16)
    grad_down = einsum("dt,jft->jdf", dy_half, hidden).astype(BF16)
    block_output, input_grad, grads, gains = last_half(
        sz, grad_both, grad_down, w_all, w_attn,
        (x_parts, normed_one, scale_one, query, key_value, earlier, mixed, bias, tables, gains),
        both_back, hidden, hidden_in, dy_parts, scale_two,
    )
    grad_gate, grad_up, grad_down, grad_attn = (grads[:, k * width : (k + 1) * width] for k in range(GROUPS))
    qc, kc = sz.qc, sz.kc
    return (
        block_output,
        input_grad.astype(F32),
        gains[0, :rows],
        grad_attn[:, :qc],
        grad_attn[:, qc : qc + kc],
        grad_attn[:, qc + kc : sz.qkv],
        grad_attn[:, sz.qkv : sz.qkv + qc].T,
        gains[1, :rows],
        grad_gate[:, :fc],
        grad_up[:, :fc],
        grad_down[:, :fc].T,
    )


def solution(mesh):
    grid = Grid(mesh.shape["gx"], mesh.shape["gy"])
    return jax.shard_map(
        functools.partial(shards, grid),
        mesh=mesh,
        in_specs=(
            P("gx", "gy"),
            P("gx"),
            P("gx", "gy"),
            P("gx", "gy"),
            P("gx", "gy"),
            P("gy", "gx"),
            P("gx"),
            P("gx", "gy"),
            P("gx", "gy"),
            P("gy", "gx"),
            P("gx", None),
            P("gx", "gy"),
        ),
        out_specs=(
            P("gx", "gy"),
            P("gx", "gy"),
            P("gx"),
            P("gx", "gy"),
            P("gx", "gy"),
            P("gx", "gy"),
            P("gy", "gx"),
            P("gx"),
            P("gx", "gy"),
            P("gx", "gy"),
            P("gy", "gx"),
        ),
        check_vma=False,
    )
```

```python
import functools
import math

import jax
import jax.numpy as jnp
from jax import lax
from jax.experimental import pallas as pl
from jax.experimental.pallas import tpu as pltpu
from jax.sharding import PartitionSpec as P

QUERY_HEADS = 15
KEY_VALUE_HEADS = 5
HEAD_SIZE = 64
PACKED_LENGTH = 1024
LONGEST_SEGMENT = 512

EPS = 1e-05
THETA = 10000.0
MESH = pl.DeviceIdType.MESH
F32 = jnp.float32
BF16 = jnp.bfloat16


class Grid:
    def __init__(self, gx, gy):
        self.gx, self.gy = gx, gy
        self.C = 2 if gy % 2 == 0 else 1
        self.X = gy // self.C
        self.Y = self.X if gx % self.X == 0 else 1
        self.Z = gx // self.Y
        self.size = {"z": self.Z, "y": self.Y, "x": self.X}

    def here(self):
        i, j = lax.axis_index("gx"), lax.axis_index("gy")
        return {"z": i // self.Y, "y": i % self.Y, "x": j // self.C, "c": j % self.C}

    def device(self, at):
        return (at["z"] * self.Y + at["y"], at["x"] * self.C + at["c"])


def remote(src, dst, send, recv, device):
    return pltpu.make_async_remote_copy(
        src_ref=src, dst_ref=dst, send_sem=send, recv_sem=recv, device_id=device, device_id_type=MESH
    )


def greet(devices):
    barrier = pltpu.get_barrier_semaphore()
    for device in devices:
        pl.semaphore_signal(barrier, inc=1, device_id=device, device_id_type=MESH)
    pl.semaphore_wait(barrier, len(devices))


def row_peers(n, me):
    return [(d, lax.rem(me + d, n)) for d in range(1, n)]


def line(n, here):
    found = []
    for k in range(1, n):
        if n & (n - 1):
            found.append((lax.rem(here + k, n), lax.rem(here + n - k, n)))
            continue
        place, bit = 0, 1
        while bit < n:
            digit = (here // bit) % 2
            place = place + bit * ((1 - digit) if k & bit else digit)
            bit *= 2
        found.append((place, place))
    return found


def places(n, here):
    return [here] + [origin for _, origin in line(n, here)]


def gather_sites(grid, me, order):
    other = [grid.device({**me, "c": 1 - me["c"]})] if grid.C == 2 else []
    onward = [[grid.device({**me, axis: to}) for to, _ in line(grid.size[axis], me[axis])] for axis in order]
    yield 0, dict(me), sum(onward, []) + other
    for stage, axis in enumerate(order, 1):
        earlier = [dict(me)]
        for done in order[: stage - 1]:
            earlier = [{**e, done: place} for place in places(grid.size[done], me[done]) for e in earlier]
        for _, origin in line(grid.size[axis], me[axis]):
            for e in earlier:
                yield stage, {**e, axis: origin}, sum(onward[stage:], []) + other


def core_sites(grid, me):
    found = [{"c": 1 - me["c"]}]
    for axis in "xyz":
        found = [{**f, axis: place} for place in places(grid.size[axis], me[axis]) for f in found]
    return found


GROUPS = 4


class Lane:
    def __init__(self, order, first, part, parts, width, base, step):
        self.order, self.first, self.part, self.parts, self.width = order, first, part, parts, width
        self.base, self.step, self.count = base, step, GROUPS

    def columns(self, m):
        return pl.ds(pl.multiple_of(self.base + m * self.step, 128), self.width)

    def own_columns(self, m):
        return pl.ds(pl.multiple_of(m * self.width, 128), self.width)

    def at(self, slot, body):
        slots = self.count * self.parts
        if isinstance(slot, int):
            if 0 <= slot < slots and slot % self.parts == self.part:
                body(slot // self.parts)
            return
        active = (slot >= 0) & (slot < slots)
        if self.parts > 1:
            active = active & (slot % self.parts == self.part)
        pl.when(active)(lambda: body(slot // self.parts))


class Plan:
    def __init__(self, cols, orders, parts):
        tiles = cols // 128 // GROUPS
        most = -(-tiles * 3 // 5)
        self.lanes, self.parts, self.slots, at = [], parts, GROUPS * parts, 0
        for part in range(parts):
            for order, total in zip(orders, (most, tiles - most)):
                width = total // parts + (part < total % parts)
                if width:
                    self.lanes.append(Lane(order, GROUPS * len(self.lanes), part, parts, width * 128, at * 128, tiles * 128))
                    at += width
        self.chunks = GROUPS * len(self.lanes)


GATHER_ORDERS = ("zyx", "zxy")
REDUCE_ORDERS = ("xyz", "yxz")
GATHER_PARTS, REDUCE_PARTS = 1, 1


def place_of(grid, piece):
    return piece["x"] * grid.C + piece["c"], piece["z"] * grid.Y + piece["y"]


def other_core(grid, me):
    return grid.device({**me, "c": 1 - me["c"]})


def peers_of(grid, i, j):
    return [(p, j) for _, p in row_peers(grid.gx, i)] + [(i, p) for _, p in row_peers(grid.gy, j)]


class Spread:
    def __init__(self, grid, me, plan, w_ref, out, send, recv):
        self.grid, self.me, self.plan = grid, me, plan
        self.w_ref, self.out, self.send, self.recv = w_ref, out, send, recv
        self.sites = [list(gather_sites(grid, me, lane.order)) for lane in plan.lanes]

    @staticmethod
    def count(grid):
        me = {"z": 0, "y": 0, "x": 0, "c": 0}
        return max(sum(len(sends) for _, _, sends in gather_sites(grid, me, order)) for order in GATHER_ORDERS)

    @staticmethod
    def semaphores(grid, plan):
        return [
            pltpu.SemaphoreType.DMA((Spread.count(grid), plan.chunks)),
            pltpu.SemaphoreType.DMA((grid.gy, grid.gx, plan.chunks)),
        ]

    def stage(self, stage, slot, finish=False):
        for lane, sites in zip(self.plan.lanes, self.sites):
            lane.at(slot, lambda m, lane=lane, sites=sites: self.chunk(lane, sites, stage, m, finish))

    def chunk(self, lane, sites, stage, m, finish):
        number, chunk = 0, lane.first + m
        for at, piece, sends in sites:
            first = number
            number += len(sends)
            if at != stage:
                continue
            j, i = place_of(self.grid, piece)
            land = self.out.at[j, i, :, lane.columns(m)]
            src = self.w_ref.at[:, lane.columns(m)] if at == 0 else land
            arrived = self.recv.at[j, i, chunk]
            if at and not finish:
                remote(land, land, self.send.at[first, chunk], arrived, (0, 0)).wait_recv()
            for n, device in enumerate(sends):
                copy = remote(src, land, self.send.at[first + n, chunk], arrived, device)
                if finish:
                    copy.wait_send()
                else:
                    copy.start()

    def start(self):
        self.stage(0, 0)
        self.stage(0, 1)

    def slot(self, t):
        self.stage(0, t + 2)
        for stage in (2, 3, 1):
            self.stage(stage, t - (stage - 1))

        @pl.when(t == 2)
        def _():
            self.cores(0)

    def cores(self, slot):
        for lane in self.plan.lanes:
            lane.at(slot, functools.partial(self.core, lane))

    def core(self, lane, m):
        if self.grid.C == 2:
            for piece in core_sites(self.grid, self.me):
                j, i = place_of(self.grid, piece)
                land, chunk = self.out.at[j, i, :, lane.columns(m)], lane.first + m
                remote(land, land, self.send.at[0, chunk], self.recv.at[j, i, chunk], (0, 0)).wait_recv()

    def finish(self):
        def end(t, carry):
            pl.when(t > 0)(lambda: self.cores(t))
            for stage in range(4):
                self.stage(stage, t, True)
            return carry

        lax.fori_loop(0, self.plan.slots, end, 0)


class Tokens:
    def __init__(self, grid, i, j, tok, send, recv, local, pairs):
        self.grid, self.i, self.j, self.tok = grid, i, j, tok
        self.send, self.recv, self.local, self.pairs = send, recv, local, pairs

    @staticmethod
    def semaphores(grid, n):
        return [
            pltpu.SemaphoreType.DMA((n, grid.gx - 1)),
            pltpu.SemaphoreType.DMA((n, grid.gx - 1)),
            pltpu.SemaphoreType.DMA((n,)),
        ]

    def of(self, ref, p):
        return ref.at[:, pl.ds(pl.multiple_of(p * self.tok, self.tok), self.tok)]

    def own(self, n):
        pick, land = self.pairs[n]
        return pltpu.make_async_copy(pick(self, self.i), land(self, self.i), self.local.at[n])

    def start(self, n):
        pick, land = self.pairs[n]
        for d, p in row_peers(self.grid.gx, self.i):
            remote(pick(self, p), land(self, self.i), self.send.at[n, d - 1], self.recv.at[n, d - 1], (p, self.j)).start()
        self.own(n).start()

    def finish(self, n):
        pick, land = self.pairs[n]
        for d, p in row_peers(self.grid.gx, self.i):
            sems = self.send.at[n, d - 1], self.recv.at[n, d - 1]
            remote(pick(self, p), land(self, self.i), *sems, (p, self.j)).wait_send()
            back = land(self, lax.rem(self.i + self.grid.gx - d, self.grid.gx))
            remote(back, back, *sems, (p, self.j)).wait_recv()
        self.own(n).wait()


def dot(a, b, contract):
    return lax.dot_general(a, b, ((contract[:1], contract[1:]), ((), ())), preferred_element_type=F32)


def attention_bias(seg_query, seg_window):
    tok, window = seg_query.shape[0], seg_window.shape[1]
    row = lax.broadcasted_iota(jnp.int32, (tok, window), 0) + (window - tok)
    column = lax.broadcasted_iota(jnp.int32, (tok, window), 1)
    return jnp.where((seg_query == seg_window) & (column <= row), 0.0, -jnp.inf).astype(F32)


def head_rows(head):
    return pl.ds(pl.multiple_of(head * HEAD_SIZE, HEAD_SIZE), HEAD_SIZE)


def in_window(win_ref, own_ref, head):
    parts = [win_ref[n, head_rows(head), :] for n in reversed(range(win_ref.shape[0]))]
    return jnp.concatenate(parts + [own_ref[head_rows(head), :]], axis=1)


def probabilities(query, key, bias):
    scores = dot(query, key, (0, 0)) * HEAD_SIZE ** (-0.5) + bias
    raised = jnp.exp(scores - jnp.max(scores, axis=1, keepdims=True))
    return raised * (1.0 / jnp.sum(raised, axis=1, keepdims=True))


def attend(k, kv_heads, groups, q_ref, win_ref, own_ref, bias_ref, o_ref):
    key, value = in_window(win_ref, own_ref, k), in_window(win_ref, own_ref, kv_heads + k)
    for g in range(groups):
        rows = head_rows(k * groups + g)
        prob = probabilities(q_ref[rows, :], key, bias_ref[...]).astype(BF16)
        o_ref[rows, :] = dot(value, prob, (1, 1)).astype(BF16).astype(F32)


def attend_back(k, kv_heads, groups, q_ref, do_ref, win_ref, own_ref, bias_ref, dq_ref, dkv_out, dkv_own):
    key, value = in_window(win_ref, own_ref, k), in_window(win_ref, own_ref, kv_heads + k)
    key_grad = value_grad = None
    for g in range(groups):
        rows = head_rows(k * groups + g)
        query, grad = q_ref[rows, :], do_ref[rows, :]
        prob = probabilities(query, key, bias_ref[...])
        prob_grad = dot(grad, value, (0, 0))
        row_dot = jnp.sum(prob * prob_grad, axis=1, keepdims=True)
        score_grad = (prob * (prob_grad - row_dot) * HEAD_SIZE ** (-0.5)).astype(BF16)
        dq_ref[rows, :] = dot(key, score_grad, (1, 1))
        dk = dot(query, score_grad, (1, 0))
        dv = dot(grad, prob.astype(BF16), (1, 0))
        key_grad = dk if g == 0 else key_grad + dk
        value_grad = dv if g == 0 else value_grad + dv
    tok = q_ref.shape[1]
    for head, grad in ((k, key_grad), (kv_heads + k, value_grad)):
        before = dkv_out.shape[0]
        for n in range(before):
            at = before - 1 - n
            dkv_out[n, head_rows(head), :] = grad[:, at * tok : (at + 1) * tok].astype(BF16)
        dkv_own[head_rows(head), :] = grad[:, before * tok :]


def over(ref, body):
    lead = ref.shape[:-2]
    total = math.prod(lead)

    def one(k, carry):
        place = []
        for n in reversed(lead):
            place.append(k % n)
            k = k // n
        body(tuple(reversed(place)))
        return carry

    if total == 1:
        body((0,) * len(lead))
    else:
        lax.fori_loop(0, total, one, 0)


def add_into(target, source):
    def one(place):
        where = place + (slice(None), slice(None))
        target[where] = target[where] + source[where]

    over(target, one)


DIMS = "xzy"


class Collect:
    def __init__(self, grid, me, plan, acc, from_core, lands, out, c_s, c_r, c_l, l_s, l_r):
        self.grid, self.me, self.plan = grid, me, plan
        self.acc, self.from_core, self.lands, self.out = acc, from_core, lands, out
        self.c_s, self.c_r, self.c_l, self.l_s, self.l_r = c_s, c_r, c_l, l_s, l_r
        self.actions = [self.actions_of(n, lane) for n, lane in enumerate(plan.lanes)]
        self.lags = max(len(actions) for actions in self.actions)

    @staticmethod
    def axes(grid, lane):
        return [axis for axis in lane.order if grid.size[axis] > 1]

    @staticmethod
    def scratch(grid, plan, rows, cols):
        size = (grid.X, grid.Z, grid.Y, rows, cols)
        shapes = [pltpu.VMEM(size, BF16), pltpu.VMEM(size, BF16)]
        for lane in plan.lanes:
            axes = Collect.axes(grid, lane)
            for level, axis in enumerate(axes):
                rest = tuple(grid.size[d] for d in DIMS if d in axes[level + 1 :])
                shapes.append(pltpu.VMEM((grid.size[axis] - 1,) + rest + (rows, lane.count * lane.width), BF16))
        sem = pltpu.SemaphoreType.DMA
        most = max(n - 1 for n in grid.size.values())
        levels = len(shapes) - 2
        return shapes, [sem((grid.X, plan.chunks))] * 3 + [sem((levels, most, plan.chunks))] * 2

    def own_copy(self, x, lane, m, g_ref, columns):
        src, chunk = g_ref.at[x * self.grid.C + self.me["c"], :, :, :, columns], lane.first + m
        return pltpu.make_async_copy(src, self.acc.at[x, :, :, :, lane.columns(m)], self.c_l.at[x, chunk])

    def core_copy(self, x, lane, m, g_ref, columns):
        src, chunk = g_ref.at[x * self.grid.C + 1 - self.me["c"], :, :, :, columns], lane.first + m
        land = self.from_core.at[x, :, :, :, lane.columns(m)]
        return remote(src, land, self.c_s.at[x, chunk], self.c_r.at[x, chunk], other_core(self.grid, self.me))

    def start(self, source):
        self.source = source
        for slot in range(self.plan.slots - self.plan.parts):
            self.load(slot)

    def load(self, slot):
        for lane in self.plan.lanes:

            def body(m, lane=lane):
                ref, at = self.source(lane.base + m * lane.step)
                for x in range(self.grid.X):
                    self.own_copy(x, lane, m, ref, pl.ds(at, lane.width)).start()
                    if self.grid.C == 2:
                        self.core_copy(x, lane, m, ref, pl.ds(at, lane.width)).start()

            lane.at(slot, body)

    def core(self, lane, m):
        columns = lane.columns(m)
        ref, _ = self.source(0)
        for x in range(self.grid.X):
            self.own_copy(x, lane, m, ref, pl.ds(0, lane.width)).wait()
            if self.grid.C == 2:
                self.core_copy(x, lane, m, ref, pl.ds(0, lane.width)).wait_recv()
                add_into(self.acc.at[x, :, :, :, columns], self.from_core.at[x, :, :, :, columns])

    def level(self, number, lane, level):
        axes = self.axes(self.grid, lane)
        axis = axes[level]
        index = sum(len(self.axes(self.grid, other)) for other in self.plan.lanes[:number]) + level
        free = len(axes) - level - 1

        def pick(t, m):
            place = []
            for d in DIMS:
                if d == axis:
                    place.append(t)
                elif d in axes[level + 1 :]:
                    place.append(slice(None))
                else:
                    place.append(self.me[d] if self.grid.size[d] > 1 else 0)
            return self.acc.at[tuple(place) + (slice(None), lane.columns(m))]

        def land(slot, m):
            return self.lands[index].at[(slot,) + (slice(None),) * (free + 1) + (lane.own_columns(m),)]

        def copies(m):
            for slot, (to, _) in enumerate(line(self.grid.size[axis], self.me[axis])):
                sems = self.l_s.at[index, slot, lane.first + m], self.l_r.at[index, slot, lane.first + m]
                yield slot, remote(pick(to, m), land(slot, m), *sems, self.grid.device({**self.me, axis: to}))

        return self.me[axis], pick, land, copies

    def actions_of(self, number, lane):
        levels = [self.level(number, lane, level) for level in range(len(self.axes(self.grid, lane)))]

        def send(m, copies):
            for _, copy in copies(m):
                copy.start()

        def take(m, p, pick, land, copies, last):
            columns = lane.columns(m)
            if last:
                self.out[:, columns] = pick(p, m)[...].astype(F32)
            for slot, copy in copies(m):
                copy.wait_recv()
                if last:
                    self.out[:, columns] += land(slot, m)[...].astype(F32)
                else:
                    add_into(pick(p, m), land(slot, m))

        actions = [[functools.partial(self.core, lane)]]
        for number, (p, pick, land, copies) in enumerate(levels):
            actions[-1].append(functools.partial(send, copies=copies))
            last = number == len(levels) - 1
            actions.append([functools.partial(take, p=p, pick=pick, land=land, copies=copies, last=last)])
        return actions

    def begin(self, slot):
        for lane, actions in zip(self.plan.lanes, self.actions):
            for action in actions[0]:
                lane.at(slot, action)

    def slot(self, t):
        for lag in range(1, self.lags):
            for lane, actions in zip(self.plan.lanes, self.actions):
                if lag < len(actions):
                    for action in actions[lag]:
                        lane.at(t - lag, action)

    def finish(self):
        def end(t, carry):
            for number, lane in enumerate(self.plan.lanes):

                def body(m, number=number, lane=lane):
                    if self.grid.C == 2:
                        ref, _ = self.source(0)
                        for x in range(self.grid.X):
                            self.core_copy(x, lane, m, ref, pl.ds(0, lane.width)).wait_send()
                    for level in range(len(self.axes(self.grid, lane))):
                        for _, copy in self.level(number, lane, level)[-1](m):
                            copy.wait_send()

                lane.at(t, body)
            return carry

        lax.fori_loop(0, self.plan.slots, end, 0)


class Shift:
    def __init__(self, span, i, j, sign, pick, land, send, recv):
        self.i, self.j, self.q, self.span, self.sign = i, j, i % span, span, sign
        self.pick, self.land, self.send, self.recv = pick, land, send, recv

    def copy(self, n):
        sems = self.send.at[n], self.recv.at[n]
        return remote(self.pick(n), self.land(n), *sems, (self.i + self.sign * (n + 1), self.j))

    def before(self, n):
        return self.q >= n + 1

    def after(self, n):
        return self.q + n + 1 < self.span

    def start(self, slots):
        for n in range(slots):
            pl.when(self.after(n) if self.sign > 0 else self.before(n))(lambda n=n: self.copy(n).start())

    def finish(self, slots, arrived, missing=None):
        for n in range(slots):
            there, goes = (self.before(n), self.after(n)) if self.sign > 0 else (self.after(n), self.before(n))

            def take(n=n):
                self.copy(n).wait_recv()
                arrived(n)

            pl.when(there)(take)
            if missing is not None:
                pl.when(jnp.logical_not(there))(lambda n=n: missing(n))
            pl.when(goes)(lambda n=n: self.copy(n).wait_send())


HBM_SPEC = pl.BlockSpec(memory_space=pl.ANY)
VMEM_SPEC = pl.BlockSpec(memory_space=pltpu.VMEM)


def params(collective_id):
    return pltpu.CompilerParams(
        collective_id=collective_id, has_side_effects=True, vmem_limit_bytes=63 * 1024 * 1024
    )


def column_of(row, size):
    n = row.shape[1]
    same = lax.broadcasted_iota(jnp.int32, (size, n), 0) == lax.broadcasted_iota(jnp.int32, (size, n), 1)
    return jnp.sum(jnp.where(same, row, 0.0), axis=1, keepdims=True)


def row_of(column, size):
    n = column.shape[0]
    same = lax.broadcasted_iota(jnp.int32, (n, size), 0) == lax.broadcasted_iota(jnp.int32, (n, size), 1)
    return jnp.sum(jnp.where(same, column, 0.0), axis=0, keepdims=True)


class Sizes:
    def __init__(self, grid, tok, rows, qc, kc):
        self.grid, self.tok, self.rows, self.qc, self.kc = grid, tok, rows, qc, kc
        self.features = rows * grid.gx
        self.q, self.kv = qc * grid.gy, kc * grid.gy
        self.heads, self.kv_heads = self.q // HEAD_SIZE, self.kv // HEAD_SIZE
        self.groups = self.heads // self.kv_heads
        self.span = PACKED_LENGTH // tok
        self.before = -(-(LONGEST_SEGMENT - 1) // tok)
        self.window = (self.before + 1) * tok
        self.qkv = qc + 2 * kc


def turn(ref, row, cos_table, sine_table, direction):
    half = HEAD_SIZE // 2
    lower = ref[pl.ds(row, half), :]
    upper = ref[pl.ds(pl.multiple_of(row + half, half), half), :]
    if direction > 0:
        lower, upper = lower.astype(BF16).astype(F32), upper.astype(BF16).astype(F32)
    return jnp.concatenate(
        [lower * cos_table - direction * upper * sine_table, upper * cos_table + direction * lower * sine_table], axis=0
    )


def first_kernel(
    sz, plan, width, row_sequences, x_ref, dy_ref, small_ref, w_ref,
    xo, dyo, wo, w_attn, smallo, xn_ref, scale_ref, q_ref, kv_ref, win, o_ref, bias, tables, gains, h_ref, xn2_ref, scale2_ref,
    raw, o_full, t_s, t_r, t_l, k_s, k_r, w_l, w_s, w_r,
):
    grid, tok = sz.grid, sz.tok
    me = grid.here()
    i, j = lax.axis_index("gx"), lax.axis_index("gy")
    greet(peers_of(grid, i, j))
    pairs = [
        (lambda c, p: small_ref, lambda c, p: smallo.at[p]),
        (lambda c, p: c.of(x_ref, p), lambda c, p: xo.at[p]),
        (lambda c, p: c.of(dy_ref, p), lambda c, p: dyo.at[p]),
    ]
    tokens = Tokens(grid, i, j, tok, t_s, t_r, t_l, pairs)
    spread = Spread(grid, me, plan, w_ref, wo, w_s, w_r)
    tokens.start(0)
    spread.start()
    tokens.start(1)
    pltpu.make_async_copy(w_ref, wo.at[j, i], w_l.at[0]).start()
    shift = Shift(sz.span, i, j, 1, lambda n: kv_ref, lambda n: win.at[n], k_s, k_r)
    sequence, q = j * row_sequences + i // sz.span, i % sz.span
    half = HEAD_SIZE // 2

    def norm(parts, scale_out, gain, out):
        total = None
        for k in range(grid.gx):
            value = parts(k)
            part = jnp.sum(value * value, axis=0, keepdims=True)
            total = part if k == 0 else total + part
        scale = lax.rsqrt(total / sz.features + EPS)
        scale_out[...] = scale
        for k in range(grid.gx):
            out[k] = (parts(k) * scale * gains[k, :, gain : gain + 1]).astype(BF16)

    def prepare():
        tokens.finish(0)

        def segments(place):
            row = smallo[sequence, pl.ds(jnp.maximum(place, 0), 1), :][:, :tok]
            return jnp.where(place >= 0, row, -1.0)

        here = segments(q)
        bias[...] = attention_bias(
            column_of(here, tok), jnp.concatenate([segments(q - n) for n in range(sz.before, 0, -1)] + [here], axis=1)
        )
        first = jnp.zeros((1, tok), F32)
        for n in range(sz.span):
            other = column_of(smallo[sequence, n : n + 1, :][:, :tok], tok)
            first = first + jnp.sum(jnp.where(other < here, 1.0, 0.0), axis=0, keepdims=True)
        positions = (q * tok).astype(F32) + lax.broadcasted_iota(jnp.int32, (1, tok), 1).astype(F32) - first
        frequency = jnp.exp(
            -math.log(THETA) * lax.broadcasted_iota(jnp.int32, (half, 1), 0).astype(F32) / half
        )
        angles = frequency * positions
        tables[0] = jnp.cos(angles)
        tables[1] = jnp.sin(angles)
        for k in range(grid.gx):
            columns = [column_of(smallo[k, sz.span + n : sz.span + n + 1, :][:, :tok], sz.rows) for n in range(2)]
            gains[k] = jnp.concatenate(columns, axis=1)

    def first_norm():
        tokens.finish(1)
        norm(lambda k: xo[k].astype(F32), scale_ref, 0, xn_ref)

    def project():
        pltpu.make_async_copy(w_ref, wo.at[j, i], w_l.at[0]).wait()
        copy = pltpu.make_async_copy(wo.at[:, :, :, pl.ds(0, width)], w_attn, w_l.at[0])
        copy.start()
        copy.wait()

        def column(b, carry):
            total = None
            for k in range(grid.gx):
                part = dot(w_attn[b, k][:, : sz.qkv], xn_ref[k], (0, 0))
                total = part if k == 0 else total + part
            for part, at, size in ((0, 0, sz.qc), (sz.qc, sz.q, sz.kc), (sz.qc + sz.kc, sz.q + sz.kv, sz.kc)):
                raw[pl.ds(pl.multiple_of(at + b * size, 8), size), :] = total[part : part + size]
            return carry

        lax.fori_loop(0, grid.gy, column, 0)

        def key(k, carry):
            kv_ref[head_rows(k), :] = turn(raw, pl.multiple_of(sz.q + k * HEAD_SIZE, HEAD_SIZE), tables[0], tables[1], 1).astype(BF16)
            kv_ref[head_rows(sz.kv_heads + k), :] = raw[head_rows(sz.heads + sz.kv_heads + k), :].astype(BF16)
            return carry

        lax.fori_loop(0, sz.kv_heads, key, 0)
        shift.start(sz.before)

        def query(k, carry):
            q_ref[head_rows(k), :] = turn(raw, pl.multiple_of(k * HEAD_SIZE, HEAD_SIZE), tables[0], tables[1], 1).astype(BF16)
            return carry

        lax.fori_loop(0, sz.heads, query, 0)

    def zero(n):
        win[n] = jnp.zeros(win.shape[1:], BF16)

    def mix():
        def block(k, carry):
            total = xo[k].astype(F32)
            for b in range(grid.gy):
                mixed = o_full[pl.ds(b * sz.qc, sz.qc), :].astype(BF16)
                total = total + dot(w_attn[b, k][:, sz.qkv : sz.qkv + sz.qc], mixed, (1, 0))
            h_ref[k] = total
            return carry

        lax.fori_loop(0, grid.gx, block, 0)
        norm(lambda k: h_ref[k], scale2_ref, 1, xn2_ref)
        o_ref[...] = o_full[...].astype(BF16)

    each = -(-sz.kv_heads // 2)

    def slot(t, carry):
        spread.slot(t)
        pl.when(t == 0)(prepare)
        pl.when(t == 1)(first_norm)
        pl.when(t == 2)(lambda: tokens.start(2))
        pl.when(t == 2)(project)
        pl.when(t == 3)(lambda: shift.finish(sz.before, lambda n: None, zero))

        @pl.when((t == 3) | (t == 4))
        def _():
            def one(k, carry):
                attend(k, sz.kv_heads, sz.groups, q_ref, win, kv_ref, bias, o_full)
                return carry

            lax.fori_loop((t - 3) * each, jnp.minimum((t - 2) * each, sz.kv_heads), one, 0)

        pl.when(t == 5)(mix)
        return carry

    lax.fori_loop(0, plan.slots + 2, slot, 0)
    spread.finish()
    tokens.finish(2)


def first_half(sz, row_sequences, x, dy, small, w):
    grid, tok = sz.grid, sz.tok
    rows, cols = w.shape
    width = cols // GROUPS
    plan = Plan(cols, GATHER_ORDERS, GATHER_PARTS)
    parts = (grid.gx, sz.rows, tok)
    outs = [
        (parts, BF16, VMEM_SPEC),
        (parts, BF16, HBM_SPEC),
        ((grid.gy, grid.gx, rows, cols), BF16, HBM_SPEC),
        ((grid.gy, grid.gx, rows, width), BF16, VMEM_SPEC),
        ((grid.gx,) + small.shape, F32, VMEM_SPEC),
        (parts, BF16, VMEM_SPEC),
        ((1, tok), F32, VMEM_SPEC),
        ((sz.q, tok), BF16, VMEM_SPEC),
        ((2 * sz.kv, tok), BF16, VMEM_SPEC),
        ((sz.before, 2 * sz.kv, tok), BF16, VMEM_SPEC),
        ((sz.q, tok), BF16, VMEM_SPEC),
        ((tok, sz.window), F32, VMEM_SPEC),
        ((2, HEAD_SIZE // 2, tok), F32, VMEM_SPEC),
        ((grid.gx, sz.rows, 2), F32, VMEM_SPEC),
        (parts, F32, VMEM_SPEC),
        (parts, BF16, VMEM_SPEC),
        ((1, tok), F32, VMEM_SPEC),
    ]
    return pl.pallas_call(
        functools.partial(first_kernel, sz, plan, width, row_sequences),
        out_shape=[jax.ShapeDtypeStruct(shape, dtype) for shape, dtype, _ in outs],
        in_specs=[VMEM_SPEC] * 4,
        out_specs=[spec for _, _, spec in outs],
        scratch_shapes=[pltpu.VMEM((sz.q + 2 * sz.kv, tok), F32), pltpu.VMEM((sz.q, tok), F32)]
        + Tokens.semaphores(grid, 3)
        + [pltpu.SemaphoreType.DMA((sz.before,))] * 2
        + [pltpu.SemaphoreType.DMA((1,))]
        + Spread.semaphores(grid, plan),
        compiler_params=params(0),
        name="first_half",
    )(x, dy, small, w)


def last_kernel(
    sz, plan, width, both_ref, down_ref, w_all, w_attn, xo, xn_ref, scale_ref, q_ref, kv_ref, win, o_ref, bias, tables, gains,
    back_ref, hidden_ref, h_ref, dy_ref, scale2_ref,
    bo, ig, go, gaino,
    do_ref, dh_ref, dh_half, bo_ref, dq, dkv_out, dkv_in, dkv, g_attn, dx, y_acc, ig_parts, gain_parts, gain_in, gain_row,
    gain_across, acc, from_core, b_l, *refs,
):
    lands, (t_s, t_r, t_l, k_s, k_r, g_s, g_r, h_s, h_r, *sems) = refs[:-14], refs[-14:]
    grid, tok = sz.grid, sz.tok
    me = grid.here()
    i, j = lax.axis_index("gx"), lax.axis_index("gy")
    peers, across = row_peers(grid.gx, i), row_peers(grid.gy, j)
    greet(peers_of(grid, i, j))
    collect = Collect(grid, me, plan, acc, from_core, lands, go, *sems)

    def source(first):
        if first < 2 * width:
            return both_ref, first
        return (down_ref, first - 2 * width) if first < 3 * width else (g_attn, first - 3 * width)

    collect.start(source)
    pairs = [
        (lambda c, p: bo_ref.at[p], lambda c, p: c.of(bo, p)),
        (lambda c, p: ig_parts.at[p], lambda c, p: c.of(ig, p)),
    ]
    tokens = Tokens(grid, i, j, tok, t_s, t_r, t_l, pairs)
    shift = Shift(sz.span, i, j, -1, lambda n: dkv_out.at[n], lambda n: dkv_in.at[n], k_s, k_r)

    def column_copies():
        for d, p in peers:
            yield d, remote(gain_parts.at[p], gain_in.at[d - 1], g_s.at[d - 1], g_r.at[d - 1], (p, j))

    def across_copies():
        for d, p in across:
            yield d, remote(gain_row, gain_across.at[d - 1], h_s.at[d - 1], h_r.at[d - 1], (i, p))

    def heads_of(part):
        def one(k, carry):
            attend_back(k, sz.kv_heads, sz.groups, q_ref, do_ref, win, kv_ref, bias, dq, dkv_out, dkv)
            return carry

        each = -(-sz.kv_heads // (2 * plan.parts))
        lax.fori_loop(part * each, jnp.minimum((part + 1) * each, sz.kv_heads), one, 0)

    def feed_back():
        dx[...] = jnp.zeros_like(dx)
        y_acc[...] = jnp.zeros_like(y_acc)

        def column(b, carry):
            copies = [
                pltpu.make_async_copy(w_all.at[b, :, :, :, pl.ds((n + 1) * width, width)], g_attn.at[n], b_l.at[n])
                for n in range(3)
            ]
            for copy in copies:
                copy.start()
            for copy in copies:
                copy.wait()
            for k in range(grid.gx):
                at = k // grid.Y, k % grid.Y
                dx[k] += dot(g_attn[(0,) + at], back_ref[b, :width, :], (1, 0)) + dot(
                    g_attn[(1,) + at], back_ref[b, width:, :], (1, 0)
                )
                y_acc[k] += dot(g_attn[(2,) + at], hidden_ref[b], (1, 0))
            return carry

        lax.fori_loop(0, grid.gy, column, 0)
        scale = scale2_ref[...]
        inner = None
        for k in range(grid.gx):
            part = jnp.sum(dx[k] * gains[k, :, 1:2] * h_ref[k], axis=0, keepdims=True)
            inner = part if k == 0 else inner + part
        inner = scale * scale * scale * inner / sz.features
        for k in range(grid.gx):
            value, grad = h_ref[k], dx[k]
            gain_parts[k] = jnp.zeros((8, 128), F32)
            gain_parts[k, 1:2, :] = row_of(jnp.sum(grad * value * scale, axis=1, keepdims=True), 128)
            bo_ref[k] = (value + y_acc[k]).astype(BF16)
            back = dy_ref[k].astype(F32) + (scale * (grad * gains[k, :, 1:2]) - value * inner)
            dh_ref[k] = back
            dh_half[k] = back.astype(BF16)

        def heads(b, carry):
            total = None
            for k in range(grid.gx):
                part = dot(w_attn[b, k][:, sz.qkv : sz.qkv + sz.qc], dh_half[k], (0, 0))
                total = part if k == 0 else total + part
            dq[pl.ds(pl.multiple_of(b * sz.qc, 8), sz.qc), :] = total
            return carry

        lax.fori_loop(0, grid.gy, heads, 0)
        do_ref[...] = dq[...].astype(BF16)
        tokens.start(0)

    def turn_back(ref, heads):
        def one(k, carry):
            row = pl.multiple_of(k * HEAD_SIZE, HEAD_SIZE)
            ref[head_rows(k), :] = turn(ref, row, tables[0], tables[1], -1)
            return carry

        lax.fori_loop(0, heads, one, 0)

    def back_of(b):
        parts = [
            dq[pl.ds(pl.multiple_of(b * sz.qc, 8), sz.qc), :],
            dkv[pl.ds(pl.multiple_of(b * sz.kc, 8), sz.kc), :],
            dkv[pl.ds(pl.multiple_of(sz.kv + b * sz.kc, 8), sz.kc), :],
        ]
        return jnp.concatenate(parts, axis=0).astype(BF16)

    def block_grads():
        turn_back(dq, sz.heads)

        def arrived(n):
            dkv[...] += dkv_in[n].astype(F32)

        shift.finish(sz.before, arrived)
        turn_back(dkv, sz.kv_heads)

        def column(b, carry):
            back = jnp.transpose(back_of(b).astype(F32)).astype(BF16)
            mixed = o_ref[pl.ds(pl.multiple_of(b * sz.qc, 8), sz.qc), :]
            mixed = jnp.transpose(mixed.astype(F32)).astype(BF16)
            for k in range(grid.gx):
                parts = [dot(xn_ref[k], back, (1, 0)), dot(dh_half[k], mixed, (1, 0))]
                left = width - sz.qkv - sz.qc
                if left:
                    parts.append(jnp.zeros((sz.rows, left), F32))
                g_attn[b, k // grid.Y, k % grid.Y] = jnp.concatenate(parts, axis=1).astype(BF16)
            return carry

        lax.fori_loop(0, grid.gy, column, 0)
        for part in range(plan.parts):
            collect.load(plan.slots - plan.parts + part)

    def input_grads():
        backs = [back_of(b) for b in range(grid.gy)]
        inner = None
        for k in range(grid.gx):
            total = None
            for b in range(grid.gy):
                part = dot(w_attn[b, k][:, : sz.qkv], backs[b], (1, 0))
                total = part if b == 0 else total + part
            dx[k] = total
            value = xo[k].astype(F32)
            part = jnp.sum(total * gains[k, :, 0:1] * value, axis=0, keepdims=True)
            inner = part if k == 0 else inner + part
            gain_parts[k, 0:1, :] = row_of(jnp.sum(total * value * scale_ref[...], axis=1, keepdims=True), 128)
        scale = scale_ref[...]
        inner = scale * scale * scale * inner / sz.features
        for k in range(grid.gx):
            value = xo[k].astype(F32)
            ig_parts[k] = (dh_ref[k] + scale * (dx[k] * gains[k, :, 0:1]) - value * inner).astype(BF16)
        tokens.start(1)
        for _, copy in column_copies():
            copy.start()

    def gain_sums():
        gain_row[...] = gain_parts[i]
        for d, copy in column_copies():
            copy.wait()
            gain_row[...] += gain_in[d - 1]
        for _, copy in across_copies():
            copy.start()

    def slot(t, carry):
        pl.when(t == plan.slots - 1)(lambda: collect.begin(t))
        collect.slot(t)
        pl.when(t < plan.slots - 2)(lambda: collect.begin(t + 1))
        pl.when(t == 0)(feed_back)

        @pl.when(t == 1)
        def _():
            heads_of(0)
            heads_of(1)
            shift.start(sz.before)

        pl.when(t == 2)(block_grads)
        pl.when(t == 3)(input_grads)
        pl.when(t == 4)(gain_sums)
        return carry

    collect.begin(0)
    lax.fori_loop(0, plan.slots + collect.lags - 1, slot, 0)
    gaino[...] = gain_row[...]
    for d, copy in across_copies():
        copy.wait()
        gaino[...] += gain_across[d - 1]
    tokens.finish(0)
    tokens.finish(1)
    collect.finish()


def last_half(sz, both, down, w_all, w_attn, kept, back, hidden, h, dy, scale_two):
    grid, tok = sz.grid, sz.tok
    rows, width = w_attn.shape[-2:]
    cols = GROUPS * width
    plan = Plan(cols, REDUCE_ORDERS, REDUCE_PARTS)
    shapes, sems = Collect.scratch(grid, plan, rows, cols)
    sem = pltpu.SemaphoreType.DMA
    parts = (grid.gx, sz.rows, tok)
    shape = lambda g: g.reshape(grid.gy, grid.Z, grid.Y, rows, -1)
    return pl.pallas_call(
        functools.partial(last_kernel, sz, plan, width),
        out_shape=[
            jax.ShapeDtypeStruct((sz.rows, grid.gx * tok), BF16),
            jax.ShapeDtypeStruct((sz.rows, grid.gx * tok), BF16),
            jax.ShapeDtypeStruct((rows, cols), F32),
            jax.ShapeDtypeStruct((8, 128), F32),
        ],
        in_specs=[HBM_SPEC] * 3 + [VMEM_SPEC] * 16,
        out_specs=[VMEM_SPEC] * 4,
        scratch_shapes=[
            pltpu.VMEM((sz.q, tok), BF16),
            pltpu.VMEM(parts, F32),
            pltpu.VMEM(parts, BF16),
            pltpu.VMEM(parts, BF16),
            pltpu.VMEM((sz.q, tok), F32),
            pltpu.VMEM((sz.before, 2 * sz.kv, tok), BF16),
            pltpu.VMEM((sz.before, 2 * sz.kv, tok), BF16),
            pltpu.VMEM((2 * sz.kv, tok), F32),
            pltpu.VMEM((grid.gy, grid.Z, grid.Y, rows, width), BF16),
            pltpu.VMEM(parts, F32),
            pltpu.VMEM(parts, F32),
            pltpu.VMEM(parts, BF16),
            pltpu.VMEM((grid.gx, 8, 128), F32),
            pltpu.VMEM((grid.gx - 1, 8, 128), F32),
            pltpu.VMEM((8, 128), F32),
            pltpu.VMEM((grid.gy - 1, 8, 128), F32),
        ]
        + shapes[:2]
        + [sem((3,))]
        + shapes[2:]
        + Tokens.semaphores(grid, 2)
        + [sem((sz.before,))] * 2
        + [sem((grid.gx - 1,))] * 2
        + [sem((grid.gy - 1,))] * 2
        + sems,
        compiler_params=params(1),
        name="last_half",
    )(shape(both), shape(down), shape(w_all), w_attn, *kept, back, hidden, h, dy, scale_two)


def einsum(form, a, b):
    return jnp.einsum(form, a, b, preferred_element_type=F32)


def padded(a, axis, size):
    pads = [(0, 0)] * a.ndim
    pads[axis] = (0, size - a.shape[axis])
    return jnp.pad(a, pads) if size != a.shape[axis] else a


def shards(
    grid,
    block_input,
    attn_gain,
    query_weight,
    key_weight,
    value_weight,
    output_weight,
    ffn_gain,
    gate_weight,
    up_weight,
    down_weight,
    segment_ids,
    out_cotangent,
):
    GX, GY = grid.gx, grid.gy
    rows, row_tokens = block_input.shape
    tok = row_tokens // GX
    sz = Sizes(grid, tok, rows, query_weight.shape[1], key_weight.shape[1])
    fc, features = gate_weight.shape[1], sz.features
    groups = [
        jnp.concatenate([query_weight, key_weight, value_weight, output_weight.T], axis=1), gate_weight, up_weight, down_weight.T
    ]
    width = -(-max(g.shape[1] for g in groups) // 128) * 128
    block = jnp.concatenate([padded(g, 1, width) for g in groups], axis=1)
    small = jnp.concatenate(
        [segment_ids.reshape(sz.span, tok).astype(F32), padded(jnp.stack([attn_gain, ffn_gain]), 1, tok)], axis=0
    )
    small = padded(small, 0, -(-small.shape[0] // 8) * 8)
    (
        x_parts, dy_parts, w_all, w_attn, _, normed_one, scale_one, query, key_value, earlier, mixed, bias, tables, gains,
        hidden_in, normed_two, scale_two,
    ) = first_half(sz, row_tokens // PACKED_LENGTH, block_input, out_cotangent, small, block)
    dy_half = dy_parts.reshape(features, tok)
    w_cols = w_all.reshape(GY, features, -1)
    w_down = w_cols[:, :, 3 * width : 3 * width + fc]
    normed_two = normed_two.reshape(features, tok)

    gate_up = einsum("jdf,dt->jft", w_cols[:, :, width : 3 * width], normed_two)
    gate, up = gate_up[:, :fc], gate_up[:, width : width + fc]
    sigmoid = jax.nn.sigmoid(gate)
    hidden = padded((jax.nn.silu(gate) * up).astype(BF16), 1, width)
    hidden_grad = einsum("jdf,dt->jft", w_down, dy_half)
    gate_back = (hidden_grad * up * sigmoid * (1.0 + gate * (1.0 - sigmoid))).astype(BF16)
    up_back = (hidden_grad * gate * sigmoid).astype(BF16)
    both_back = jnp.concatenate([padded(gate_back, 1, width), padded(up_back, 1, width)], axis=1)
    grad_both = einsum("dt,jft->jdf", normed_two, both_back).astype(BF16)
    grad_down = einsum("dt,jft->jdf", dy_half, hidden).astype(BF16)
    block_output, input_grad, grads, gains = last_half(
        sz, grad_both, grad_down, w_all, w_attn,
        (x_parts, normed_one, scale_one, query, key_value, earlier, mixed, bias, tables, gains),
        both_back, hidden, hidden_in, dy_parts, scale_two,
    )
    grad_gate, grad_up, grad_down, grad_attn = (grads[:, k * width : (k + 1) * width] for k in range(GROUPS))
    qc, kc = sz.qc, sz.kc
    return (
        block_output,
        input_grad.astype(F32),
        gains[0, :rows],
        grad_attn[:, :qc],
        grad_attn[:, qc : qc + kc],
        grad_attn[:, qc + kc : sz.qkv],
        grad_attn[:, sz.qkv : sz.qkv + qc].T,
        gains[1, :rows],
        grad_gate[:, :fc],
        grad_up[:, :fc],
        grad_down[:, :fc].T,
    )


def solution(mesh):
    grid = Grid(mesh.shape["gx"], mesh.shape["gy"])
    return jax.shard_map(
        functools.partial(shards, grid),
        mesh=mesh,
        in_specs=(
            P("gx", "gy"),
            P("gx"),
            P("gx", "gy"),
            P("gx", "gy"),
            P("gx", "gy"),
            P("gy", "gx"),
            P("gx"),
            P("gx", "gy"),
            P("gx", "gy"),
            P("gy", "gx"),
            P("gx", None),
            P("gx", "gy"),
        ),
        out_specs=(
            P("gx", "gy"),
            P("gx", "gy"),
            P("gx"),
            P("gx", "gy"),
            P("gx", "gy"),
            P("gx", "gy"),
            P("gy", "gx"),
            P("gx"),
            P("gx", "gy"),
            P("gx", "gy"),
            P("gy", "gx"),
        ),
        check_vma=False,
    )
```
